8 devices in a mesh: dp: 1 (over z), cp: 8 (over y, x, core).
Axes of the slice: x: 2, y: 2, z: 1, core: 2. Of those that a mesh axis runs over, the one named last changes fastest.
Arguments:
- hidden: bfloat16 [16, 1024, 2048], P('dp', 'cp')
- positions: int32 [16, 1024], P('dp', 'cp')
- norm_gain: bfloat16 [2048], replicated
- w_query: bfloat16 [2048, 2048], replicated
- w_key: bfloat16 [2048, 512], replicated
- w_value: bfloat16 [2048, 512], replicated
- w_out: bfloat16 [32, 64, 2048], replicated
Outputs:
- output: bfloat16 [16, 1024, 2048], P('dp', 'cp')
All inputs are finite; a program needn't handle non-finite values.
Results may differ from the reference program's by a relative error of at most 0.00742257.
Values are sent between devices in bfloat16 or wider.
A program may use at most 1 GiB of HBM per device.

```python
import jax
import jax.numpy as jnp
from jax import lax

BATCH = 16
SEQ = 1024
QBLOCK = 128
D = 2048
HEADS = 32
KV_HEADS = 8
HEAD = 64

GROUPS = HEADS // KV_HEADS
NBLOCKS = SEQ // QBLOCK


def draw_positions(pos_key):
    off_key, stride_key = jax.random.split(pos_key)
    offsets = jax.random.randint(off_key, (BATCH, 1), 0, SEQ)
    strides = jax.random.randint(stride_key, (BATCH, SEQ), 1, 3)
    return (offsets + jnp.cumsum(strides, axis=1) - 1).astype(jnp.int32)


def normal_weight(weight_key, shape, scale):
    return (scale * jax.random.normal(weight_key, shape, jnp.float32)).astype(jnp.bfloat16)


def setup_inputs(seed: int = 0, part: int = 0) -> dict:
    root = jax.random.key(seed)
    part_key = jax.random.fold_in(root, part)
    shared = jax.random.fold_in(root, 1000003)
    hid_key, pos_key = jax.random.split(part_key)
    gain_key, q_key, k_key, v_key, o_key = jax.random.split(shared, 5)
    hidden = (0.25 * jax.random.normal(hid_key, (BATCH, SEQ, D), jnp.float32)).astype(jnp.bfloat16)
    norm_gain = (1.0 + 0.3 * jax.random.normal(gain_key, (D,), jnp.float32)).astype(jnp.bfloat16)
    return {
        'hidden': hidden,
        'positions': draw_positions(pos_key),
        'norm_gain': norm_gain,
        'w_query': normal_weight(q_key, (D, HEADS * HEAD), 1.3 * D ** -0.5),
        'w_key': normal_weight(k_key, (D, KV_HEADS * HEAD), 1.3 * D ** -0.5),
        'w_value': normal_weight(v_key, (D, KV_HEADS * HEAD), D ** -0.5),
        'w_out': normal_weight(o_key, (HEADS, HEAD, D), 2.0 * (HEADS * HEAD) ** -0.5),
    }


def rms_norm(hidden, norm_gain):
    x_f32 = hidden.astype(jnp.float32)
    inv_rms = lax.rsqrt(jnp.mean(x_f32 * x_f32, axis=-1, keepdims=True) + 1e-5)
    return (x_f32 * inv_rms * norm_gain.astype(jnp.float32)).astype(jnp.bfloat16)


def rotary(proj_f32, positions):
    head_dim = proj_f32.shape[-1]
    half_dim = head_dim // 2
    inv_freq = 10000.0 ** (-2.0 * jnp.arange(half_dim, dtype=jnp.float32) / head_dim)
    angles = positions.astype(jnp.float32)[:, :, None] * inv_freq
    cos_part = jnp.cos(angles)[:, :, None, :]
    sin_part = jnp.sin(angles)[:, :, None, :]
    first_half = proj_f32[..., :half_dim]
    second_half = proj_f32[..., half_dim:]
    return jnp.concatenate([first_half * cos_part - second_half * sin_part, second_half * cos_part + first_half * sin_part], axis=-1).astype(jnp.bfloat16)


def reference(hidden, positions, norm_gain, w_query, w_key, w_value, w_out):
    normed = rms_norm(hidden, norm_gain).reshape(BATCH * SEQ, D)
    q_rot = rotary(jnp.dot(normed, w_query, preferred_element_type=jnp.float32).reshape(BATCH, SEQ, HEADS, HEAD), positions)
    k_rot = rotary(jnp.dot(normed, w_key, preferred_element_type=jnp.float32).reshape(BATCH, SEQ, KV_HEADS, HEAD), positions)
    v_all = jnp.dot(normed, w_value, preferred_element_type=jnp.float32).astype(jnp.bfloat16).reshape(BATCH, SEQ, KV_HEADS, HEAD)
    q_grp = q_rot.reshape(BATCH, SEQ, KV_HEADS, GROUPS, HEAD).astype(jnp.float32)
    k_f32 = k_rot.astype(jnp.float32)
    v_f32 = v_all.astype(jnp.float32)
    w_out_grp = w_out.reshape(KV_HEADS, GROUPS, HEAD, D).astype(jnp.float32)
    token_idx = jnp.arange(QBLOCK)

    def query_block(query_idx):
        q_blk = lax.dynamic_slice_in_dim(q_grp, query_idx * QBLOCK, QBLOCK, axis=1)

        def key_step(att_state, key_idx):
            def consume(state_in):
                run_max, run_sum, acc_out = state_in
                k_blk = lax.dynamic_slice_in_dim(k_f32, key_idx * QBLOCK, QBLOCK, axis=1)
                v_blk = lax.dynamic_slice_in_dim(v_f32, key_idx * QBLOCK, QBLOCK, axis=1)
                scores = jnp.einsum('bqkgd,bskd->bkgqs', q_blk, k_blk) * (HEAD ** -0.5)
                allowed = (query_idx * QBLOCK + token_idx)[:, None] >= (key_idx * QBLOCK + token_idx)[None, :]
                scores = jnp.where(allowed, scores, -jnp.inf)
                new_max = jnp.maximum(run_max, jnp.max(scores, axis=-1))
                prob_blk = jnp.exp(scores - new_max[..., None])
                rescale = jnp.exp(run_max - new_max)
                new_sum = run_sum * rescale + jnp.sum(prob_blk, axis=-1)
                new_acc = acc_out * rescale[..., None] + jnp.einsum('bkgqs,bskd->bkgqd', prob_blk, v_blk)
                return new_max, new_sum, new_acc
            return lax.cond(key_idx <= query_idx, consume, lambda state_kept: state_kept, att_state), None

        start_state = (
            jnp.full((BATCH, KV_HEADS, GROUPS, QBLOCK), -jnp.inf, jnp.float32),
            jnp.zeros((BATCH, KV_HEADS, GROUPS, QBLOCK), jnp.float32),
            jnp.zeros((BATCH, KV_HEADS, GROUPS, QBLOCK, HEAD), jnp.float32),
        )
        final_state, _ = lax.scan(key_step, start_state, jnp.arange(NBLOCKS))
        attn_out = (final_state[2] / final_state[1][..., None]).astype(jnp.bfloat16).astype(jnp.float32)
        x_blk = lax.dynamic_slice_in_dim(hidden, query_idx * QBLOCK, QBLOCK, axis=1).astype(jnp.float32)
        return (x_blk + jnp.einsum('bkgqd,kgde->bqe', attn_out, w_out_grp)).astype(jnp.bfloat16)

    out_blocks = lax.map(query_block, jnp.arange(NBLOCKS))
    return jnp.moveaxis(out_blocks, 0, 1).reshape(BATCH, SEQ, D)
```

```python
import functools

import jax
import jax.numpy as jnp
from jax import lax
from jax.experimental import pallas as pl
from jax.experimental.pallas import tpu as pltpu
from jax.sharding import PartitionSpec as P

HEAD = 64
LANES = 128
CHUNKS = 4
F32, BF16 = jnp.float32, jnp.bfloat16


def normed_rows(x, gain):
    x = x.astype(F32)
    inv_rms = lax.rsqrt(jnp.mean(x * x, axis=-1, keepdims=True) + 1e-5)
    return (x * inv_rms * gain.astype(F32)).astype(BF16)


def lane_masks(rows):
    lane = lax.broadcasted_iota(jnp.int32, (rows, LANES), 1)
    return lane % HEAD < HEAD // 2, lane < HEAD


def rope(x, cos, sin, first_half):
    other = jnp.where(first_half, pltpu.roll(x, LANES - HEAD // 2, 1), pltpu.roll(x, HEAD // 2, 1))
    return x * cos + other * sin


def kv_kernel(x_ref, gain_ref, wk_ref, wv_ref, cos_ref, sin_ref, kv_ref):
    rows = x_ref.shape[0]
    width = wk_ref.shape[1]
    normed = normed_rows(x_ref[...], gain_ref[...])
    first_half, _ = lane_masks(rows)
    k = jnp.dot(normed, wk_ref[...], preferred_element_type=F32)
    cos, sin = cos_ref[...], sin_ref[...]
    for col in range(0, width, LANES):
        kv_ref[:, col:col + LANES] = rope(k[:, col:col + LANES], cos, sin, first_half).astype(BF16)
    kv_ref[:, width:] = jnp.dot(normed, wv_ref[...], preferred_element_type=F32).astype(BF16)


def q_kernel(x_ref, gain_ref, wq_ref, cos_ref, sin_ref, q_ref):
    rows = x_ref.shape[0]
    normed = normed_rows(x_ref[...], gain_ref[...])
    first_half, low = lane_masks(rows)
    cos, sin = cos_ref[...], sin_ref[...]
    for base in range(0, wq_ref.shape[1], 4 * LANES):
        q = jnp.dot(normed, wq_ref[:, base:base + 4 * LANES], preferred_element_type=F32)
        s = [rope(q[:, i * LANES:(i + 1) * LANES], cos, sin, first_half) * (HEAD ** -0.5) for i in range(4)]
        for i in range(2):
            q_ref[:, base + 2 * i * LANES:base + (2 * i + 1) * LANES] = jnp.where(low, s[i], pltpu.roll(s[i + 2], HEAD, 1)).astype(BF16)
            q_ref[:, base + (2 * i + 1) * LANES:base + (2 * i + 2) * LANES] = jnp.where(low, pltpu.roll(s[i], HEAD, 1), s[i + 2]).astype(BF16)


def softmax_values(scores, values, bias):
    n_keys, tail = scores.shape[1], bias.shape[1]
    last = scores[:, n_keys - tail:] + bias
    scores = last if n_keys == tail else jnp.concatenate([scores[:, :n_keys - tail], last], axis=1)
    peak = jnp.max(scores, axis=-1, keepdims=True)
    prob = jnp.exp(scores - peak)
    total = jnp.sum(prob, axis=-1, keepdims=True)
    return jnp.dot(prob.astype(BF16), values, preferred_element_type=F32) / total


def attend(q_ref, kv_ref, seq, o_ref, n_blocks, core, tokens):
    width = kv_ref.shape[-1] // 2
    n_keys = n_blocks * tokens
    _, low = lane_masks(tokens)
    key = lax.broadcasted_iota(jnp.int32, (tokens, 2 * tokens), 1)
    row = lax.broadcasted_iota(jnp.int32, (tokens, 2 * tokens), 0)
    bias = jnp.where(key <= row + core * tokens, 0.0, -jnp.inf).astype(F32)
    bias = jnp.concatenate([bias] * 4, axis=0)
    rows = pl.ds(seq * tokens, tokens)

    def pair(j, carry):
        keys = kv_ref[:n_blocks, seq, :, pl.ds(pl.multiple_of(j * LANES, LANES), LANES)].reshape(n_keys, LANES)
        values = kv_ref[:n_blocks, seq, :, pl.ds(pl.multiple_of(width + j * LANES, LANES), LANES)].reshape(n_keys, LANES)
        base = pl.multiple_of(j * 4 * LANES, LANES)
        q = [q_ref[rows, pl.ds(pl.multiple_of(base + i * LANES, LANES), LANES)] for i in range(4)]
        zero = jnp.zeros_like(q[0])
        halves = []
        for side in range(2):
            lhs = jnp.concatenate([jnp.where(low, t, zero) if side == 0 else jnp.where(low, zero, t) for t in q], axis=0)
            halves.append(lax.dot_general(lhs, keys, (((1,), (1,)), ((), ())), preferred_element_type=F32))
        outs = [softmax_values(scores, values, bias) for scores in halves]
        for i in range(4):
            part = slice(i * tokens, (i + 1) * tokens)
            o_ref[rows, pl.ds(pl.multiple_of(base + i * LANES, LANES), LANES)] = jnp.where(low, outs[0][part], outs[1][part]).astype(BF16)
        return carry

    lax.fori_loop(0, width // LANES, pair, 0)


def attention_kernel(q_ref, kv_ref, x_ref, wo_ref, *rest):
    y_ref, o_ref = rest[-2:]
    n_dev, seqs, tokens, _ = kv_ref.shape
    me = lax.axis_index('cp')
    chip, core = me // 2, me % 2
    for c in range(n_dev // 2):
        @pl.when(chip == c)
        def _():
            for seq in range(seqs):
                attend(q_ref, kv_ref, seq, o_ref, 2 * (c + 1), core, tokens)
    proj = jnp.dot(o_ref[...], wo_ref[...], preferred_element_type=F32)
    y_ref[...] = (x_ref[...].astype(F32) + proj).astype(BF16)


def solution(mesh):
    n_cp = mesh.shape['cp']

    def local_block(hidden, positions, norm_gain, w_query, w_key, w_value, w_out):
        batch, tokens, dim = hidden.shape
        n_heads = w_out.shape[0]
        kv_width = w_key.shape[1]
        rows = batch * tokens
        x = hidden.reshape(rows, dim)
        gain = norm_gain.reshape(1, dim)
        half = HEAD // 2
        lane = jnp.arange(LANES)
        inv_freq = 10000.0 ** (-2.0 * (lane % half).astype(F32) / HEAD)
        angles = positions.reshape(rows, 1).astype(F32) * inv_freq
        cos = jnp.cos(angles)
        sin = jnp.sin(angles) * jnp.where(lane % HEAD < half, -1.0, 1.0)
        wo = w_out.reshape(n_heads // 8, 2, 4, HEAD, dim).transpose(0, 2, 1, 3, 4).reshape(n_heads * HEAD, dim)
        crows = rows // CHUNKS
        cseq = batch // CHUNKS
        whole = lambda a: pl.BlockSpec(a.shape, lambda i: (0,) * a.ndim)
        params = pltpu.CompilerParams(vmem_limit_bytes=60 * 2 ** 20, dimension_semantics=('arbitrary',))

        gathered = []
        for c in range(CHUNKS):
            at = lambda n, c=c: pl.BlockSpec((crows, n), lambda i: (c, 0))
            kv = pl.pallas_call(
                kv_kernel,
                grid=(1,),
                out_shape=jax.ShapeDtypeStruct((crows, 2 * kv_width), BF16),
                in_specs=[at(dim), whole(gain), whole(w_key), whole(w_value), at(LANES), at(LANES)],
                out_specs=pl.BlockSpec((crows, 2 * kv_width), lambda i: (0, 0)),
                compiler_params=params,
                cost_estimate=pl.CostEstimate(flops=4 * crows * dim * kv_width, bytes_accessed=2 * crows * dim, transcendentals=0),
                name='kv',
            )(x, gain, w_key, w_value, cos, sin)
            gathered.append(lax.all_gather(kv.reshape(cseq, tokens, 2 * kv_width), 'cp'))

        at = lambda n: pl.BlockSpec((crows, n), lambda i: (i, 0))
        q = pl.pallas_call(
            q_kernel,
            grid=(CHUNKS,),
            out_shape=jax.ShapeDtypeStruct((rows, dim), BF16),
            in_specs=[at(dim), whole(gain), whole(w_query), at(LANES), at(LANES)],
            out_specs=at(dim),
            compiler_params=params,
            cost_estimate=pl.CostEstimate(flops=2 * rows * dim * dim, bytes_accessed=4 * rows * dim, transcendentals=0),
            name='q',
        )(x, gain, w_query, cos, sin)

        y = None
        sb = 2
        for c in range(CHUNKS):
            steps = cseq // sb
            at = lambda n, c=c: pl.BlockSpec((sb * tokens, n), lambda i: (c * steps + i, 0))
            kv_spec = pl.BlockSpec((n_cp, sb, tokens, 2 * kv_width), lambda i: (0, i, 0, 0))
            operands = [q, gathered[c], x, wo]
            specs = [at(dim), kv_spec, at(dim), whole(wo)]
            alias = {}
            if y is not None:
                operands.append(y)
                specs.append(pl.BlockSpec(memory_space=pl.ANY))
                alias = {4: 0}
            y = pl.pallas_call(
                attention_kernel,
                grid=(steps,),
                out_shape=jax.ShapeDtypeStruct((rows, dim), BF16),
                in_specs=specs,
                out_specs=at(dim),
                scratch_shapes=[pltpu.VMEM((sb * tokens, dim), BF16)],
                input_output_aliases=alias,
                compiler_params=params,
                cost_estimate=pl.CostEstimate(flops=8 * crows * dim * dim, bytes_accessed=4 * crows * dim, transcendentals=0),
                name='attention',
            )(*operands)
        return y.reshape(batch, tokens, dim)

    act_spec = P('dp', 'cp', None)
    return jax.shard_map(local_block, mesh=mesh, in_specs=(act_spec, P('dp', 'cp'), P(), P(), P(), P(), P()), out_specs=act_spec, check_vma=False)
```

```python
import functools

import jax
import jax.numpy as jnp
from jax import lax
from jax.experimental import pallas as pl
from jax.experimental.pallas import tpu as pltpu
from jax.sharding import PartitionSpec as P

MESH = pl.DeviceIdType.MESH
HEAD = 64
HALF = HEAD // 2
TOK = 128
GROUP = 4
AHEAD = 4
CHUNK = 4 * TOK
WBLOCK = 256
F32, BF16 = jnp.float32, jnp.bfloat16
NT = (((1,), (1,)), ((), ()))


def rope_rows(x, cos, sin):
    heads, n = x.shape[0] // HEAD, x.shape[1]
    x = x.reshape(heads, 2, HALF, n)
    a, b = x[:, 0], x[:, 1]
    rotated = jnp.stack([a * cos - b * sin, b * cos + a * sin], axis=1)
    return rotated.reshape(heads * HEAD, n)


def attend(q_ref, slot_ref, bias_ref, s_ref, m_ref, o_ref, seq, slot, n_blocks, between):
    width = slot_ref.shape[2] // 2
    pairs = width // (2 * HEAD)
    key_chunks = n_blocks // 2
    kc = 2 * TOK
    cols = GROUP * TOK

    def queries(g):
        base = g * GROUP * HEAD
        return jnp.concatenate([q_ref[seq, pl.ds(pl.multiple_of(base + i * HEAD, HEAD), HEAD), :] for i in range(GROUP)], axis=1)

    def scores(q, g, c, peak):
        row = pl.ds(pl.multiple_of(g * HEAD, HEAD), HEAD)
        keys = jnp.concatenate([slot_ref[slot, 2 * c + i, row, :].T for i in range(2)], axis=0)
        s = jnp.dot(keys, q, preferred_element_type=F32)
        if c == key_chunks - 1:
            s = s + bias_ref[...]
        s_ref[c * kc:(c + 1) * kc, :] = s
        top = jnp.max(s.reshape(kc // 8, 8, cols), axis=0)
        return top if peak is None else jnp.maximum(peak, top)

    def unit(g, g_next, peak):
        peak = jnp.max(peak, axis=0, keepdims=True)
        q_next = queries(g_next)
        vrow = pl.ds(pl.multiple_of(width + g * HEAD, HEAD), HEAD)
        total, out, peak_next = None, None, None
        for c in range(key_chunks):
            prob = jnp.exp(s_ref[c * kc:(c + 1) * kc, :] - peak)
            part = jnp.sum(prob.reshape(kc // 8, 8, cols), axis=0)
            total = part if total is None else total + part
            values = jnp.concatenate([slot_ref[slot, 2 * c + i, vrow, :] for i in range(2)], axis=1)
            term = jnp.dot(values, prob.astype(BF16), preferred_element_type=F32)
            out = term if out is None else out + term
            peak_next = scores(q_next, g_next, c, peak_next)
        out = out / jnp.sum(total, axis=0, keepdims=True)
        for i in range(GROUP):
            o_ref[pl.ds(pl.multiple_of((g * GROUP + i) * HEAD, HEAD), HEAD), :] = out[:, i * TOK:(i + 1) * TOK].astype(BF16)
        return peak_next

    q_first, peak = queries(0), None
    for c in range(key_chunks):
        peak = scores(q_first, 0, c, peak)
    m_ref[...] = peak

    def pair(j, carry):
        @pl.when(j == pairs - 1)
        def _():
            between()

        peak = unit(2 * j, 2 * j + 1, m_ref[...])
        m_ref[...] = unit(2 * j + 1, jnp.minimum(2 * j + 2, 2 * pairs - 1), peak)
        return carry

    lax.fori_loop(0, pairs, pair, 0)


def block_kernel(
    n_cp, x_hbm, gain_ref, wq_hbm, wk_hbm, wv_hbm, wo_hbm, cos_ref, sin_ref, y_hbm, kv_hbm,
    x_st, h_ref, w_st, wkv_ref, w_ref, kv_st, q_ref, slot_ref, s_ref, m_ref, bias_ref, ot_ref, o_ref, xr_ref, y_st,
    x_sem, w_sem, wo_sem, recv_sem, own_sem, fwd_sem, load_sem, sib_recv, sib_send, xr_sem, y_sem, credit,
):
    me = lax.axis_index('cp')
    chip, core = me // 2, me % 2
    sibling = me + 1 - 2 * core
    n_seq = kv_st.shape[0]
    dim = x_st.shape[2]
    kv_rows = wkv_ref.shape[0]
    n_chunks = n_seq * TOK // CHUNK
    seqs = CHUNK // TOK
    last_chip = n_cp // 2 - 1

    barrier = pltpu.get_barrier_semaphore()
    for step in range(1, n_cp):
        pl.semaphore_signal(barrier, inc=1, device_id={'cp': (me + step) % n_cp}, device_id_type=MESH)

    def x_copy(chunk):
        return pltpu.make_async_copy(x_hbm.at[pl.ds(chunk * CHUNK, CHUNK), :], x_st.at[chunk % 2], x_sem.at[chunk % 2])

    def w_copy(hbm, block, slot):
        return pltpu.make_async_copy(hbm.at[:, pl.ds(block * WBLOCK, WBLOCK)], w_st.at[slot], w_sem.at[slot])

    kv_blocks = [(wk_hbm, i) for i in range(kv_rows // 2 // WBLOCK)] + [(wv_hbm, i) for i in range(kv_rows // 2 // WBLOCK)]
    q_blocks = dim // WBLOCK
    x_copy(0).start()
    for i in range(2):
        w_copy(*kv_blocks[i], i).start()
    x_copy(1).start()

    key = lax.broadcasted_iota(jnp.int32, (2 * TOK, TOK), 0)
    tok = lax.broadcasted_iota(jnp.int32, (2 * TOK, TOK), 1)
    bias = jnp.where(key <= tok + core * TOK, 0.0, -jnp.inf).astype(F32)
    bias_ref[...] = jnp.concatenate([bias] * GROUP, axis=1)

    for i, (hbm, block) in enumerate(kv_blocks):
        w_copy(hbm, block, i % 2).wait()
        wkv_ref[i * WBLOCK:(i + 1) * WBLOCK, :] = w_st[i % 2].T
        nxt = i + 2
        if nxt < len(kv_blocks):
            w_copy(*kv_blocks[nxt], i % 2).start()
        else:
            w_copy(wq_hbm, nxt - len(kv_blocks), i % 2).start()

    def own_send(seq, target, to_chip, from_chip):
        return pltpu.make_async_remote_copy(
            src_ref=kv_st.at[seq], dst_ref=kv_hbm.at[seq, from_chip], send_sem=own_sem.at[seq, target],
            recv_sem=recv_sem.at[seq, from_chip], device_id={'cp': 2 * to_chip + core}, device_id_type=MESH)

    def forward(seq, block, to_chip):
        return pltpu.make_async_remote_copy(
            src_ref=kv_hbm.at[seq, block], dst_ref=kv_hbm.at[seq, block], send_sem=fwd_sem.at[seq],
            recv_sem=recv_sem.at[seq, block], device_id={'cp': 2 * to_chip + core}, device_id_type=MESH)

    def project_kv(chunk, carry):
        x_copy(chunk).wait()
        x = x_st[chunk % 2].astype(F32)
        inv_rms = lax.rsqrt(jnp.mean(x * x, axis=-1, keepdims=True) + 1e-5)
        rows = pl.ds(pl.multiple_of(chunk * CHUNK, CHUNK), CHUNK)
        h_ref[rows, :] = (x * inv_rms * gain_ref[...].astype(F32)).astype(BF16)

        @pl.when(chunk + 2 < n_chunks)
        def _():
            x_copy(chunk + 2).start()

        kv = lax.dot_general(wkv_ref[...], h_ref[rows, :], NT, preferred_element_type=F32)
        k = rope_rows(kv[:kv_rows // 2], cos_ref[chunk], sin_ref[chunk]).astype(BF16)
        v = kv[kv_rows // 2:].astype(BF16)
        for i in range(seqs):
            kv_st[chunk * seqs + i, :kv_rows // 2, :] = k[:, i * TOK:(i + 1) * TOK]
            kv_st[chunk * seqs + i, kv_rows // 2:, :] = v[:, i * TOK:(i + 1) * TOK]

        @pl.when(chunk == 0)
        def _():
            pl.semaphore_wait(barrier, n_cp - 1)

        @pl.when(chip == 0)
        def _():
            for i in range(seqs):
                own_send(chunk * seqs + i, 0, 1, 0).start()
                own_send(chunk * seqs + i, 1, 2, 0).start()

        for c in range(1, last_chip):
            @pl.when((chip == c) & (chunk == 0))
            def _():
                for i in range(AHEAD):
                    own_send(i, 0, last_chip, c).start()

        return carry

    lax.fori_loop(0, n_chunks, project_kv, 0)

    def turn_wq(i, carry):
        for k in range(2):
            w_copy(wq_hbm, 2 * i + k, k).wait()
            w_ref[pl.ds(pl.multiple_of((2 * i + k) * WBLOCK, WBLOCK), WBLOCK), :] = w_st[k].T

            @pl.when(2 * i + k + 2 < q_blocks)
            def _():
                w_copy(wq_hbm, 2 * i + k + 2, k).start()

        return carry

    lax.fori_loop(0, q_blocks // 2, turn_wq, 0)

    def hop(seq):
        for c in range(1, last_chip):
            @pl.when(chip == c)
            def _():
                own_send(seq, 0, c, 0).wait_recv()

                @pl.when(core == c - 1)
                def _():
                    forward(seq, 0, last_chip).start()

                @pl.when(seq + AHEAD < n_seq)
                def _():
                    own_send(seq + AHEAD, 0, last_chip, c).start()

        @pl.when(chip == last_chip)
        def _():
            own_send(seq, 0, last_chip, 1).wait_recv()
            forward(seq, 1, 2).start()

    q_rows = dim // 2

    def project_q(i, carry):
        chunk, part = i // 2, i % 2
        base = pl.multiple_of(part * q_rows, q_rows)
        h = h_ref[pl.ds(pl.multiple_of(chunk * CHUNK, CHUNK), CHUNK), :]
        q = lax.dot_general(w_ref[pl.ds(base, q_rows), :], h, NT, preferred_element_type=F32)
        q = (rope_rows(q, cos_ref[chunk], sin_ref[chunk]) * (HEAD ** -0.5)).astype(BF16)
        for k in range(seqs):
            q_ref[chunk * seqs + k, pl.ds(base, q_rows), :] = q[:, k * TOK:(k + 1) * TOK]

        @pl.when(part == 1)
        def _():
            hop(chunk)

        return carry

    lax.fori_loop(0, 2 * n_chunks, project_q, 0)
    wo_copy = pltpu.make_async_copy(wo_hbm, w_ref, wo_sem)
    wo_copy.start()

    def xr_copy(p):
        return pltpu.make_async_copy(x_hbm.at[pl.ds(p * 2 * TOK, 2 * TOK), :], xr_ref.at[p % 2], xr_sem.at[p % 2])

    def y_copy(p):
        return pltpu.make_async_copy(y_st.at[p % 2], y_hbm.at[pl.ds(p * 2 * TOK, 2 * TOK), :], y_sem.at[p % 2])

    xr_copy(0).start()
    xr_copy(1).start()

    def load(seq, a):
        return pltpu.make_async_copy(kv_hbm.at[seq, a], slot_ref.at[seq % 2, 2 * a + core], load_sem.at[seq % 2, a])

    def share(seq, a, src):
        return pltpu.make_async_remote_copy(
            src_ref=src, dst_ref=slot_ref.at[seq % 2, 2 * a + core], send_sem=sib_send.at[seq % 2, a],
            recv_sem=sib_recv.at[seq % 2, a], device_id={'cp': sibling}, device_id_type=MESH)

    def stage(c, seq):
        @pl.when(seq >= 2)
        def _():
            pl.semaphore_wait(credit, 1)
            for a in range(c + 1):
                share(seq, a, kv_st.at[seq]).wait_send()

        share(seq, c, kv_st.at[seq]).start()
        slot_ref[seq % 2, 2 * c + core] = kv_st[seq]
        hopped = 1 if c == last_chip else 0
        for a in [hopped] + [a for a in range(c) if a != hopped] if c else []:
            if a != hopped:
                own_send(seq, 0, c, a).wait_recv()
            share(seq, a, kv_hbm.at[seq, a]).start()
            load(seq, a).start()

    for c in range(last_chip + 1):
        @pl.when(chip == c)
        def _():
            stage(c, 0)

    def project_out(p):
        @pl.when(p == 0)
        def _():
            wo_copy.wait()

        xr_copy(p).wait()

        @pl.when(p >= 2)
        def _():
            y_copy(p - 2).wait()

        step = 512
        for col in range(0, dim, step):
            proj = jnp.dot(o_ref[...], w_ref[:, col:col + step], preferred_element_type=F32)
            y_st[p % 2, :, col:col + step] = (xr_ref[p % 2, :, col:col + step].astype(F32) + proj).astype(BF16)
        y_copy(p).start()

        @pl.when(p + 2 < n_seq // 2)
        def _():
            xr_copy(p + 2).start()

    def sequence(seq, carry):
        for c in range(last_chip + 1):
            @pl.when(chip == c)
            def _():
                for a in range(c):
                    load(seq, a).wait()
                for a in range(c + 1):
                    share(seq, a, kv_st.at[seq]).wait_recv()

                def between():
                    @pl.when(seq + 1 < n_seq)
                    def _():
                        stage(c, seq + 1)

                    if c:
                        @pl.when(seq + AHEAD < n_seq)
                        def _():
                            hop(seq + AHEAD)

                attend(q_ref, slot_ref, bias_ref, s_ref, m_ref, ot_ref, seq, seq % 2, 2 * (c + 1), between)

        @pl.when(seq + 2 < n_seq)
        def _():
            pl.semaphore_signal(credit, inc=1, device_id={'cp': sibling}, device_id_type=MESH)

        o_ref[pl.ds(pl.multiple_of(seq % 2 * TOK, TOK), TOK), :] = ot_ref[...].T

        @pl.when(seq % 2 == 1)
        def _():
            project_out(seq // 2)

        return carry

    lax.fori_loop(0, n_seq, sequence, 0)

    for p in (n_seq // 2 - 2, n_seq // 2 - 1):
        y_copy(p).wait()
    for c in range(last_chip + 1):
        @pl.when(chip == c)
        def _():
            for seq in (n_seq - 2, n_seq - 1):
                for a in range(c + 1):
                    share(seq, a, kv_st.at[seq]).wait_send()

    def drain(seq, carry):
        @pl.when(chip == 0)
        def _():
            own_send(seq, 0, 1, 0).wait_send()
            own_send(seq, 1, 2, 0).wait_send()

        for c in range(1, last_chip):
            @pl.when(chip == c)
            def _():
                own_send(seq, 0, last_chip, c).wait_send()

                @pl.when(core == c - 1)
                def _():
                    forward(seq, 0, last_chip).wait_send()

        @pl.when(chip == last_chip)
        def _():
            forward(seq, 1, 2).wait_send()

        return carry

    lax.fori_loop(0, n_seq, drain, 0)


def solution(mesh):
    n_cp = mesh.shape['cp']

    def local_block(hidden, positions, norm_gain, w_query, w_key, w_value, w_out):
        batch, tokens, dim = hidden.shape
        kv_rows = 2 * w_key.shape[1]
        rows = batch * tokens
        chunks = rows // CHUNK
        chips = n_cp // 2
        x = hidden.reshape(rows, dim)
        inv_freq = 10000.0 ** (-2.0 * jnp.arange(HALF, dtype=F32) / HEAD)
        angles = positions.reshape(chunks, 1, CHUNK).astype(F32) * inv_freq[None, :, None]
        hbm = pl.BlockSpec(memory_space=pl.ANY)
        vmem = pl.BlockSpec(memory_space=pltpu.VMEM)
        dma = pltpu.SemaphoreType.DMA
        y, _ = pl.pallas_call(
            functools.partial(block_kernel, n_cp),
            out_shape=[jax.ShapeDtypeStruct((rows, dim), BF16), jax.ShapeDtypeStruct((batch, chips - 1, kv_rows, TOK), BF16)],
            in_specs=[hbm, vmem, hbm, hbm, hbm, hbm, vmem, vmem],
            out_specs=[hbm, hbm],
            scratch_shapes=[
                pltpu.VMEM((2, CHUNK, dim), BF16),
                pltpu.VMEM((rows, dim), BF16),
                pltpu.VMEM((2, dim, WBLOCK), BF16),
                pltpu.VMEM((kv_rows, dim), BF16),
                pltpu.VMEM((dim, dim), BF16),
                pltpu.VMEM((batch, kv_rows, TOK), BF16),
                pltpu.VMEM((batch, dim, TOK), BF16),
                pltpu.VMEM((2, n_cp, kv_rows, TOK), BF16),
                pltpu.VMEM((n_cp * TOK, GROUP * TOK), F32),
                pltpu.VMEM((8, GROUP * TOK), F32),
                pltpu.VMEM((2 * TOK, GROUP * TOK), F32),
                pltpu.VMEM((dim, TOK), BF16),
                pltpu.VMEM((2 * TOK, dim), BF16),
                pltpu.VMEM((2, 2 * TOK, dim), BF16),
                pltpu.VMEM((2, 2 * TOK, dim), BF16),
                dma((2,)), dma((2,)), dma, dma((batch, chips - 1)), dma((batch, 2)), dma((batch,)),
                dma((2, chips - 1)), dma((2, chips)), dma((2, chips)), dma((2,)), dma((2,)),
                pltpu.SemaphoreType.REGULAR,
            ],
            compiler_params=pltpu.CompilerParams(collective_id=0, has_side_effects=True, vmem_limit_bytes=62 * 2 ** 20),
            name='block',
        )(x, norm_gain.reshape(1, dim), w_query, w_key, w_value, w_out.reshape(dim, dim), jnp.cos(angles), jnp.sin(angles))
        return y.reshape(batch, tokens, dim)

    act_spec = P('dp', 'cp', None)
    return jax.shard_map(local_block, mesh=mesh, in_specs=(act_spec, P('dp', 'cp'), P(), P(), P(), P(), P()), out_specs=act_spec, check_vma=False)
```

```python
import functools

import jax
import jax.numpy as jnp
from jax import lax
from jax.experimental import pallas as pl
from jax.experimental.pallas import tpu as pltpu
from jax.sharding import PartitionSpec as P

MESH = pl.DeviceIdType.MESH
HEAD = 64
HALF = HEAD // 2
TOK = 128
GROUP = 4
AHEAD = 4
CHUNK = 4 * TOK
WBLOCK = 256
F32, BF16 = jnp.float32, jnp.bfloat16
NT = (((1,), (1,)), ((), ()))


def rope_rows(x, cos, sin):
    heads, n = x.shape[0] // HEAD, x.shape[1]
    x = x.reshape(heads, 2, HALF, n)
    a, b = x[:, 0], x[:, 1]
    rotated = jnp.stack([a * cos - b * sin, b * cos + a * sin], axis=1)
    return rotated.reshape(heads * HEAD, n)


def attend(q_ref, slot_ref, bias_ref, s_ref, m_ref, o_ref, seq, slot, n_blocks, between):
    width = slot_ref.shape[2] // 2
    pairs = width // (2 * HEAD)
    key_chunks = n_blocks // 2
    kc = 2 * TOK
    cols = GROUP * TOK

    def queries(g):
        base = g * GROUP * HEAD
        return jnp.concatenate([q_ref[seq, pl.ds(pl.multiple_of(base + i * HEAD, HEAD), HEAD), :] for i in range(GROUP)], axis=1)

    def scores(q, g, c, peak):
        row = pl.ds(pl.multiple_of(g * HEAD, HEAD), HEAD)
        keys = jnp.concatenate([slot_ref[slot, 2 * c + i, row, :].T for i in range(2)], axis=0)
        s = jnp.dot(keys, q, preferred_element_type=F32)
        if c == key_chunks - 1:
            s = s + bias_ref[...]
        s_ref[c * kc:(c + 1) * kc, :] = s
        top = jnp.max(s.reshape(kc // 8, 8, cols), axis=0)
        return top if peak is None else jnp.maximum(peak, top)

    def unit(g, g_next, peak):
        peak = jnp.max(peak, axis=0, keepdims=True)
        q_next = queries(g_next)
        vrow = pl.ds(pl.multiple_of(width + g * HEAD, HEAD), HEAD)
        total, out, peak_next = None, None, None
        for c in range(key_chunks):
            prob = jnp.exp(s_ref[c * kc:(c + 1) * kc, :] - peak)
            part = jnp.sum(prob.reshape(kc // 8, 8, cols), axis=0)
            total = part if total is None else total + part
            values = jnp.concatenate([slot_ref[slot, 2 * c + i, vrow, :] for i in range(2)], axis=1)
            term = jnp.dot(values, prob.astype(BF16), preferred_element_type=F32)
            out = term if out is None else out + term
            peak_next = scores(q_next, g_next, c, peak_next)
        out = out / jnp.sum(total, axis=0, keepdims=True)
        for i in range(GROUP):
            o_ref[pl.ds(pl.multiple_of((g * GROUP + i) * HEAD, HEAD), HEAD), :] = out[:, i * TOK:(i + 1) * TOK].astype(BF16)
        return peak_next

    q_first, peak = queries(0), None
    for c in range(key_chunks):
        peak = scores(q_first, 0, c, peak)
    m_ref[...] = peak

    def pair(j, carry):
        @pl.when(j == 1)
        def _():
            between()

        peak = unit(2 * j, 2 * j + 1, m_ref[...])
        m_ref[...] = unit(2 * j + 1, jnp.minimum(2 * j + 2, 2 * pairs - 1), peak)
        return carry

    lax.fori_loop(0, pairs, pair, 0)


def block_kernel(
    n_cp, x_hbm, gain_ref, wq_hbm, wk_hbm, wv_hbm, wo_hbm, cos_ref, sin_ref, y_hbm, kv_hbm,
    x_st, h_ref, w_st, wkv_ref, w_ref, kv_st, q_ref, slot_ref, s_ref, m_ref, bias_ref, ot_ref, o_ref, xr_ref, y_st, gain_row,
    x_sem, w_sem, wo_sem, recv_sem, own_sem, fwd_sem, load_sem, sib_recv, sib_send, xr_sem, y_sem, credit,
):
    me = lax.axis_index('cp')
    chip, core = me // 2, me % 2
    sibling = me + 1 - 2 * core
    n_seq = kv_st.shape[0]
    dim = x_st.shape[2]
    kv_rows = wkv_ref.shape[0]
    n_chunks = n_seq * TOK // CHUNK
    seqs = CHUNK // TOK
    last_chip = n_cp // 2 - 1

    barrier = pltpu.get_barrier_semaphore()
    for step in range(1, n_cp):
        pl.semaphore_signal(barrier, inc=1, device_id={'cp': (me + step) % n_cp}, device_id_type=MESH)

    def x_copy(chunk):
        return pltpu.make_async_copy(x_hbm.at[pl.ds(chunk * CHUNK, CHUNK), :], x_st.at[chunk % 2], x_sem.at[chunk % 2])

    def w_copy(hbm, block, slot):
        return pltpu.make_async_copy(hbm.at[:, pl.ds(block * WBLOCK, WBLOCK)], w_st.at[slot], w_sem.at[slot])

    kv_blocks = [(wk_hbm, i) for i in range(kv_rows // 2 // WBLOCK)] + [(wv_hbm, i) for i in range(kv_rows // 2 // WBLOCK)]
    q_blocks = dim // WBLOCK
    x_copy(0).start()
    for i in range(2):
        w_copy(*kv_blocks[i], i).start()
    x_copy(1).start()

    key = lax.broadcasted_iota(jnp.int32, (2 * TOK, TOK), 0)
    tok = lax.broadcasted_iota(jnp.int32, (2 * TOK, TOK), 1)
    bias = jnp.where(key <= tok + core * TOK, 0.0, -jnp.inf).astype(F32)
    bias_ref[...] = jnp.concatenate([bias] * GROUP, axis=1)

    gain = gain_ref[...].astype(F32)
    for i in range(gain.shape[0]):
        gain_row[:, i * gain.shape[1]:(i + 1) * gain.shape[1]] = gain[i:i + 1]

    def tables(chunk):
        return [jnp.concatenate([t[chunk * seqs + i] for i in range(seqs)], axis=1) for t in (cos_ref, sin_ref)]

    for i, (hbm, block) in enumerate(kv_blocks):
        w_copy(hbm, block, i % 2).wait()
        wkv_ref[i * WBLOCK:(i + 1) * WBLOCK, :] = w_st[i % 2].T
        nxt = i + 2
        if nxt < len(kv_blocks):
            w_copy(*kv_blocks[nxt], i % 2).start()
        else:
            w_copy(wq_hbm, nxt - len(kv_blocks), i % 2).start()

    def own_send(seq, target, to_chip, from_chip):
        return pltpu.make_async_remote_copy(
            src_ref=kv_st.at[seq], dst_ref=kv_hbm.at[seq, from_chip], send_sem=own_sem.at[seq, target],
            recv_sem=recv_sem.at[seq, from_chip], device_id={'cp': 2 * to_chip + core}, device_id_type=MESH)

    def forward(seq, block, to_chip):
        return pltpu.make_async_remote_copy(
            src_ref=kv_hbm.at[seq, block], dst_ref=kv_hbm.at[seq, block], send_sem=fwd_sem.at[seq],
            recv_sem=recv_sem.at[seq, block], device_id={'cp': 2 * to_chip + core}, device_id_type=MESH)

    def project_kv(chunk, carry):
        x_copy(chunk).wait()
        x = x_st[chunk % 2].astype(F32)
        inv_rms = lax.rsqrt(jnp.mean(x * x, axis=-1, keepdims=True) + 1e-5)
        rows = pl.ds(pl.multiple_of(chunk * CHUNK, CHUNK), CHUNK)
        h_ref[rows, :] = (x * inv_rms * gain_row[...]).astype(BF16)

        @pl.when(chunk + 2 < n_chunks)
        def _():
            x_copy(chunk + 2).start()

        kv = lax.dot_general(wkv_ref[...], h_ref[rows, :], NT, preferred_element_type=F32)
        k = rope_rows(kv[:kv_rows // 2], *tables(chunk)).astype(BF16)
        v = kv[kv_rows // 2:].astype(BF16)
        for i in range(seqs):
            kv_st[chunk * seqs + i, :kv_rows // 2, :] = k[:, i * TOK:(i + 1) * TOK]
            kv_st[chunk * seqs + i, kv_rows // 2:, :] = v[:, i * TOK:(i + 1) * TOK]

        @pl.when(chunk == 0)
        def _():
            pl.semaphore_wait(barrier, n_cp - 1)

        @pl.when(chip == 0)
        def _():
            for i in range(seqs):
                own_send(chunk * seqs + i, 0, 1, 0).start()
                own_send(chunk * seqs + i, 1, 2, 0).start()

        for c in range(1, last_chip):
            @pl.when((chip == c) & (chunk == 0))
            def _():
                for i in range(AHEAD):
                    own_send(i, 0, last_chip, c).start()

        return carry

    lax.fori_loop(0, n_chunks, project_kv, 0)

    def turn_wq(i, carry):
        for k in range(2):
            w_copy(wq_hbm, 2 * i + k, k).wait()
            w_ref[pl.ds(pl.multiple_of((2 * i + k) * WBLOCK, WBLOCK), WBLOCK), :] = w_st[k].T

            @pl.when(2 * i + k + 2 < q_blocks)
            def _():
                w_copy(wq_hbm, 2 * i + k + 2, k).start()

        return carry

    lax.fori_loop(0, q_blocks // 2, turn_wq, 0)

    def hop(seq):
        for c in range(1, last_chip):
            @pl.when(chip == c)
            def _():
                own_send(seq, 0, c, 0).wait_recv()

                @pl.when(core == c - 1)
                def _():
                    forward(seq, 0, last_chip).start()

                @pl.when(seq + AHEAD < n_seq)
                def _():
                    own_send(seq + AHEAD, 0, last_chip, c).start()

        @pl.when(chip == last_chip)
        def _():
            own_send(seq, 0, last_chip, 1).wait_recv()
            forward(seq, 1, 2).start()

    q_rows = dim // 2

    def project_q(i, carry):
        chunk, part = i // 2, i % 2
        base = pl.multiple_of(part * q_rows, q_rows)
        h = h_ref[pl.ds(pl.multiple_of(chunk * CHUNK, CHUNK), CHUNK), :]
        q = lax.dot_general(w_ref[pl.ds(base, q_rows), :], h, NT, preferred_element_type=F32)
        q = (rope_rows(q, *tables(chunk)) * (HEAD ** -0.5)).astype(BF16)
        for k in range(seqs):
            q_ref[chunk * seqs + k, pl.ds(base, q_rows), :] = q[:, k * TOK:(k + 1) * TOK]

        @pl.when(part == 1)
        def _():
            hop(chunk)

        return carry

    lax.fori_loop(0, 2 * n_chunks, project_q, 0)
    wo_copy = pltpu.make_async_copy(wo_hbm, w_ref, wo_sem)
    wo_copy.start()

    def xr_copy(p):
        return pltpu.make_async_copy(x_hbm.at[pl.ds(p * 2 * TOK, 2 * TOK), :], xr_ref.at[p % 2], xr_sem.at[p % 2])

    def y_copy(p):
        return pltpu.make_async_copy(y_st.at[p % 2], y_hbm.at[pl.ds(p * 2 * TOK, 2 * TOK), :], y_sem.at[p % 2])

    xr_copy(0).start()
    xr_copy(1).start()

    def load(seq, a):
        return pltpu.make_async_copy(kv_hbm.at[seq, a], slot_ref.at[seq % 2, 2 * a + core], load_sem.at[seq % 2, a])

    def share(seq, a, src):
        return pltpu.make_async_remote_copy(
            src_ref=src, dst_ref=slot_ref.at[seq % 2, 2 * a + core], send_sem=sib_send.at[seq % 2, a],
            recv_sem=sib_recv.at[seq % 2, a], device_id={'cp': sibling}, device_id_type=MESH)

    def stage(c, seq):
        @pl.when(seq >= 2)
        def _():
            pl.semaphore_wait(credit, 1)
            for a in range(c + 1):
                share(seq, a, kv_st.at[seq]).wait_send()

        share(seq, c, kv_st.at[seq]).start()
        slot_ref[seq % 2, 2 * c + core] = kv_st[seq]
        hopped = 1 if c == last_chip else 0
        for a in [hopped] + [a for a in range(c) if a != hopped] if c else []:
            if a != hopped:
                own_send(seq, 0, c, a).wait_recv()
            share(seq, a, kv_hbm.at[seq, a]).start()
            load(seq, a).start()

    for c in range(last_chip + 1):
        @pl.when(chip == c)
        def _():
            stage(c, 0)

    def project_out(p):
        @pl.when(p == 0)
        def _():
            wo_copy.wait()

        xr_copy(p).wait()

        @pl.when(p >= 2)
        def _():
            y_copy(p - 2).wait()

        step = 512
        for col in range(0, dim, step):
            proj = jnp.dot(o_ref[...], w_ref[:, col:col + step], preferred_element_type=F32)
            y_st[p % 2, :, col:col + step] = (xr_ref[p % 2, :, col:col + step].astype(F32) + proj).astype(BF16)
        y_copy(p).start()

        @pl.when(p + 2 < n_seq // 2)
        def _():
            xr_copy(p + 2).start()

    def sequence(seq, carry):
        for c in range(last_chip + 1):
            @pl.when(chip == c)
            def _():
                for a in range(c):
                    load(seq, a).wait()
                for a in range(c + 1):
                    share(seq, a, kv_st.at[seq]).wait_recv()

                def between():
                    @pl.when(seq + 1 < n_seq)
                    def _():
                        stage(c, seq + 1)

                    if c:
                        @pl.when(seq + AHEAD < n_seq)
                        def _():
                            hop(seq + AHEAD)

                attend(q_ref, slot_ref, bias_ref, s_ref, m_ref, ot_ref, seq, seq % 2, 2 * (c + 1), between)

        @pl.when(seq + 2 < n_seq)
        def _():
            pl.semaphore_signal(credit, inc=1, device_id={'cp': sibling}, device_id_type=MESH)

        o_ref[pl.ds(pl.multiple_of(seq % 2 * TOK, TOK), TOK), :] = ot_ref[...].T

        @pl.when(seq % 2 == 1)
        def _():
            project_out(seq // 2)

        return carry

    lax.fori_loop(0, n_seq, sequence, 0)

    for p in (n_seq // 2 - 2, n_seq // 2 - 1):
        y_copy(p).wait()
    for c in range(last_chip + 1):
        @pl.when(chip == c)
        def _():
            for seq in (n_seq - 2, n_seq - 1):
                for a in range(c + 1):
                    share(seq, a, kv_st.at[seq]).wait_send()

    def drain(seq, carry):
        @pl.when(chip == 0)
        def _():
            own_send(seq, 0, 1, 0).wait_send()
            own_send(seq, 1, 2, 0).wait_send()

        for c in range(1, last_chip):
            @pl.when(chip == c)
            def _():
                own_send(seq, 0, last_chip, c).wait_send()

                @pl.when(core == c - 1)
                def _():
                    forward(seq, 0, last_chip).wait_send()

        @pl.when(chip == last_chip)
        def _():
            forward(seq, 1, 2).wait_send()

        return carry

    lax.fori_loop(0, n_seq, drain, 0)


def solution(mesh):
    n_cp = mesh.shape['cp']

    def local_block(hidden, positions, norm_gain, w_query, w_key, w_value, w_out):
        batch, tokens, dim = hidden.shape
        kv_rows = 2 * w_key.shape[1]
        rows = batch * tokens
        chips = n_cp // 2
        x = hidden.reshape(rows, dim)
        inv_freq = 10000.0 ** (-2.0 * jnp.arange(HALF, dtype=F32) / HEAD)
        angles = positions.reshape(batch, 1, tokens).astype(F32) * inv_freq[None, :, None]
        hbm = pl.BlockSpec(memory_space=pl.ANY)
        vmem = pl.BlockSpec(memory_space=pltpu.VMEM)
        dma = pltpu.SemaphoreType.DMA
        y, _ = pl.pallas_call(
            functools.partial(block_kernel, n_cp),
            out_shape=[jax.ShapeDtypeStruct((rows, dim), BF16), jax.ShapeDtypeStruct((batch, chips - 1, kv_rows, TOK), BF16)],
            in_specs=[hbm, vmem, hbm, hbm, hbm, hbm, vmem, vmem],
            out_specs=[hbm, hbm],
            scratch_shapes=[
                pltpu.VMEM((2, CHUNK, dim), BF16),
                pltpu.VMEM((rows, dim), BF16),
                pltpu.VMEM((2, dim, WBLOCK), BF16),
                pltpu.VMEM((kv_rows, dim), BF16),
                pltpu.VMEM((dim, dim), BF16),
                pltpu.VMEM((batch, kv_rows, TOK), BF16),
                pltpu.VMEM((batch, dim, TOK), BF16),
                pltpu.VMEM((2, n_cp, kv_rows, TOK), BF16),
                pltpu.VMEM((n_cp * TOK, GROUP * TOK), F32),
                pltpu.VMEM((8, GROUP * TOK), F32),
                pltpu.VMEM((2 * TOK, GROUP * TOK), F32),
                pltpu.VMEM((dim, TOK), BF16),
                pltpu.VMEM((2 * TOK, dim), BF16),
                pltpu.VMEM((2, 2 * TOK, dim), BF16),
                pltpu.VMEM((2, 2 * TOK, dim), BF16),
                pltpu.VMEM((1, dim), F32),
                dma((2,)), dma((2,)), dma, dma((batch, chips - 1)), dma((batch, 2)), dma((batch,)),
                dma((2, chips - 1)), dma((2, chips)), dma((2, chips)), dma((2,)), dma((2,)),
                pltpu.SemaphoreType.REGULAR,
            ],
            compiler_params=pltpu.CompilerParams(collective_id=0, has_side_effects=True, vmem_limit_bytes=62 * 2 ** 20),
            name='block',
        )(x, norm_gain.reshape(dim // 128, 128), w_query, w_key, w_value, w_out.reshape(dim, dim), jnp.cos(angles), jnp.sin(angles))
        return y.reshape(batch, tokens, dim)

    act_spec = P('dp', 'cp', None)
    return jax.shard_map(local_block, mesh=mesh, in_specs=(act_spec, P('dp', 'cp'), P(), P(), P(), P(), P()), out_specs=act_spec, check_vma=False)
```

```python
import functools

import jax
import jax.numpy as jnp
from jax import lax
from jax.experimental import pallas as pl
from jax.experimental.pallas import tpu as pltpu
from jax.sharding import PartitionSpec as P

MESH = pl.DeviceIdType.MESH
HEAD = 64
HALF = HEAD // 2
TOK = 128
GROUP = 4
AHEAD = 4
LEAD = 2
CHUNK = 4 * TOK
WBLOCK = 256
F32, BF16 = jnp.float32, jnp.bfloat16
NT = (((1,), (1,)), ((), ()))


def rope_rows(x, cos, sin):
    heads, n = x.shape[0] // HEAD, x.shape[1]
    x = x.reshape(heads, 2, HALF, n)
    a, b = x[:, 0], x[:, 1]
    rotated = jnp.stack([a * cos - b * sin, b * cos + a * sin], axis=1)
    return rotated.reshape(heads * HEAD, n)


def attend(q_ref, slot_ref, bias_ref, s_ref, m_ref, o_ref, seq, n_seq, n_blocks, stage_next, wait_next):
    width = slot_ref.shape[2] // 2
    pairs = width // (2 * HEAD)
    key_chunks = n_blocks // 2
    kc = 2 * TOK
    cols = GROUP * TOK

    def queries(sq, g):
        base = g * GROUP * HEAD
        return jnp.concatenate([q_ref[sq, pl.ds(pl.multiple_of(base + i * HEAD, HEAD), HEAD), :] for i in range(GROUP)], axis=1)

    def scores(q, sq, g, c, peak):
        row = pl.ds(pl.multiple_of(g * HEAD, HEAD), HEAD)
        keys = jnp.concatenate([slot_ref[sq % 2, 2 * c + i, row, :].T for i in range(2)], axis=0)
        s = jnp.dot(keys, q, preferred_element_type=F32)
        if c == key_chunks - 1:
            s = s + bias_ref[...]
        s_ref[c * kc:(c + 1) * kc, :] = s
        top = jnp.max(s.reshape(kc // 8, 8, cols), axis=0)
        return top if peak is None else jnp.maximum(peak, top)

    def unit(g, sq_next, g_next, peak):
        peak = jnp.max(peak, axis=0, keepdims=True)
        q_next = queries(sq_next, g_next)
        vrow = pl.ds(pl.multiple_of(width + g * HEAD, HEAD), HEAD)
        total, out, peak_next = None, None, None
        for c in range(key_chunks):
            prob = jnp.exp(s_ref[c * kc:(c + 1) * kc, :] - peak)
            part = jnp.sum(prob.reshape(kc // 8, 8, cols), axis=0)
            total = part if total is None else total + part
            values = jnp.concatenate([slot_ref[seq % 2, 2 * c + i, vrow, :] for i in range(2)], axis=1)
            term = jnp.dot(values, prob.astype(BF16), preferred_element_type=F32)
            out = term if out is None else out + term
            peak_next = scores(q_next, sq_next, g_next, c, peak_next)
        out = out / jnp.sum(total, axis=0, keepdims=True)
        for i in range(GROUP):
            o_ref[pl.ds(pl.multiple_of((g * GROUP + i) * HEAD, HEAD), HEAD), :] = out[:, i * TOK:(i + 1) * TOK].astype(BF16)
        return peak_next

    @pl.when(seq == 0)
    def _():
        q_first, peak = queries(seq, 0), None
        for c in range(key_chunks):
            peak = scores(q_first, seq, 0, c, peak)
        m_ref[...] = peak

    def pair(j, carry):
        @pl.when(j == 1)
        def _():
            stage_next()

        last = j == pairs - 1

        @pl.when(last)
        def _():
            wait_next()

        sq_next = jnp.where(last, jnp.minimum(seq + 1, n_seq - 1), seq)
        g_next = jnp.where(last, 0, 2 * j + 2)
        peak = unit(2 * j, seq, 2 * j + 1, m_ref[...])
        m_ref[...] = unit(2 * j + 1, sq_next, g_next, peak)
        return carry

    lax.fori_loop(0, pairs, pair, 0)


def block_kernel(
    n_cp, x_hbm, gain_ref, wq_hbm, wk_hbm, wv_hbm, wo_hbm, cos_ref, sin_ref, y_hbm, kv_hbm,
    x_st, h_ref, w_st, wkv_ref, w_ref, kv_st, q_ref, slot_ref, s_ref, m_ref, bias_ref, ot_ref, o_ref, xr_ref, y_st, gain_row,
    x_sem, w_sem, wo_sem, recv_sem, own_sem, fwd_sem, load_sem, sib_recv, sib_send, xr_sem, y_sem, credit,
):
    me = lax.axis_index('cp')
    chip, core = me // 2, me % 2
    sibling = me + 1 - 2 * core
    n_seq = kv_st.shape[0]
    dim = x_st.shape[2]
    kv_rows = wkv_ref.shape[0]
    n_chunks = n_seq * TOK // CHUNK
    seqs = CHUNK // TOK
    last_chip = n_cp // 2 - 1

    barrier = pltpu.get_barrier_semaphore()
    for step in range(1, n_cp):
        pl.semaphore_signal(barrier, inc=1, device_id={'cp': (me + step) % n_cp}, device_id_type=MESH)

    def x_copy(chunk):
        return pltpu.make_async_copy(x_hbm.at[pl.ds(chunk * CHUNK, CHUNK), :], x_st.at[chunk % 2], x_sem.at[chunk % 2])

    def w_copy(hbm, block, slot):
        return pltpu.make_async_copy(hbm.at[:, pl.ds(block * WBLOCK, WBLOCK)], w_st.at[slot], w_sem.at[slot])

    kv_blocks = [(wk_hbm, i) for i in range(kv_rows // 2 // WBLOCK)] + [(wv_hbm, i) for i in range(kv_rows // 2 // WBLOCK)]
    q_blocks = dim // WBLOCK
    x_copy(0).start()
    for i in range(2):
        w_copy(*kv_blocks[i], i).start()
    x_copy(1).start()

    key = lax.broadcasted_iota(jnp.int32, (2 * TOK, TOK), 0)
    tok = lax.broadcasted_iota(jnp.int32, (2 * TOK, TOK), 1)
    bias = jnp.where(key <= tok + core * TOK, 0.0, -jnp.inf).astype(F32)
    bias_ref[...] = jnp.concatenate([bias] * GROUP, axis=1)

    gain = gain_ref[...].astype(F32)
    for i in range(gain.shape[0]):
        gain_row[:, i * gain.shape[1]:(i + 1) * gain.shape[1]] = gain[i:i + 1]

    def tables(chunk):
        return [jnp.concatenate([t[chunk * seqs + i] for i in range(seqs)], axis=1) for t in (cos_ref, sin_ref)]

    for i, (hbm, block) in enumerate(kv_blocks):
        w_copy(hbm, block, i % 2).wait()
        wkv_ref[i * WBLOCK:(i + 1) * WBLOCK, :] = w_st[i % 2].T
        nxt = i + 2
        if nxt < len(kv_blocks):
            w_copy(*kv_blocks[nxt], i % 2).start()
        else:
            w_copy(wq_hbm, nxt - len(kv_blocks), i % 2).start()

    def own_send(seq, target, to_chip, from_chip):
        return pltpu.make_async_remote_copy(
            src_ref=kv_st.at[seq], dst_ref=kv_hbm.at[seq, from_chip], send_sem=own_sem.at[seq, target],
            recv_sem=recv_sem.at[seq, from_chip], device_id={'cp': 2 * to_chip + core}, device_id_type=MESH)

    def forward(seq, block, to_chip):
        return pltpu.make_async_remote_copy(
            src_ref=kv_hbm.at[seq, block], dst_ref=kv_hbm.at[seq, block], send_sem=fwd_sem.at[seq],
            recv_sem=recv_sem.at[seq, block], device_id={'cp': 2 * to_chip + core}, device_id_type=MESH)

    def project_kv(chunk, carry):
        x_copy(chunk).wait()
        x = x_st[chunk % 2].astype(F32)
        inv_rms = lax.rsqrt(jnp.mean(x * x, axis=-1, keepdims=True) + 1e-5)
        rows = pl.ds(pl.multiple_of(chunk * CHUNK, CHUNK), CHUNK)
        h_ref[rows, :] = (x * inv_rms * gain_row[...]).astype(BF16)

        @pl.when(chunk + 2 < n_chunks)
        def _():
            x_copy(chunk + 2).start()

        kv = lax.dot_general(wkv_ref[...], h_ref[rows, :], NT, preferred_element_type=F32)
        k = rope_rows(kv[:kv_rows // 2], *tables(chunk)).astype(BF16)
        v = kv[kv_rows // 2:].astype(BF16)
        for i in range(seqs):
            kv_st[chunk * seqs + i, :kv_rows // 2, :] = k[:, i * TOK:(i + 1) * TOK]
            kv_st[chunk * seqs + i, kv_rows // 2:, :] = v[:, i * TOK:(i + 1) * TOK]

        @pl.when(chunk == 0)
        def _():
            pl.semaphore_wait(barrier, n_cp - 1)

        @pl.when(chip == 0)
        def _():
            for i in range(seqs):
                own_send(chunk * seqs + i, 0, 1, 0).start()
                own_send(chunk * seqs + i, 1, 2, 0).start()

        for c in range(1, last_chip):
            @pl.when((chip == c) & (chunk == 0))
            def _():
                for i in range(AHEAD):
                    own_send(i, 0, last_chip, c).start()

        return carry

    lax.fori_loop(0, n_chunks, project_kv, 0)

    def turn_wq(i, carry):
        for k in range(2):
            w_copy(wq_hbm, 2 * i + k, k).wait()
            w_ref[pl.ds(pl.multiple_of((2 * i + k) * WBLOCK, WBLOCK), WBLOCK), :] = w_st[k].T

            @pl.when(2 * i + k + 2 < q_blocks)
            def _():
                w_copy(wq_hbm, 2 * i + k + 2, k).start()

        return carry

    lax.fori_loop(0, q_blocks // 2, turn_wq, 0)

    def hop(seq):
        for c in range(1, last_chip):
            @pl.when(chip == c)
            def _():
                own_send(seq, 0, c, 0).wait_recv()

                @pl.when(core == c - 1)
                def _():
                    forward(seq, 0, last_chip).start()

                @pl.when((seq + LEAD >= AHEAD) & (seq + LEAD < n_seq))
                def _():
                    own_send(seq + LEAD, 0, last_chip, c).start()

        @pl.when(chip == last_chip)
        def _():
            own_send(seq, 0, last_chip, 1).wait_recv()
            forward(seq, 1, 2).start()

    q_rows = dim // 2

    def project_q(i, carry):
        chunk, part = i // 2, i % 2
        base = pl.multiple_of(part * q_rows, q_rows)
        h = h_ref[pl.ds(pl.multiple_of(chunk * CHUNK, CHUNK), CHUNK), :]
        q = lax.dot_general(w_ref[pl.ds(base, q_rows), :], h, NT, preferred_element_type=F32)
        q = (rope_rows(q, *tables(chunk)) * (HEAD ** -0.5)).astype(BF16)
        for k in range(seqs):
            q_ref[chunk * seqs + k, pl.ds(base, q_rows), :] = q[:, k * TOK:(k + 1) * TOK]

        @pl.when((part == 1) & ((chip < last_chip) | (chunk < LEAD)))
        def _():
            hop(chunk)

        return carry

    lax.fori_loop(0, 2 * n_chunks, project_q, 0)
    wo_copy = pltpu.make_async_copy(wo_hbm, w_ref, wo_sem)
    wo_copy.start()

    def xr_copy(p):
        return pltpu.make_async_copy(x_hbm.at[pl.ds(p * 2 * TOK, 2 * TOK), :], xr_ref.at[p % 2], xr_sem.at[p % 2])

    def y_copy(p):
        return pltpu.make_async_copy(y_st.at[p % 2], y_hbm.at[pl.ds(p * 2 * TOK, 2 * TOK), :], y_sem.at[p % 2])

    xr_copy(0).start()
    xr_copy(1).start()

    def load(seq, a):
        return pltpu.make_async_copy(kv_hbm.at[seq, a], slot_ref.at[seq % 2, 2 * a + core], load_sem.at[seq % 2, a])

    def share(seq, a, src):
        return pltpu.make_async_remote_copy(
            src_ref=src, dst_ref=slot_ref.at[seq % 2, 2 * a + core], send_sem=sib_send.at[seq % 2, a],
            recv_sem=sib_recv.at[seq % 2, a], device_id={'cp': sibling}, device_id_type=MESH)

    def stage(c, seq):
        @pl.when(seq >= 2)
        def _():
            pl.semaphore_wait(credit, 1)
            for a in range(c + 1):
                share(seq, a, kv_st.at[seq]).wait_send()

        share(seq, c, kv_st.at[seq]).start()
        slot_ref[seq % 2, 2 * c + core] = kv_st[seq]
        hopped = 1 if c == last_chip else 0
        for a in [hopped] + [a for a in range(c) if a != hopped] if c else []:
            if a != hopped:
                own_send(seq, 0, c, a).wait_recv()
            share(seq, a, kv_hbm.at[seq, a]).start()
            load(seq, a).start()

    for c in range(last_chip + 1):
        @pl.when(chip == c)
        def _():
            stage(c, 0)

    def project_out(p):
        @pl.when(p == 0)
        def _():
            wo_copy.wait()

        xr_copy(p).wait()

        @pl.when(p >= 2)
        def _():
            y_copy(p - 2).wait()

        step = 512
        for col in range(0, dim, step):
            proj = jnp.dot(o_ref[...], w_ref[:, col:col + step], preferred_element_type=F32)
            y_st[p % 2, :, col:col + step] = (xr_ref[p % 2, :, col:col + step].astype(F32) + proj).astype(BF16)
        y_copy(p).start()

        @pl.when(p + 2 < n_seq // 2)
        def _():
            xr_copy(p + 2).start()

    def sequence(seq, carry):
        for c in range(last_chip + 1):
            @pl.when(chip == c)
            def _():
                def arrived(sq):
                    for a in range(c):
                        load(sq, a).wait()
                    for a in range(c + 1):
                        share(sq, a, kv_st.at[sq]).wait_recv()

                @pl.when(seq == 0)
                def _():
                    arrived(seq)

                def stage_next():
                    @pl.when(seq + 1 < n_seq)
                    def _():
                        stage(c, seq + 1)

                    if c:
                        ahead = LEAD if c == last_chip else AHEAD

                        @pl.when(seq + ahead < n_seq)
                        def _():
                            hop(seq + ahead)

                def wait_next():
                    @pl.when(seq + 1 < n_seq)
                    def _():
                        arrived(seq + 1)

                attend(q_ref, slot_ref, bias_ref, s_ref, m_ref, ot_ref, seq, n_seq, 2 * (c + 1), stage_next, wait_next)

        @pl.when(seq + 2 < n_seq)
        def _():
            pl.semaphore_signal(credit, inc=1, device_id={'cp': sibling}, device_id_type=MESH)

        o_ref[pl.ds(pl.multiple_of(seq % 2 * TOK, TOK), TOK), :] = ot_ref[...].T

        @pl.when(seq % 2 == 1)
        def _():
            project_out(seq // 2)

        return carry

    lax.fori_loop(0, n_seq, sequence, 0)

    for p in (n_seq // 2 - 2, n_seq // 2 - 1):
        y_copy(p).wait()
    for c in range(last_chip + 1):
        @pl.when(chip == c)
        def _():
            for seq in (n_seq - 2, n_seq - 1):
                for a in range(c + 1):
                    share(seq, a, kv_st.at[seq]).wait_send()

    def drain(seq, carry):
        @pl.when(chip == 0)
        def _():
            own_send(seq, 0, 1, 0).wait_send()
            own_send(seq, 1, 2, 0).wait_send()

        for c in range(1, last_chip):
            @pl.when(chip == c)
            def _():
                own_send(seq, 0, last_chip, c).wait_send()

                @pl.when(core == c - 1)
                def _():
                    forward(seq, 0, last_chip).wait_send()

        @pl.when(chip == last_chip)
        def _():
            forward(seq, 1, 2).wait_send()

        return carry

    lax.fori_loop(0, n_seq, drain, 0)


def solution(mesh):
    n_cp = mesh.shape['cp']

    def local_block(hidden, positions, norm_gain, w_query, w_key, w_value, w_out):
        batch, tokens, dim = hidden.shape
        kv_rows = 2 * w_key.shape[1]
        rows = batch * tokens
        chips = n_cp // 2
        x = hidden.reshape(rows, dim)
        inv_freq = 10000.0 ** (-2.0 * jnp.arange(HALF, dtype=F32) / HEAD)
        angles = positions.reshape(batch, 1, tokens).astype(F32) * inv_freq[None, :, None]
        hbm = pl.BlockSpec(memory_space=pl.ANY)
        vmem = pl.BlockSpec(memory_space=pltpu.VMEM)
        dma = pltpu.SemaphoreType.DMA
        y, _ = pl.pallas_call(
            functools.partial(block_kernel, n_cp),
            out_shape=[jax.ShapeDtypeStruct((rows, dim), BF16), jax.ShapeDtypeStruct((batch, chips - 1, kv_rows, TOK), BF16)],
            in_specs=[hbm, vmem, hbm, hbm, hbm, hbm, vmem, vmem],
            out_specs=[hbm, hbm],
            scratch_shapes=[
                pltpu.VMEM((2, CHUNK, dim), BF16),
                pltpu.VMEM((rows, dim), BF16),
                pltpu.VMEM((2, dim, WBLOCK), BF16),
                pltpu.VMEM((kv_rows, dim), BF16),
                pltpu.VMEM((dim, dim), BF16),
                pltpu.VMEM((batch, kv_rows, TOK), BF16),
                pltpu.VMEM((batch, dim, TOK), BF16),
                pltpu.VMEM((2, n_cp, kv_rows, TOK), BF16),
                pltpu.VMEM((n_cp * TOK, GROUP * TOK), F32),
                pltpu.VMEM((8, GROUP * TOK), F32),
                pltpu.VMEM((2 * TOK, GROUP * TOK), F32),
                pltpu.VMEM((dim, TOK), BF16),
                pltpu.VMEM((2 * TOK, dim), BF16),
                pltpu.VMEM((2, 2 * TOK, dim), BF16),
                pltpu.VMEM((2, 2 * TOK, dim), BF16),
                pltpu.VMEM((1, dim), F32),
                dma((2,)), dma((2,)), dma, dma((batch, chips - 1)), dma((batch, 2)), dma((batch,)),
                dma((2, chips - 1)), dma((2, chips)), dma((2, chips)), dma((2,)), dma((2,)),
                pltpu.SemaphoreType.REGULAR,
            ],
            compiler_params=pltpu.CompilerParams(collective_id=0, has_side_effects=True, vmem_limit_bytes=62 * 2 ** 20),
            name='block',
        )(x, norm_gain.reshape(dim // 128, 128), w_query, w_key, w_value, w_out.reshape(dim, dim), jnp.cos(angles), jnp.sin(angles))
        return y.reshape(batch, tokens, dim)

    act_spec = P('dp', 'cp', None)
    return jax.shard_map(local_block, mesh=mesh, in_specs=(act_spec, P('dp', 'cp'), P(), P(), P(), P(), P()), out_specs=act_spec, check_vma=False)
```

```python
import functools

import jax
import jax.numpy as jnp
from jax import lax
from jax.experimental import pallas as pl
from jax.experimental.pallas import tpu as pltpu
from jax.sharding import PartitionSpec as P

MESH = pl.DeviceIdType.MESH
HEAD = 64
HALF = HEAD // 2
TOK = 128
GROUP = 4
AHEAD = 4
LEAD = 2
GUESTS = 2
CHUNK = 4 * TOK
WBLOCK = 256
F32, BF16 = jnp.float32, jnp.bfloat16
NT = (((1,), (1,)), ((), ()))


def rope_rows(x, cos, sin):
    heads, n = x.shape[0] // HEAD, x.shape[1]
    x = x.reshape(heads, 2, HALF, n)
    a, b = x[:, 0], x[:, 1]
    rotated = jnp.stack([a * cos - b * sin, b * cos + a * sin], axis=1)
    return rotated.reshape(heads * HEAD, n)


def attend(q_ref, slot_ref, bias_ref, s_ref, m_ref, o_ref, seq, following, first, n_blocks, stage_next, wait_next):
    width = slot_ref.shape[2] // 2
    pairs = width // (2 * HEAD)
    key_chunks = n_blocks // 2
    kc = 2 * TOK
    cols = GROUP * TOK

    def queries(sq, g):
        base = g * GROUP * HEAD
        return jnp.concatenate([q_ref[sq, pl.ds(pl.multiple_of(base + i * HEAD, HEAD), HEAD), :] for i in range(GROUP)], axis=1)

    def scores(q, sq, g, c, peak):
        row = pl.ds(pl.multiple_of(g * HEAD, HEAD), HEAD)
        keys = jnp.concatenate([slot_ref[sq % 2, 2 * c + i, row, :].T for i in range(2)], axis=0)
        s = jnp.dot(keys, q, preferred_element_type=F32)
        if c == key_chunks - 1:
            s = s + bias_ref[...]
        s_ref[c * kc:(c + 1) * kc, :] = s
        top = jnp.max(s.reshape(kc // 8, 8, cols), axis=0)
        return top if peak is None else jnp.maximum(peak, top)

    def unit(g, sq_next, g_next, peak):
        peak = jnp.max(peak, axis=0, keepdims=True)
        q_next = queries(sq_next, g_next)
        vrow = pl.ds(pl.multiple_of(width + g * HEAD, HEAD), HEAD)
        total, out, peak_next = None, None, None
        for c in range(key_chunks):
            prob = jnp.exp(s_ref[c * kc:(c + 1) * kc, :] - peak)
            part = jnp.sum(prob.reshape(kc // 8, 8, cols), axis=0)
            total = part if total is None else total + part
            values = jnp.concatenate([slot_ref[seq % 2, 2 * c + i, vrow, :] for i in range(2)], axis=1)
            term = jnp.dot(values, prob.astype(BF16), preferred_element_type=F32)
            out = term if out is None else out + term
            peak_next = scores(q_next, sq_next, g_next, c, peak_next)
        out = out / jnp.sum(total, axis=0, keepdims=True)
        for i in range(GROUP):
            o_ref[pl.ds(pl.multiple_of((g * GROUP + i) * HEAD, HEAD), HEAD), :] = out[:, i * TOK:(i + 1) * TOK].astype(BF16)
        return peak_next

    @pl.when(first)
    def _():
        q_first, peak = queries(seq, 0), None
        for c in range(key_chunks):
            peak = scores(q_first, seq, 0, c, peak)
        m_ref[...] = peak

    def pair(j, carry):
        @pl.when(j == 1)
        def _():
            stage_next()

        last = j == pairs - 1

        @pl.when(last)
        def _():
            wait_next()

        sq_next = jnp.where(last, following, seq)
        g_next = jnp.where(last, 0, 2 * j + 2)
        peak = unit(2 * j, seq, 2 * j + 1, m_ref[...])
        m_ref[...] = unit(2 * j + 1, sq_next, g_next, peak)
        return carry

    lax.fori_loop(0, pairs, pair, 0)


def block_kernel(
    n_cp, x_hbm, gain_ref, wq_hbm, wk_hbm, wv_hbm, wo_hbm, cos_ref, sin_ref, y_hbm, kv_hbm, gx_hbm,
    x_st, h_ref, w_st, wkv_ref, w_ref, kv_st, q_ref, slot_ref, s_ref, m_ref, bias_ref, ot_ref, o_ref, xr_ref, y_st, gain_row, gtab,
    x_sem, w_sem, wo_sem, recv_sem, own_sem, fwd_sem, load_sem, sib_recv, sib_send, xr_sem, y_sem, gx_sem, gt_sem, gy_sem, credit,
):
    me = lax.axis_index('cp')
    chip, core = me // 2, me % 2
    sibling = me + 1 - 2 * core
    n_seq = cos_ref.shape[0]
    kept = n_seq - GUESTS
    guest_rows = GUESTS * TOK
    dim = x_st.shape[2]
    kv_rows = wkv_ref.shape[0]
    n_chunks = n_seq * TOK // CHUNK
    seqs = CHUNK // TOK
    last_chip = n_cp // 2 - 1

    barrier = pltpu.get_barrier_semaphore()
    for step in range(1, n_cp):
        pl.semaphore_signal(barrier, inc=1, device_id={'cp': (me + step) % n_cp}, device_id_type=MESH)

    def x_copy(chunk):
        return pltpu.make_async_copy(x_hbm.at[pl.ds(chunk * CHUNK, CHUNK), :], x_st.at[chunk % 2], x_sem.at[chunk % 2])

    def w_copy(hbm, block, slot):
        return pltpu.make_async_copy(hbm.at[:, pl.ds(block * WBLOCK, WBLOCK)], w_st.at[slot], w_sem.at[slot])

    kv_blocks = [(wk_hbm, i) for i in range(kv_rows // 2 // WBLOCK)] + [(wv_hbm, i) for i in range(kv_rows // 2 // WBLOCK)]
    q_blocks = dim // WBLOCK
    x_copy(0).start()
    for i in range(2):
        w_copy(*kv_blocks[i], i).start()
    x_copy(1).start()

    key = lax.broadcasted_iota(jnp.int32, (2 * TOK, TOK), 0)
    tok = lax.broadcasted_iota(jnp.int32, (2 * TOK, TOK), 1)
    bias = jnp.where(key <= tok + core * TOK, 0.0, -jnp.inf).astype(F32)
    bias_ref[...] = jnp.concatenate([bias] * GROUP, axis=1)

    gain = gain_ref[...].astype(F32)
    for i in range(gain.shape[0]):
        gain_row[:, i * gain.shape[1]:(i + 1) * gain.shape[1]] = gain[i:i + 1]

    def tables(chunk):
        return [jnp.concatenate([t[chunk * seqs + i] for i in range(seqs)], axis=1) for t in (cos_ref, sin_ref)]

    for i, (hbm, block) in enumerate(kv_blocks):
        w_copy(hbm, block, i % 2).wait()
        wkv_ref[i * WBLOCK:(i + 1) * WBLOCK, :] = w_st[i % 2].T
        nxt = i + 2
        if nxt < len(kv_blocks):
            w_copy(*kv_blocks[nxt], i % 2).start()
        else:
            w_copy(wq_hbm, nxt - len(kv_blocks), i % 2).start()

    def own_send(seq, target, to_chip, from_chip):
        return pltpu.make_async_remote_copy(
            src_ref=kv_st.at[seq], dst_ref=kv_hbm.at[seq, from_chip], send_sem=own_sem.at[seq, target],
            recv_sem=recv_sem.at[seq, from_chip], device_id={'cp': 2 * to_chip + core}, device_id_type=MESH)

    def forward(seq, block, to_chip):
        return pltpu.make_async_remote_copy(
            src_ref=kv_hbm.at[seq, block], dst_ref=kv_hbm.at[seq, block], send_sem=fwd_sem.at[seq],
            recv_sem=recv_sem.at[seq, block], device_id={'cp': 2 * to_chip + core}, device_id_type=MESH)

    def to_host(src, dst, sems, k):
        return pltpu.make_async_remote_copy(
            src_ref=src, dst_ref=dst, send_sem=sems.at[0, k], recv_sem=sems.at[1, k], device_id={'cp': core}, device_id_type=MESH)

    host_copies = [
        to_host(cos_ref.at[pl.ds(kept, GUESTS)], gtab.at[0], gt_sem, 0),
        to_host(sin_ref.at[pl.ds(kept, GUESTS)], gtab.at[1], gt_sem, 1),
        to_host(x_hbm.at[pl.ds(kept * TOK, guest_rows), :], gx_hbm, gx_sem, 0),
    ]
    pl.semaphore_wait(barrier, n_cp - 1)

    @pl.when(chip == last_chip)
    def _():
        for copy in host_copies:
            copy.start()

    def normed(x):
        x = x.astype(F32)
        inv_rms = lax.rsqrt(jnp.mean(x * x, axis=-1, keepdims=True) + 1e-5)
        return (x * inv_rms * gain_row[...]).astype(BF16)

    def keep_kv(h, cos, sin, first):
        kv = lax.dot_general(wkv_ref[...], h, NT, preferred_element_type=F32)
        k = rope_rows(kv[:kv_rows // 2], cos, sin).astype(BF16)
        v = kv[kv_rows // 2:].astype(BF16)
        for i in range(h.shape[0] // TOK):
            kv_st[first + i, :kv_rows // 2, :] = k[:, i * TOK:(i + 1) * TOK]
            kv_st[first + i, kv_rows // 2:, :] = v[:, i * TOK:(i + 1) * TOK]

    def keep_q(h, cos, sin, first, base):
        q = lax.dot_general(w_ref[pl.ds(base, q_rows), :], h, NT, preferred_element_type=F32)
        q = (rope_rows(q, cos, sin) * (HEAD ** -0.5)).astype(BF16)
        for i in range(h.shape[0] // TOK):
            q_ref[first + i, pl.ds(base, q_rows), :] = q[:, i * TOK:(i + 1) * TOK]

    q_rows = dim // 2

    def project_kv(chunk, carry):
        x_copy(chunk).wait()
        rows = pl.ds(pl.multiple_of(chunk * CHUNK, CHUNK), CHUNK)
        h_ref[rows, :] = normed(x_st[chunk % 2])

        @pl.when(chunk + 2 < n_chunks)
        def _():
            x_copy(chunk + 2).start()

        keep_kv(h_ref[rows, :], *tables(chunk), chunk * seqs)

        @pl.when(chip == 0)
        def _():
            for i in range(seqs):
                own_send(chunk * seqs + i, 0, 1, 0).start()
                own_send(chunk * seqs + i, 1, 2, 0).start()

        for c in range(1, last_chip):
            @pl.when((chip == c) & (chunk == 0))
            def _():
                for i in range(AHEAD):
                    own_send(i, 0, last_chip, c).start()

            @pl.when((chip == c) & (chunk == n_chunks - 1))
            def _():
                for i in range(kept, n_seq):
                    own_send(i, 0, 0, c).start()

        return carry

    lax.fori_loop(0, n_chunks, project_kv, 0)

    def turn_wq(i, carry):
        for k in range(2):
            w_copy(wq_hbm, 2 * i + k, k).wait()
            w_ref[pl.ds(pl.multiple_of((2 * i + k) * WBLOCK, WBLOCK), WBLOCK), :] = w_st[k].T

            @pl.when(2 * i + k + 2 < q_blocks)
            def _():
                w_copy(wq_hbm, 2 * i + k + 2, k).start()

        return carry

    lax.fori_loop(0, q_blocks // 2, turn_wq, 0)

    def forwards(c, seq):
        by_second = (core == 1) | (seq % 4 == 3)
        return (seq < kept) & (by_second if c == 2 else jnp.logical_not(by_second))

    def hop(seq):
        for c in range(1, last_chip):
            @pl.when(chip == c)
            def _():
                own_send(seq, 0, c, 0).wait_recv()

                @pl.when(forwards(c, seq))
                def _():
                    forward(seq, 0, last_chip).start()

                @pl.when((seq + LEAD >= AHEAD) & (seq + LEAD < kept))
                def _():
                    own_send(seq + LEAD, 0, last_chip, c).start()

        @pl.when(chip == last_chip)
        def _():
            own_send(seq, 0, last_chip, 1).wait_recv()
            forward(seq, 1, 2).start()

    def project_q(i, carry):
        chunk, part = i // 2, i % 2
        h = h_ref[pl.ds(pl.multiple_of(chunk * CHUNK, CHUNK), CHUNK), :]
        keep_q(h, *tables(chunk), chunk * seqs, pl.multiple_of(part * q_rows, q_rows))

        @pl.when((part == 1) & ((chip < last_chip) | (chunk < LEAD)))
        def _():
            hop(chunk)

        return carry

    lax.fori_loop(0, 2 * n_chunks, project_q, 0)

    @pl.when(chip == 0)
    def _():
        for copy in host_copies:
            copy.wait_recv()
        guest_in = pltpu.make_async_copy(gx_hbm, x_st.at[0, pl.ds(0, guest_rows)], x_sem.at[0])
        guest_in.start()
        guest_in.wait()
        h_ref[:guest_rows, :] = normed(x_st[0, :guest_rows])
        cos, sin = [jnp.concatenate([gtab[k, g] for g in range(GUESTS)], axis=1) for k in range(2)]
        keep_kv(h_ref[:guest_rows, :], cos, sin, n_seq)
        for part in range(2):
            keep_q(h_ref[:guest_rows, :], cos, sin, n_seq, part * q_rows)

    wo_copy = pltpu.make_async_copy(wo_hbm, w_ref, wo_sem)
    wo_copy.start()
    guest_turns = jnp.where(chip == 0, GUESTS // 2, 0)
    steps = jnp.where(chip == 0, n_seq + GUESTS, jnp.where(chip == last_chip, kept, n_seq))

    def xr_start(turn):
        @pl.when(turn < guest_turns)
        def _():
            pltpu.make_async_copy(gx_hbm.at[pl.ds(turn * 2 * TOK, 2 * TOK), :], xr_ref.at[turn % 2], xr_sem.at[turn % 2]).start()

        @pl.when(turn >= guest_turns)
        def _():
            pltpu.make_async_copy(x_hbm.at[pl.ds((turn - guest_turns) * 2 * TOK, 2 * TOK), :], xr_ref.at[turn % 2], xr_sem.at[turn % 2]).start()

    def xr_wait(turn):
        pltpu.make_async_copy(x_hbm.at[pl.ds(0, 2 * TOK), :], xr_ref.at[turn % 2], xr_sem.at[turn % 2]).wait()

    def y_copy(turn, row):
        return pltpu.make_async_copy(y_st.at[turn % 2], y_hbm.at[pl.ds(row, 2 * TOK), :], y_sem.at[turn % 2])

    def guest_y(turn):
        return pltpu.make_async_remote_copy(
            src_ref=y_st.at[turn % 2], dst_ref=y_hbm.at[pl.ds((kept + 2 * turn) * TOK, 2 * TOK), :], send_sem=gy_sem.at[0, turn],
            recv_sem=gy_sem.at[1, turn], device_id={'cp': 2 * last_chip + core}, device_id_type=MESH)

    xr_start(jnp.int32(0))
    xr_start(jnp.int32(1))

    def load(seq, a):
        return pltpu.make_async_copy(kv_hbm.at[seq, a], slot_ref.at[seq % 2, 2 * a + core], load_sem.at[seq % 2, a])

    def share(seq, a, src):
        return pltpu.make_async_remote_copy(
            src_ref=src, dst_ref=slot_ref.at[seq % 2, 2 * a + core], send_sem=sib_send.at[seq % 2, a],
            recv_sem=sib_recv.at[seq % 2, a], device_id={'cp': sibling}, device_id_type=MESH)

    def reuse(step, shares):
        pl.semaphore_wait(credit, 1)
        for a in range(shares):
            share(step, a, kv_st.at[0]).wait_send()

    def stage(c, seq):
        if c == 0:
            @pl.when(seq < GUESTS)
            def _():
                reuse(seq, last_chip + 1)

            @pl.when(seq >= GUESTS)
            def _():
                reuse(seq, 1)
        else:
            @pl.when(seq >= 2)
            def _():
                reuse(seq, c + 1)

        share(seq, c, kv_st.at[seq]).start()
        slot_ref[seq % 2, 2 * c + core] = kv_st[seq]
        hopped = 1 if c == last_chip else 0
        for a in [hopped] + [a for a in range(c) if a != hopped] if c else []:
            if a != hopped:
                own_send(seq, 0, c, a).wait_recv()
            share(seq, a, kv_hbm.at[seq, a]).start()
            load(seq, a).start()

    def stage_guest(g):
        seq = kept + g
        for a, k in ((0, seq), (last_chip, n_seq + g)):
            share(seq, a, kv_st.at[k]).start()
            slot_ref[seq % 2, 2 * a + core] = kv_st[k]
        for a in range(1, last_chip):
            own_send(seq, 0, 0, a).wait_recv()
            if a == 1:
                forward(seq, 1, 2).start()
            share(seq, a, kv_hbm.at[seq, a]).start()
            load(seq, a).start()

    def arrived(c, seq):
        for a in range(c):
            load(seq, a).wait()
        for a in range(c + 1):
            share(seq, a, kv_st.at[0]).wait_recv()

    def guest_arrived(g):
        for a in range(1, last_chip):
            load(g, a).wait()
        for a in range(last_chip + 1):
            share(g, a, kv_st.at[0]).wait_recv()

    @pl.when(chip == 0)
    def _():
        stage_guest(0)

    for c in range(1, last_chip + 1):
        @pl.when(chip == c)
        def _():
            stage(c, 0)

    def project_out(turn):
        @pl.when(turn == 0)
        def _():
            wo_copy.wait()

        xr_wait(turn)

        @pl.when((turn >= 2) & (turn - 2 >= guest_turns))
        def _():
            y_copy(turn, 0).wait()

        @pl.when((turn >= 2) & (turn - 2 < guest_turns))
        def _():
            guest_y(0).wait_send()

        width = 512
        for col in range(0, dim, width):
            proj = jnp.dot(o_ref[...], w_ref[:, col:col + width], preferred_element_type=F32)
            y_st[turn % 2, :, col:col + width] = (xr_ref[turn % 2, :, col:col + width].astype(F32) + proj).astype(BF16)

        @pl.when(turn >= guest_turns)
        def _():
            y_copy(turn, (turn - guest_turns) * 2 * TOK).start()

        @pl.when(turn < guest_turns)
        def _():
            guest_y(0).start()

        @pl.when(turn + 2 < steps // 2)
        def _():
            xr_start(turn + 2)

    buffers = (q_ref, slot_ref, bias_ref, s_ref, m_ref, ot_ref)

    def step(it, carry):
        @pl.when((chip == 0) & (it < GUESTS))
        def _():
            def stage_next():
                @pl.when(it + 1 < GUESTS)
                def _():
                    stage_guest(it + 1)

                @pl.when(it + 1 == GUESTS)
                def _():
                    stage(0, jnp.int32(0))

            def wait_next():
                @pl.when(it + 1 < GUESTS)
                def _():
                    guest_arrived(it + 1)

                @pl.when(it + 1 == GUESTS)
                def _():
                    arrived(0, 0)

            @pl.when(it == 0)
            def _():
                guest_arrived(0)

            attend(*buffers, n_seq + it, n_seq + jnp.minimum(it + 1, GUESTS - 1), it == 0, n_cp, stage_next, wait_next)

        for c in range(last_chip + 1):
            seq = it - GUESTS if c == 0 else it
            last = steps - 1 - (GUESTS if c == 0 else 0)

            @pl.when((chip == c) & (seq >= 0))
            def _():
                if c:
                    @pl.when(seq == 0)
                    def _():
                        arrived(c, seq)

                def stage_next():
                    @pl.when(seq < last)
                    def _():
                        stage(c, seq + 1)

                    if c:
                        ahead, end = (LEAD, kept) if c == last_chip else (AHEAD, n_seq)

                        @pl.when(seq + ahead < end)
                        def _():
                            hop(seq + ahead)

                def wait_next():
                    @pl.when(seq < last)
                    def _():
                        arrived(c, seq + 1)

                attend(*buffers, seq, jnp.minimum(seq + 1, last), seq == 0, 2 * (c + 1), stage_next, wait_next)

        @pl.when(it + 2 < steps)
        def _():
            pl.semaphore_signal(credit, inc=1, device_id={'cp': sibling}, device_id_type=MESH)

        o_ref[pl.ds(pl.multiple_of(it % 2 * TOK, TOK), TOK), :] = ot_ref[...].T

        @pl.when(it % 2 == 1)
        def _():
            project_out(it // 2)

        return carry

    lax.fori_loop(0, steps, step, 0)

    for turn in range(2):
        y_copy(turn, 0).wait()
    for c in range(last_chip + 1):
        @pl.when(chip == c)
        def _():
            for seq in range(2):
                for a in range(c + 1):
                    share(seq, a, kv_st.at[0]).wait_send()

    @pl.when(chip == last_chip)
    def _():
        for copy in host_copies:
            copy.wait_send()
        for turn in range(GUESTS // 2):
            guest_y(turn).wait_recv()

    def drain(seq, carry):
        @pl.when(chip == 0)
        def _():
            own_send(seq, 0, 1, 0).wait_send()
            own_send(seq, 1, 2, 0).wait_send()

            @pl.when(seq >= kept)
            def _():
                forward(seq, 1, 2).wait_send()

        for c in range(1, last_chip):
            @pl.when(chip == c)
            def _():
                own_send(seq, 0, last_chip, c).wait_send()

                @pl.when(forwards(c, seq))
                def _():
                    forward(seq, 0, last_chip).wait_send()

        @pl.when((chip == last_chip) & (seq < kept))
        def _():
            forward(seq, 1, 2).wait_send()

        return carry

    lax.fori_loop(0, n_seq, drain, 0)


def solution(mesh):
    n_cp = mesh.shape['cp']

    def local_block(hidden, positions, norm_gain, w_query, w_key, w_value, w_out):
        batch, tokens, dim = hidden.shape
        kv_rows = 2 * w_key.shape[1]
        rows = batch * tokens
        chips = n_cp // 2
        x = hidden.reshape(rows, dim)
        inv_freq = 10000.0 ** (-2.0 * jnp.arange(HALF, dtype=F32) / HEAD)
        angles = positions.reshape(batch, 1, tokens).astype(F32) * inv_freq[None, :, None]
        hbm = pl.BlockSpec(memory_space=pl.ANY)
        vmem = pl.BlockSpec(memory_space=pltpu.VMEM)
        dma = pltpu.SemaphoreType.DMA
        y, _, _ = pl.pallas_call(
            functools.partial(block_kernel, n_cp),
            out_shape=[jax.ShapeDtypeStruct((rows, dim), BF16), jax.ShapeDtypeStruct((batch, chips - 1, kv_rows, TOK), BF16), jax.ShapeDtypeStruct((GUESTS * TOK, dim), BF16)],
            in_specs=[hbm, vmem, hbm, hbm, hbm, hbm, vmem, vmem],
            out_specs=[hbm, hbm, hbm],
            scratch_shapes=[
                pltpu.VMEM((2, CHUNK, dim), BF16),
                pltpu.VMEM((rows, dim), BF16),
                pltpu.VMEM((2, dim, WBLOCK), BF16),
                pltpu.VMEM((kv_rows, dim), BF16),
                pltpu.VMEM((dim, dim), BF16),
                pltpu.VMEM((batch + GUESTS, kv_rows, TOK), BF16),
                pltpu.VMEM((batch + GUESTS, dim, TOK), BF16),
                pltpu.VMEM((2, n_cp, kv_rows, TOK), BF16),
                pltpu.VMEM((n_cp * TOK, GROUP * TOK), F32),
                pltpu.VMEM((8, GROUP * TOK), F32),
                pltpu.VMEM((2 * TOK, GROUP * TOK), F32),
                pltpu.VMEM((dim, TOK), BF16),
                pltpu.VMEM((2 * TOK, dim), BF16),
                pltpu.VMEM((2, 2 * TOK, dim), BF16),
                pltpu.VMEM((2, 2 * TOK, dim), BF16),
                pltpu.VMEM((1, dim), F32),
                pltpu.VMEM((2, GUESTS, HALF, TOK), F32),
                dma((2,)), dma((2,)), dma, dma((batch, chips - 1)), dma((batch, 2)), dma((batch,)),
                dma((2, chips - 1)), dma((2, chips)), dma((2, chips)), dma((2,)), dma((2,)), dma((2, 1)), dma((2, 2)), dma((2, GUESTS // 2)),
                pltpu.SemaphoreType.REGULAR,
            ],
            compiler_params=pltpu.CompilerParams(collective_id=0, has_side_effects=True, vmem_limit_bytes=62 * 2 ** 20),
            name='block',
        )(x, norm_gain.reshape(dim // 128, 128), w_query, w_key, w_value, w_out.reshape(dim, dim), jnp.cos(angles), jnp.sin(angles))
        return y.reshape(batch, tokens, dim)

    act_spec = P('dp', 'cp', None)
    return jax.shard_map(local_block, mesh=mesh, in_specs=(act_spec, P('dp', 'cp'), P(), P(), P(), P(), P()), out_specs=act_spec, check_vma=False)
```

```python
import functools

import jax
import jax.numpy as jnp
from jax import lax
from jax.experimental import pallas as pl
from jax.experimental.pallas import tpu as pltpu
from jax.sharding import PartitionSpec as P

MESH = pl.DeviceIdType.MESH
HEAD = 64
HALF = HEAD // 2
TOK = 128
GROUP = 4
AHEAD = 4
LEAD = 2
GUESTS = 2
ROUND = 4
CHUNK = 4 * TOK
WBLOCK = 256
F32, BF16 = jnp.float32, jnp.bfloat16
NT = (((1,), (1,)), ((), ()))


def rope_rows(x, cos, sin):
    heads, n = x.shape[0] // HEAD, x.shape[1]
    x = x.reshape(heads, 2, HALF, n)
    a, b = x[:, 0], x[:, 1]
    rotated = jnp.stack([a * cos - b * sin, b * cos + a * sin], axis=1)
    return rotated.reshape(heads * HEAD, n)


def attend(q_ref, slot_ref, bias_ref, s_ref, m_ref, o_ref, seq, following, first, n_blocks, stage_next, wait_next):
    width = slot_ref.shape[2] // 2
    pairs = width // (2 * HEAD)
    key_chunks = n_blocks // 2
    kc = 2 * TOK
    cols = GROUP * TOK

    def queries(sq, g):
        base = g * GROUP * HEAD
        return jnp.concatenate([q_ref[sq, pl.ds(pl.multiple_of(base + i * HEAD, HEAD), HEAD), :] for i in range(GROUP)], axis=1)

    def scores(q, sq, g, c, peak):
        row = pl.ds(pl.multiple_of(g * HEAD, HEAD), HEAD)
        keys = jnp.concatenate([slot_ref[sq % 2, 2 * c + i, row, :].T for i in range(2)], axis=0)
        s = jnp.dot(keys, q, preferred_element_type=F32)
        if c == key_chunks - 1:
            s = s + bias_ref[...]
        s_ref[c * kc:(c + 1) * kc, :] = s
        top = jnp.max(s.reshape(kc // 8, 8, cols), axis=0)
        return top if peak is None else jnp.maximum(peak, top)

    def unit(g, sq_next, g_next, peak):
        peak = jnp.max(peak, axis=0, keepdims=True)
        q_next = queries(sq_next, g_next)
        vrow = pl.ds(pl.multiple_of(width + g * HEAD, HEAD), HEAD)
        total, out, peak_next = None, None, None
        for c in range(key_chunks):
            prob = jnp.exp(s_ref[c * kc:(c + 1) * kc, :] - peak)
            part = jnp.sum(prob.reshape(kc // 8, 8, cols), axis=0)
            total = part if total is None else total + part
            values = jnp.concatenate([slot_ref[seq % 2, 2 * c + i, vrow, :] for i in range(2)], axis=1)
            term = jnp.dot(values, prob.astype(BF16), preferred_element_type=F32)
            out = term if out is None else out + term
            peak_next = scores(q_next, sq_next, g_next, c, peak_next)
        out = out / jnp.sum(total, axis=0, keepdims=True)
        for i in range(GROUP):
            o_ref[pl.ds(pl.multiple_of((g * GROUP + i) * HEAD, HEAD), HEAD), :] = out[:, i * TOK:(i + 1) * TOK].astype(BF16)
        return peak_next

    @pl.when(first)
    def _():
        q_first, peak = queries(seq, 0), None
        for c in range(key_chunks):
            peak = scores(q_first, seq, 0, c, peak)
        m_ref[...] = peak

    def pair(j, carry):
        @pl.when(j == 1)
        def _():
            stage_next()

        last = j == pairs - 1

        @pl.when(last)
        def _():
            wait_next()

        sq_next = jnp.where(last, following, seq)
        g_next = jnp.where(last, 0, 2 * j + 2)
        peak = unit(2 * j, seq, 2 * j + 1, m_ref[...])
        m_ref[...] = unit(2 * j + 1, sq_next, g_next, peak)
        return carry

    lax.fori_loop(0, pairs, pair, 0)


def block_kernel(
    n_cp, x_hbm, gain_ref, wq_hbm, wk_hbm, wv_hbm, wo_hbm, cos_ref, sin_ref, y_hbm, kv_hbm, gx_hbm,
    x_st, h_ref, w_st, wkv_ref, w_ref, kv_st, q_ref, slot_ref, s_ref, m_ref, bias_ref, ot_ref, o_ref, xr_ref, y_st, gain_row, gtab, gy_st,
    x_sem, w_sem, wo_sem, recv_sem, own_sem, fwd_sem, load_sem, sib_recv, sib_send, xr_sem, y_sem, gx_sem, gt_sem, gy_sem, credit,
):
    me = lax.axis_index('cp')
    chip, core = me // 2, me % 2
    sibling = me + 1 - 2 * core
    n_seq = cos_ref.shape[0]
    kept = n_seq - GUESTS
    guest_rows = GUESTS * TOK
    straight = n_seq - ROUND
    dim = x_st.shape[2]
    kv_rows = wkv_ref.shape[0]
    n_chunks = n_seq * TOK // CHUNK
    seqs = CHUNK // TOK
    last_chip = n_cp // 2 - 1

    barrier = pltpu.get_barrier_semaphore()
    for step in range(1, n_cp):
        pl.semaphore_signal(barrier, inc=1, device_id={'cp': (me + step) % n_cp}, device_id_type=MESH)

    def x_copy(chunk):
        return pltpu.make_async_copy(x_hbm.at[pl.ds(chunk * CHUNK, CHUNK), :], x_st.at[chunk % 2], x_sem.at[chunk % 2])

    def w_copy(hbm, block, slot):
        return pltpu.make_async_copy(hbm.at[:, pl.ds(block * WBLOCK, WBLOCK)], w_st.at[slot], w_sem.at[slot])

    kv_blocks = [(wk_hbm, i) for i in range(kv_rows // 2 // WBLOCK)] + [(wv_hbm, i) for i in range(kv_rows // 2 // WBLOCK)]
    q_blocks = dim // WBLOCK
    x_copy(0).start()
    for i in range(2):
        w_copy(*kv_blocks[i], i).start()
    x_copy(1).start()

    key = lax.broadcasted_iota(jnp.int32, (2 * TOK, TOK), 0)
    tok = lax.broadcasted_iota(jnp.int32, (2 * TOK, TOK), 1)
    bias = jnp.where(key <= tok + core * TOK, 0.0, -jnp.inf).astype(F32)
    bias_ref[...] = jnp.concatenate([bias] * GROUP, axis=1)

    gain = gain_ref[...].astype(F32)
    for i in range(gain.shape[0]):
        gain_row[:, i * gain.shape[1]:(i + 1) * gain.shape[1]] = gain[i:i + 1]

    def tables(chunk):
        return [jnp.concatenate([t[chunk * seqs + i] for i in range(seqs)], axis=1) for t in (cos_ref, sin_ref)]

    for i, (hbm, block) in enumerate(kv_blocks):
        w_copy(hbm, block, i % 2).wait()
        wkv_ref[i * WBLOCK:(i + 1) * WBLOCK, :] = w_st[i % 2].T
        nxt = i + 2
        if nxt < len(kv_blocks):
            w_copy(*kv_blocks[nxt], i % 2).start()
        else:
            w_copy(wq_hbm, nxt - len(kv_blocks), i % 2).start()

    def own_send(seq, target, to_chip, from_chip):
        return pltpu.make_async_remote_copy(
            src_ref=kv_st.at[seq], dst_ref=kv_hbm.at[seq, from_chip], send_sem=own_sem.at[seq, target],
            recv_sem=recv_sem.at[seq, from_chip], device_id={'cp': 2 * to_chip + core}, device_id_type=MESH)

    def forward(seq, block, to_chip):
        return pltpu.make_async_remote_copy(
            src_ref=kv_hbm.at[seq, block], dst_ref=kv_hbm.at[seq, block], send_sem=fwd_sem.at[seq],
            recv_sem=recv_sem.at[seq, block], device_id={'cp': 2 * to_chip + core}, device_id_type=MESH)

    def to_host(src, dst, sems, k):
        return pltpu.make_async_remote_copy(
            src_ref=src, dst_ref=dst, send_sem=sems.at[0, k], recv_sem=sems.at[1, k], device_id={'cp': core}, device_id_type=MESH)

    host_copies = [
        to_host(cos_ref.at[pl.ds(kept, GUESTS)], gtab.at[0], gt_sem, 0),
        to_host(sin_ref.at[pl.ds(kept, GUESTS)], gtab.at[1], gt_sem, 1),
        to_host(x_hbm.at[pl.ds(kept * TOK, guest_rows), :], gx_hbm, gx_sem, 0),
    ]
    pl.semaphore_wait(barrier, n_cp - 1)

    @pl.when(chip == last_chip)
    def _():
        for copy in host_copies:
            copy.start()

    def normed(x):
        x = x.astype(F32)
        inv_rms = lax.rsqrt(jnp.mean(x * x, axis=-1, keepdims=True) + 1e-5)
        return (x * inv_rms * gain_row[...]).astype(BF16)

    def keep_kv(h, cos, sin, first):
        kv = lax.dot_general(wkv_ref[...], h, NT, preferred_element_type=F32)
        k = rope_rows(kv[:kv_rows // 2], cos, sin).astype(BF16)
        v = kv[kv_rows // 2:].astype(BF16)
        for i in range(h.shape[0] // TOK):
            kv_st[first + i, :kv_rows // 2, :] = k[:, i * TOK:(i + 1) * TOK]
            kv_st[first + i, kv_rows // 2:, :] = v[:, i * TOK:(i + 1) * TOK]

    def keep_q(h, cos, sin, first, base):
        q = lax.dot_general(w_ref[pl.ds(base, q_rows), :], h, NT, preferred_element_type=F32)
        q = (rope_rows(q, cos, sin) * (HEAD ** -0.5)).astype(BF16)
        for i in range(h.shape[0] // TOK):
            q_ref[first + i, pl.ds(base, q_rows), :] = q[:, i * TOK:(i + 1) * TOK]

    q_rows = dim // 2

    def send_both(chunk):
        for i in range(seqs):
            own_send(chunk * seqs + i, 0, 1, 0).start()
            own_send(chunk * seqs + i, 1, 2, 0).start()

    def project_kv(chunk, carry):
        x_copy(chunk).wait()
        rows = pl.ds(pl.multiple_of(chunk * CHUNK, CHUNK), CHUNK)
        h_ref[rows, :] = normed(x_st[chunk % 2])

        @pl.when(chunk + 2 < n_chunks)
        def _():
            x_copy(chunk + 2).start()

        keep_kv(h_ref[rows, :], *tables(chunk), chunk * seqs)

        @pl.when((chip == 0) & (chunk < n_chunks // 2))
        def _():
            send_both(chunk)

        for c in range(1, last_chip):
            @pl.when((chip == c) & (chunk == 0))
            def _():
                for i in range(AHEAD):
                    own_send(i, 0, last_chip, c).start()

            @pl.when((chip == c) & (chunk == n_chunks - 1))
            def _():
                for i in range(kept, n_seq):
                    own_send(i, 0, 0, c).start()
                if c == 1:
                    for i in range(straight, kept):
                        own_send(i, 1, 0, c).start()

        return carry

    lax.fori_loop(0, n_chunks, project_kv, 0)

    def turn_wq(i, carry):
        for k in range(2):
            w_copy(wq_hbm, 2 * i + k, k).wait()
            w_ref[pl.ds(pl.multiple_of((2 * i + k) * WBLOCK, WBLOCK), WBLOCK), :] = w_st[k].T

            @pl.when(2 * i + k + 2 < q_blocks)
            def _():
                w_copy(wq_hbm, 2 * i + k + 2, k).start()

        return carry

    lax.fori_loop(0, q_blocks // 2, turn_wq, 0)

    def forwards(c, seq):
        by_second = (core == 1) | (seq % 4 == 3)
        return (seq < kept) & (by_second if c == 2 else jnp.logical_not(by_second))

    def hop(seq):
        for c in range(1, last_chip):
            @pl.when(chip == c)
            def _():
                own_send(seq, 0, c, 0).wait_recv()

                @pl.when(forwards(c, seq))
                def _():
                    forward(seq, 0, last_chip).start()

                @pl.when((seq + LEAD >= AHEAD) & (seq + LEAD < kept))
                def _():
                    own_send(seq + LEAD, 0, last_chip, c).start()

        @pl.when(chip == last_chip)
        def _():
            own_send(seq, 0, last_chip, 1).wait_recv()
            forward(seq, 1, 2).start()

    def project_q(i, carry):
        chunk, part = i // 2, i % 2
        h = h_ref[pl.ds(pl.multiple_of(chunk * CHUNK, CHUNK), CHUNK), :]
        keep_q(h, *tables(chunk), chunk * seqs, pl.multiple_of(part * q_rows, q_rows))

        @pl.when((part == 1) & ((chip < last_chip) | (chunk < LEAD)))
        def _():
            hop(chunk)

        return carry

    lax.fori_loop(0, 2 * n_chunks, project_q, 0)

    @pl.when(chip == 0)
    def _():
        for copy in host_copies:
            copy.wait_recv()
        guest_in = pltpu.make_async_copy(gx_hbm, x_st.at[0, pl.ds(0, guest_rows)], x_sem.at[0])
        guest_in.start()
        guest_in.wait()
        h_ref[:guest_rows, :] = normed(x_st[0, :guest_rows])
        cos, sin = [jnp.concatenate([gtab[k, g] for g in range(GUESTS)], axis=1) for k in range(2)]
        keep_kv(h_ref[:guest_rows, :], cos, sin, n_seq)
        for part in range(2):
            keep_q(h_ref[:guest_rows, :], cos, sin, n_seq, part * q_rows)

    wo_copy = pltpu.make_async_copy(wo_hbm, w_ref, wo_sem)
    wo_copy.start()
    guest_turns = jnp.where(chip == 0, GUESTS // 2, 0)
    steps = jnp.where(chip == 0, n_seq + GUESTS, jnp.where(chip == last_chip, kept, n_seq))

    def xr_start(turn):
        @pl.when(turn < guest_turns)
        def _():
            pltpu.make_async_copy(gx_hbm.at[pl.ds(turn * 2 * TOK, 2 * TOK), :], xr_ref.at[turn % 2], xr_sem.at[turn % 2]).start()

        @pl.when(turn >= guest_turns)
        def _():
            pltpu.make_async_copy(x_hbm.at[pl.ds((turn - guest_turns) * 2 * TOK, 2 * TOK), :], xr_ref.at[turn % 2], xr_sem.at[turn % 2]).start()

    def xr_wait(turn):
        pltpu.make_async_copy(x_hbm.at[pl.ds(0, 2 * TOK), :], xr_ref.at[turn % 2], xr_sem.at[turn % 2]).wait()

    def y_copy(turn, row):
        return pltpu.make_async_copy(y_st.at[turn % 2], y_hbm.at[pl.ds(row, 2 * TOK), :], y_sem.at[turn % 2])

    def guest_y(turn):
        return pltpu.make_async_remote_copy(
            src_ref=gy_st, dst_ref=y_hbm.at[pl.ds((kept + 2 * turn) * TOK, 2 * TOK), :], send_sem=gy_sem.at[0, turn],
            recv_sem=gy_sem.at[1, turn], device_id={'cp': 2 * last_chip + core}, device_id_type=MESH)

    xr_start(jnp.int32(0))
    xr_start(jnp.int32(1))

    def load(seq, a):
        return pltpu.make_async_copy(kv_hbm.at[seq, a], slot_ref.at[seq % 2, 2 * a + core], load_sem.at[seq % 2, a])

    def share(seq, a, src):
        return pltpu.make_async_remote_copy(
            src_ref=src, dst_ref=slot_ref.at[seq % 2, 2 * a + core], send_sem=sib_send.at[seq % 2, a],
            recv_sem=sib_recv.at[seq % 2, a], device_id={'cp': sibling}, device_id_type=MESH)

    def reuse(step, shares):
        pl.semaphore_wait(credit, 1)
        for a in range(shares):
            share(step, a, kv_st.at[0]).wait_send()

    def stage(c, seq):
        if c == 0:
            @pl.when(seq < GUESTS)
            def _():
                reuse(seq, last_chip + 1)

            @pl.when(seq >= GUESTS)
            def _():
                reuse(seq, 1)
        else:
            @pl.when(seq >= 2)
            def _():
                reuse(seq, c + 1)

        share(seq, c, kv_st.at[seq]).start()
        slot_ref[seq % 2, 2 * c + core] = kv_st[seq]
        hopped = 1 if c == last_chip else 0
        for a in [hopped] + [a for a in range(c) if a != hopped] if c else []:
            if a != hopped:
                own_send(seq, 0, c, a).wait_recv()
            elif c == last_chip:
                @pl.when(seq >= straight)
                def _():
                    own_send(seq, 0, c, a).wait_recv()
            share(seq, a, kv_hbm.at[seq, a]).start()
            load(seq, a).start()

    def stage_guest(g):
        seq = kept + g

        @pl.when(g == 0)
        def _():
            for k in range(straight, kept):
                own_send(k, 1, 0, 1).wait_recv()
                forward(k, 1, 2).start()

        for a, k in ((0, seq), (last_chip, n_seq + g)):
            share(seq, a, kv_st.at[k]).start()
            slot_ref[seq % 2, 2 * a + core] = kv_st[k]
        for a in range(1, last_chip):
            own_send(seq, 0, 0, a).wait_recv()
            if a == 1:
                forward(seq, 1, 2).start()
            share(seq, a, kv_hbm.at[seq, a]).start()
            load(seq, a).start()

        @pl.when(g == GUESTS - 1)
        def _():
            for chunk in range(n_chunks // 2, n_chunks - 1):
                send_both(chunk)

    def arrived(c, seq):
        for a in range(c):
            load(seq, a).wait()
        for a in range(c + 1):
            share(seq, a, kv_st.at[0]).wait_recv()

    def guest_arrived(g):
        for a in range(1, last_chip):
            load(g, a).wait()
        for a in range(last_chip + 1):
            share(g, a, kv_st.at[0]).wait_recv()

    @pl.when(chip == 0)
    def _():
        stage_guest(0)

    for c in range(1, last_chip + 1):
        @pl.when(chip == c)
        def _():
            stage(c, 0)

    def project_out(turn):
        @pl.when(turn == 0)
        def _():
            wo_copy.wait()

        xr_wait(turn)

        @pl.when((turn >= 2) & (turn - 2 >= guest_turns))
        def _():
            y_copy(turn, 0).wait()

        width = 512
        for col in range(0, dim, width):
            proj = jnp.dot(o_ref[...], w_ref[:, col:col + width], preferred_element_type=F32)
            part = (xr_ref[turn % 2, :, col:col + width].astype(F32) + proj).astype(BF16)
            y_st[turn % 2, :, col:col + width] = part

            @pl.when(turn < guest_turns)
            def _():
                gy_st[:, col:col + width] = part

        @pl.when(turn >= guest_turns)
        def _():
            y_copy(turn, (turn - guest_turns) * 2 * TOK).start()

        @pl.when(turn < guest_turns)
        def _():
            guest_y(0).start()
            send_both(n_chunks - 1)

        @pl.when(turn + 2 < steps // 2)
        def _():
            xr_start(turn + 2)

    buffers = (q_ref, slot_ref, bias_ref, s_ref, m_ref, ot_ref)

    def step(it, carry):
        @pl.when((chip == 0) & (it < GUESTS))
        def _():
            def stage_next():
                @pl.when(it + 1 < GUESTS)
                def _():
                    stage_guest(it + 1)

                @pl.when(it + 1 == GUESTS)
                def _():
                    stage(0, jnp.int32(0))

            def wait_next():
                @pl.when(it + 1 < GUESTS)
                def _():
                    guest_arrived(it + 1)

                @pl.when(it + 1 == GUESTS)
                def _():
                    arrived(0, 0)

            @pl.when(it == 0)
            def _():
                guest_arrived(0)

            attend(*buffers, n_seq + it, n_seq + jnp.minimum(it + 1, GUESTS - 1), it == 0, n_cp, stage_next, wait_next)

        for c in range(last_chip + 1):
            seq = it - GUESTS if c == 0 else it
            last = steps - 1 - (GUESTS if c == 0 else 0)

            @pl.when((chip == c) & (seq >= 0))
            def _():
                if c:
                    @pl.when(seq == 0)
                    def _():
                        arrived(c, seq)

                def stage_next():
                    @pl.when(seq < last)
                    def _():
                        stage(c, seq + 1)

                    if c:
                        ahead, end = (LEAD, straight) if c == last_chip else (AHEAD, n_seq)

                        @pl.when(seq + ahead < end)
                        def _():
                            hop(seq + ahead)

                def wait_next():
                    @pl.when(seq < last)
                    def _():
                        arrived(c, seq + 1)

                attend(*buffers, seq, jnp.minimum(seq + 1, last), seq == 0, 2 * (c + 1), stage_next, wait_next)

        @pl.when(it + 2 < steps)
        def _():
            pl.semaphore_signal(credit, inc=1, device_id={'cp': sibling}, device_id_type=MESH)

        o_ref[pl.ds(pl.multiple_of(it % 2 * TOK, TOK), TOK), :] = ot_ref[...].T

        @pl.when(it % 2 == 1)
        def _():
            project_out(it // 2)

        return carry

    lax.fori_loop(0, steps, step, 0)

    for turn in range(2):
        y_copy(turn, 0).wait()
    for c in range(last_chip + 1):
        @pl.when(chip == c)
        def _():
            for seq in range(2):
                for a in range(c + 1):
                    share(seq, a, kv_st.at[0]).wait_send()

    @pl.when(chip == 0)
    def _():
        guest_y(0).wait_send()

    @pl.when(chip == last_chip)
    def _():
        for copy in host_copies:
            copy.wait_send()
        for turn in range(GUESTS // 2):
            guest_y(turn).wait_recv()

    def drain(seq, carry):
        @pl.when(chip == 0)
        def _():
            own_send(seq, 0, 1, 0).wait_send()
            own_send(seq, 1, 2, 0).wait_send()

            @pl.when(seq >= straight)
            def _():
                forward(seq, 1, 2).wait_send()

        @pl.when((chip == 1) & (seq >= straight) & (seq < kept))
        def _():
            own_send(seq, 1, 0, 1).wait_send()

        for c in range(1, last_chip):
            @pl.when(chip == c)
            def _():
                own_send(seq, 0, last_chip, c).wait_send()

                @pl.when(forwards(c, seq))
                def _():
                    forward(seq, 0, last_chip).wait_send()

        @pl.when((chip == last_chip) & (seq < straight))
        def _():
            forward(seq, 1, 2).wait_send()

        return carry

    lax.fori_loop(0, n_seq, drain, 0)


def solution(mesh):
    n_cp = mesh.shape['cp']

    def local_block(hidden, positions, norm_gain, w_query, w_key, w_value, w_out):
        batch, tokens, dim = hidden.shape
        kv_rows = 2 * w_key.shape[1]
        rows = batch * tokens
        chips = n_cp // 2
        x = hidden.reshape(rows, dim)
        inv_freq = 10000.0 ** (-2.0 * jnp.arange(HALF, dtype=F32) / HEAD)
        angles = positions.reshape(batch, 1, tokens).astype(F32) * inv_freq[None, :, None]
        hbm = pl.BlockSpec(memory_space=pl.ANY)
        vmem = pl.BlockSpec(memory_space=pltpu.VMEM)
        dma = pltpu.SemaphoreType.DMA
        y, _, _ = pl.pallas_call(
            functools.partial(block_kernel, n_cp),
            out_shape=[jax.ShapeDtypeStruct((rows, dim), BF16), jax.ShapeDtypeStruct((batch, chips - 1, kv_rows, TOK), BF16), jax.ShapeDtypeStruct((GUESTS * TOK, dim), BF16)],
            in_specs=[hbm, vmem, hbm, hbm, hbm, hbm, vmem, vmem],
            out_specs=[hbm, hbm, hbm],
            scratch_shapes=[
                pltpu.VMEM((2, CHUNK, dim), BF16),
                pltpu.VMEM((rows, dim), BF16),
                pltpu.VMEM((2, dim, WBLOCK), BF16),
                pltpu.VMEM((kv_rows, dim), BF16),
                pltpu.VMEM((dim, dim), BF16),
                pltpu.VMEM((batch + GUESTS, kv_rows, TOK), BF16),
                pltpu.VMEM((batch + GUESTS, dim, TOK), BF16),
                pltpu.VMEM((2, n_cp, kv_rows, TOK), BF16),
                pltpu.VMEM((n_cp * TOK, GROUP * TOK), F32),
                pltpu.VMEM((8, GROUP * TOK), F32),
                pltpu.VMEM((2 * TOK, GROUP * TOK), F32),
                pltpu.VMEM((dim, TOK), BF16),
                pltpu.VMEM((2 * TOK, dim), BF16),
                pltpu.VMEM((2, 2 * TOK, dim), BF16),
                pltpu.VMEM((2, 2 * TOK, dim), BF16),
                pltpu.VMEM((1, dim), F32),
                pltpu.VMEM((2, GUESTS, HALF, TOK), F32),
                pltpu.VMEM((GUESTS * TOK, dim), BF16),
                dma((2,)), dma((2,)), dma, dma((batch, chips - 1)), dma((batch, 2)), dma((batch,)),
                dma((2, chips - 1)), dma((2, chips)), dma((2, chips)), dma((2,)), dma((2,)), dma((2, 1)), dma((2, 2)), dma((2, GUESTS // 2)),
                pltpu.SemaphoreType.REGULAR,
            ],
            compiler_params=pltpu.CompilerParams(collective_id=0, has_side_effects=True, vmem_limit_bytes=62 * 2 ** 20),
            name='block',
        )(x, norm_gain.reshape(dim // 128, 128), w_query, w_key, w_value, w_out.reshape(dim, dim), jnp.cos(angles), jnp.sin(angles))
        return y.reshape(batch, tokens, dim)

    act_spec = P('dp', 'cp', None)
    return jax.shard_map(local_block, mesh=mesh, in_specs=(act_spec, P('dp', 'cp'), P(), P(), P(), P(), P()), out_specs=act_spec, check_vma=False)
```

```python
import functools

import jax
import jax.numpy as jnp
from jax import lax
from jax.experimental import pallas as pl
from jax.experimental.pallas import tpu as pltpu
from jax.sharding import PartitionSpec as P

MESH = pl.DeviceIdType.MESH
HEAD = 64
HALF = HEAD // 2
TOK = 128
GROUP = 4
AHEAD = 4
LEAD = 2
GUESTS = 2
ROUND = 4
CHUNK = 4 * TOK
WBLOCK = 256
F32, BF16 = jnp.float32, jnp.bfloat16
NT = (((1,), (1,)), ((), ()))


def rope_rows(x, cos, sin):
    heads, n = x.shape[0] // HEAD, x.shape[1]
    x = x.reshape(heads, 2, HALF, n)
    a, b = x[:, 0], x[:, 1]
    rotated = jnp.stack([a * cos - b * sin, b * cos + a * sin], axis=1)
    return rotated.reshape(heads * HEAD, n)


def attend(q_ref, slot_ref, bias_ref, s_ref, m_ref, o_ref, seq, following, first, n_blocks, pass_on, stage_next, wait_next):
    width = slot_ref.shape[2] // 2
    pairs = width // (2 * HEAD)
    key_chunks = n_blocks // 2
    kc = 2 * TOK
    cols = GROUP * TOK

    def queries(sq, g):
        base = g * GROUP * HEAD
        return jnp.concatenate([q_ref[sq, pl.ds(pl.multiple_of(base + i * HEAD, HEAD), HEAD), :] for i in range(GROUP)], axis=1)

    def scores(q, sq, g, c, peak):
        row = pl.ds(pl.multiple_of(g * HEAD, HEAD), HEAD)
        keys = jnp.concatenate([slot_ref[sq % 2, 2 * c + i, row, :].T for i in range(2)], axis=0)
        s = jnp.dot(keys, q, preferred_element_type=F32)
        if c == key_chunks - 1:
            s = s + bias_ref[...]
        s_ref[c * kc:(c + 1) * kc, :] = s
        top = jnp.max(s.reshape(kc // 8, 8, cols), axis=0)
        return top if peak is None else jnp.maximum(peak, top)

    def unit(g, sq_next, g_next, peak):
        peak = jnp.max(peak, axis=0, keepdims=True)
        q_next = queries(sq_next, g_next)
        vrow = pl.ds(pl.multiple_of(width + g * HEAD, HEAD), HEAD)
        total, out, peak_next = None, None, None
        for c in range(key_chunks):
            prob = jnp.exp(s_ref[c * kc:(c + 1) * kc, :] - peak)
            part = jnp.sum(prob.reshape(kc // 8, 8, cols), axis=0)
            total = part if total is None else total + part
            values = jnp.concatenate([slot_ref[seq % 2, 2 * c + i, vrow, :] for i in range(2)], axis=1)
            term = jnp.dot(values, prob.astype(BF16), preferred_element_type=F32)
            out = term if out is None else out + term
            peak_next = scores(q_next, sq_next, g_next, c, peak_next)
        out = out / jnp.sum(total, axis=0, keepdims=True)
        for i in range(GROUP):
            o_ref[pl.ds(pl.multiple_of((g * GROUP + i) * HEAD, HEAD), HEAD), :] = out[:, i * TOK:(i + 1) * TOK].astype(BF16)
        return peak_next

    @pl.when(first)
    def _():
        q_first, peak = queries(seq, 0), None
        for c in range(key_chunks):
            peak = scores(q_first, seq, 0, c, peak)
        m_ref[...] = peak

    def pair(j, carry):
        @pl.when(j == 0)
        def _():
            pass_on()

        @pl.when(j == 1)
        def _():
            stage_next()

        last = j == pairs - 1

        @pl.when(last)
        def _():
            wait_next()

        sq_next = jnp.where(last, following, seq)
        g_next = jnp.where(last, 0, 2 * j + 2)
        peak = unit(2 * j, seq, 2 * j + 1, m_ref[...])
        m_ref[...] = unit(2 * j + 1, sq_next, g_next, peak)
        return carry

    lax.fori_loop(0, pairs, pair, 0)


def block_kernel(
    n_cp, x_hbm, gain_ref, wq_hbm, wk_hbm, wv_hbm, wo_hbm, cos_ref, sin_ref, y_hbm, kv_hbm, gx_hbm,
    x_st, h_ref, w_st, wkv_ref, w_ref, kv_st, q_ref, slot_ref, s_ref, m_ref, bias_ref, ot_ref, o_ref, xr_ref, y_st, gain_row, gtab, gy_st,
    x_sem, w_sem, wo_sem, recv_sem, own_sem, fwd_sem, load_sem, sib_recv, sib_send, xr_sem, y_sem, gx_sem, gt_sem, gy_sem, credit,
):
    me = lax.axis_index('cp')
    chip, core = me // 2, me % 2
    sibling = me + 1 - 2 * core
    n_seq = cos_ref.shape[0]
    kept = n_seq - GUESTS
    guest_rows = GUESTS * TOK
    straight = n_seq - ROUND
    dim = x_st.shape[2]
    kv_rows = wkv_ref.shape[0]
    n_chunks = n_seq * TOK // CHUNK
    seqs = CHUNK // TOK
    last_chip = n_cp // 2 - 1

    barrier = pltpu.get_barrier_semaphore()
    for step in range(1, n_cp):
        pl.semaphore_signal(barrier, inc=1, device_id={'cp': (me + step) % n_cp}, device_id_type=MESH)

    def x_copy(chunk):
        return pltpu.make_async_copy(x_hbm.at[pl.ds(chunk * CHUNK, CHUNK), :], x_st.at[chunk % 2], x_sem.at[chunk % 2])

    def w_copy(hbm, block, slot):
        return pltpu.make_async_copy(hbm.at[:, pl.ds(block * WBLOCK, WBLOCK)], w_st.at[slot], w_sem.at[slot])

    kv_blocks = [(wk_hbm, i) for i in range(kv_rows // 2 // WBLOCK)] + [(wv_hbm, i) for i in range(kv_rows // 2 // WBLOCK)]
    q_blocks = dim // WBLOCK
    x_copy(0).start()
    for i in range(2):
        w_copy(*kv_blocks[i], i).start()
    x_copy(1).start()

    key = lax.broadcasted_iota(jnp.int32, (2 * TOK, TOK), 0)
    tok = lax.broadcasted_iota(jnp.int32, (2 * TOK, TOK), 1)
    bias = jnp.where(key <= tok + core * TOK, 0.0, -jnp.inf).astype(F32)
    bias_ref[...] = jnp.concatenate([bias] * GROUP, axis=1)

    gain = gain_ref[...].astype(F32)
    for i in range(gain.shape[0]):
        gain_row[:, i * gain.shape[1]:(i + 1) * gain.shape[1]] = gain[i:i + 1]

    def tables(chunk):
        return [jnp.concatenate([t[chunk * seqs + i] for i in range(seqs)], axis=1) for t in (cos_ref, sin_ref)]

    for i, (hbm, block) in enumerate(kv_blocks):
        w_copy(hbm, block, i % 2).wait()
        wkv_ref[i * WBLOCK:(i + 1) * WBLOCK, :] = w_st[i % 2].T
        nxt = i + 2
        if nxt < len(kv_blocks):
            w_copy(*kv_blocks[nxt], i % 2).start()
        else:
            w_copy(wq_hbm, nxt - len(kv_blocks), i % 2).start()

    def own_send(seq, target, to_chip, from_chip):
        return pltpu.make_async_remote_copy(
            src_ref=kv_st.at[seq], dst_ref=kv_hbm.at[seq, from_chip], send_sem=own_sem.at[seq, target],
            recv_sem=recv_sem.at[seq, from_chip], device_id={'cp': 2 * to_chip + core}, device_id_type=MESH)

    def forward(seq, block, to_chip):
        return pltpu.make_async_remote_copy(
            src_ref=kv_hbm.at[seq, block], dst_ref=kv_hbm.at[seq, block], send_sem=fwd_sem.at[seq],
            recv_sem=recv_sem.at[seq, block], device_id={'cp': 2 * to_chip + core}, device_id_type=MESH)

    def to_host(src, dst, sems, k):
        return pltpu.make_async_remote_copy(
            src_ref=src, dst_ref=dst, send_sem=sems.at[0, k], recv_sem=sems.at[1, k], device_id={'cp': core}, device_id_type=MESH)

    host_copies = [
        to_host(cos_ref.at[pl.ds(kept, GUESTS)], gtab.at[0], gt_sem, 0),
        to_host(sin_ref.at[pl.ds(kept, GUESTS)], gtab.at[1], gt_sem, 1),
        to_host(x_hbm.at[pl.ds(kept * TOK, guest_rows), :], gx_hbm, gx_sem, 0),
    ]
    pl.semaphore_wait(barrier, n_cp - 1)

    @pl.when(chip == last_chip)
    def _():
        for copy in host_copies:
            copy.start()

    def normed(x):
        x = x.astype(F32)
        inv_rms = lax.rsqrt(jnp.mean(x * x, axis=-1, keepdims=True) + 1e-5)
        return (x * inv_rms * gain_row[...]).astype(BF16)

    def keep_kv(h, cos, sin, first):
        kv = lax.dot_general(wkv_ref[...], h, NT, preferred_element_type=F32)
        k = rope_rows(kv[:kv_rows // 2], cos, sin).astype(BF16)
        v = kv[kv_rows // 2:].astype(BF16)
        for i in range(h.shape[0] // TOK):
            kv_st[first + i, :kv_rows // 2, :] = k[:, i * TOK:(i + 1) * TOK]
            kv_st[first + i, kv_rows // 2:, :] = v[:, i * TOK:(i + 1) * TOK]

    def keep_q(h, cos, sin, first, base):
        q = lax.dot_general(w_ref[pl.ds(base, q_rows), :], h, NT, preferred_element_type=F32)
        q = (rope_rows(q, cos, sin) * (HEAD ** -0.5)).astype(BF16)
        for i in range(h.shape[0] // TOK):
            q_ref[first + i, pl.ds(base, q_rows), :] = q[:, i * TOK:(i + 1) * TOK]

    q_rows = dim // 2

    def send_both(chunk):
        for i in range(seqs):
            own_send(chunk * seqs + i, 0, 1, 0).start()
            own_send(chunk * seqs + i, 1, 2, 0).start()

    def project_kv(chunk, carry):
        x_copy(chunk).wait()
        rows = pl.ds(pl.multiple_of(chunk * CHUNK, CHUNK), CHUNK)
        h_ref[rows, :] = normed(x_st[chunk % 2])

        @pl.when(chunk + 2 < n_chunks)
        def _():
            x_copy(chunk + 2).start()

        keep_kv(h_ref[rows, :], *tables(chunk), chunk * seqs)

        @pl.when((chip == 0) & (chunk < n_chunks // 2))
        def _():
            send_both(chunk)

        for c in range(1, last_chip):
            @pl.when((chip == c) & (chunk == 0))
            def _():
                for i in range(AHEAD):
                    own_send(i, 0, last_chip, c).start()

            @pl.when((chip == c) & (chunk == n_chunks - 1))
            def _():
                for i in range(kept, n_seq):
                    own_send(i, 0, 0, c).start()
                if c == 1:
                    for i in range(straight, kept):
                        own_send(i, 1, 0, c).start()

        return carry

    lax.fori_loop(0, n_chunks, project_kv, 0)

    def turn_wq(i, carry):
        for k in range(2):
            w_copy(wq_hbm, 2 * i + k, k).wait()
            w_ref[pl.ds(pl.multiple_of((2 * i + k) * WBLOCK, WBLOCK), WBLOCK), :] = w_st[k].T

            @pl.when(2 * i + k + 2 < q_blocks)
            def _():
                w_copy(wq_hbm, 2 * i + k + 2, k).start()

        return carry

    lax.fori_loop(0, q_blocks // 2, turn_wq, 0)

    def forwards(c, seq):
        by_second = (core == 1) | (seq % 4 == 3)
        return (seq < kept) & (by_second if c == 2 else jnp.logical_not(by_second))

    def hop(seq):
        for c in range(1, last_chip):
            @pl.when(chip == c)
            def _():
                own_send(seq, 0, c, 0).wait_recv()

                @pl.when(forwards(c, seq))
                def _():
                    forward(seq, 0, last_chip).start()

                @pl.when((seq + LEAD >= AHEAD) & (seq + LEAD < kept))
                def _():
                    own_send(seq + LEAD, 0, last_chip, c).start()

        @pl.when(chip == last_chip)
        def _():
            own_send(seq, 0, last_chip, 1).wait_recv()
            forward(seq, 1, 2).start()

    def project_q(i, carry):
        chunk, part = i // 2, i % 2
        h = h_ref[pl.ds(pl.multiple_of(chunk * CHUNK, CHUNK), CHUNK), :]
        keep_q(h, *tables(chunk), chunk * seqs, pl.multiple_of(part * q_rows, q_rows))

        @pl.when((part == 1) & ((chip < last_chip) | (chunk < LEAD)))
        def _():
            hop(chunk)

        return carry

    lax.fori_loop(0, 2 * n_chunks, project_q, 0)

    @pl.when(chip == 0)
    def _():
        for copy in host_copies:
            copy.wait_recv()
        guest_in = pltpu.make_async_copy(gx_hbm, x_st.at[0, pl.ds(0, guest_rows)], x_sem.at[0])
        guest_in.start()
        guest_in.wait()
        h_ref[:guest_rows, :] = normed(x_st[0, :guest_rows])
        cos, sin = [jnp.concatenate([gtab[k, g] for g in range(GUESTS)], axis=1) for k in range(2)]
        keep_kv(h_ref[:guest_rows, :], cos, sin, n_seq)
        for part in range(2):
            keep_q(h_ref[:guest_rows, :], cos, sin, n_seq, part * q_rows)

    wo_copy = pltpu.make_async_copy(wo_hbm, w_ref, wo_sem)
    wo_copy.start()
    guest_turns = jnp.where(chip == 0, GUESTS // 2, 0)
    steps = jnp.where(chip == 0, n_seq + GUESTS, jnp.where(chip == last_chip, kept, n_seq))

    def xr_start(turn):
        @pl.when(turn < guest_turns)
        def _():
            pltpu.make_async_copy(gx_hbm.at[pl.ds(turn * 2 * TOK, 2 * TOK), :], xr_ref.at[turn % 2], xr_sem.at[turn % 2]).start()

        @pl.when(turn >= guest_turns)
        def _():
            pltpu.make_async_copy(x_hbm.at[pl.ds((turn - guest_turns) * 2 * TOK, 2 * TOK), :], xr_ref.at[turn % 2], xr_sem.at[turn % 2]).start()

    def xr_wait(turn):
        pltpu.make_async_copy(x_hbm.at[pl.ds(0, 2 * TOK), :], xr_ref.at[turn % 2], xr_sem.at[turn % 2]).wait()

    def y_copy(turn, row):
        return pltpu.make_async_copy(y_st.at[turn % 2], y_hbm.at[pl.ds(row, 2 * TOK), :], y_sem.at[turn % 2])

    def guest_y(turn):
        return pltpu.make_async_remote_copy(
            src_ref=gy_st, dst_ref=y_hbm.at[pl.ds((kept + 2 * turn) * TOK, 2 * TOK), :], send_sem=gy_sem.at[0, turn],
            recv_sem=gy_sem.at[1, turn], device_id={'cp': 2 * last_chip + core}, device_id_type=MESH)

    xr_start(jnp.int32(0))
    xr_start(jnp.int32(1))

    def load(seq, a):
        return pltpu.make_async_copy(kv_hbm.at[seq, a], slot_ref.at[seq % 2, 2 * a + core], load_sem.at[seq % 2, a])

    def share(seq, a, src):
        return pltpu.make_async_remote_copy(
            src_ref=src, dst_ref=slot_ref.at[seq % 2, 2 * a + core], send_sem=sib_send.at[seq % 2, a],
            recv_sem=sib_recv.at[seq % 2, a], device_id={'cp': sibling}, device_id_type=MESH)

    def reuse(step, shares):
        pl.semaphore_wait(credit, 1)
        for a in range(shares):
            share(step, a, kv_st.at[0]).wait_send()

    def stage(c, seq):
        if c == 0:
            @pl.when(seq < GUESTS)
            def _():
                reuse(seq, last_chip + 1)

            @pl.when(seq >= GUESTS)
            def _():
                reuse(seq, 1)
        else:
            @pl.when(seq >= 2)
            def _():
                reuse(seq, c + 1)

        share(seq, c, kv_st.at[seq]).start()
        slot_ref[seq % 2, 2 * c + core] = kv_st[seq]
        hopped = 1 if c == last_chip else 0
        for a in [hopped] + [a for a in range(c) if a != hopped] if c else []:
            if a != hopped:
                own_send(seq, 0, c, a).wait_recv()
            elif c == last_chip:
                @pl.when(seq >= straight)
                def _():
                    own_send(seq, 0, c, a).wait_recv()
            share(seq, a, kv_hbm.at[seq, a]).start()
            load(seq, a).start()

    def stage_guest(g):
        seq = kept + g

        @pl.when(g == 0)
        def _():
            for k in range(straight, kept):
                own_send(k, 1, 0, 1).wait_recv()
                forward(k, 1, 2).start()

        for a, k in ((0, seq), (last_chip, n_seq + g)):
            share(seq, a, kv_st.at[k]).start()
            slot_ref[seq % 2, 2 * a + core] = kv_st[k]
        for a in range(1, last_chip):
            own_send(seq, 0, 0, a).wait_recv()
            if a == 1:
                forward(seq, 1, 2).start()
            share(seq, a, kv_hbm.at[seq, a]).start()
            load(seq, a).start()

        @pl.when(g == GUESTS - 1)
        def _():
            for chunk in range(n_chunks // 2, n_chunks - 1):
                send_both(chunk)

    def arrived(c, seq):
        for a in range(c):
            load(seq, a).wait()
        for a in range(c + 1):
            share(seq, a, kv_st.at[0]).wait_recv()

    def guest_arrived(g):
        for a in range(1, last_chip):
            load(g, a).wait()
        for a in range(last_chip + 1):
            share(g, a, kv_st.at[0]).wait_recv()

    @pl.when(chip == 0)
    def _():
        stage_guest(0)

    for c in range(1, last_chip + 1):
        @pl.when(chip == c)
        def _():
            stage(c, 0)

    def project_out(turn):
        @pl.when(turn == 0)
        def _():
            wo_copy.wait()

        xr_wait(turn)

        @pl.when((turn >= 2) & (turn - 2 >= guest_turns))
        def _():
            y_copy(turn, 0).wait()

        width = 512
        for col in range(0, dim, width):
            proj = jnp.dot(o_ref[...], w_ref[:, col:col + width], preferred_element_type=F32)
            part = (xr_ref[turn % 2, :, col:col + width].astype(F32) + proj).astype(BF16)
            y_st[turn % 2, :, col:col + width] = part

            @pl.when(turn < guest_turns)
            def _():
                gy_st[:, col:col + width] = part

        @pl.when(turn >= guest_turns)
        def _():
            y_copy(turn, (turn - guest_turns) * 2 * TOK).start()

        @pl.when(turn < guest_turns)
        def _():
            guest_y(0).start()
            send_both(n_chunks - 1)

        @pl.when(turn + 2 < steps // 2)
        def _():
            xr_start(turn + 2)

    buffers = (q_ref, slot_ref, bias_ref, s_ref, m_ref, ot_ref)

    def step(it, carry):
        @pl.when((chip == 0) & (it < GUESTS))
        def _():
            def stage_next():
                @pl.when(it + 1 < GUESTS)
                def _():
                    stage_guest(it + 1)

                @pl.when(it + 1 == GUESTS)
                def _():
                    stage(0, jnp.int32(0))

            def wait_next():
                @pl.when(it + 1 < GUESTS)
                def _():
                    guest_arrived(it + 1)

                @pl.when(it + 1 == GUESTS)
                def _():
                    arrived(0, 0)

            @pl.when(it == 0)
            def _():
                guest_arrived(0)

            attend(*buffers, n_seq + it, n_seq + jnp.minimum(it + 1, GUESTS - 1), it == 0, n_cp, lambda: None, stage_next, wait_next)

        for c in range(last_chip + 1):
            seq = it - GUESTS if c == 0 else it
            last = steps - 1 - (GUESTS if c == 0 else 0)

            @pl.when((chip == c) & (seq >= 0))
            def _():
                if c:
                    @pl.when(seq == 0)
                    def _():
                        arrived(c, seq)

                def stage_next():
                    @pl.when(seq < last)
                    def _():
                        stage(c, seq + 1)

                def pass_on():
                    if c:
                        ahead, end = (LEAD, straight) if c == last_chip else (AHEAD, n_seq)

                        @pl.when(seq + ahead < end)
                        def _():
                            hop(seq + ahead)

                def wait_next():
                    @pl.when(seq < last)
                    def _():
                        arrived(c, seq + 1)

                attend(*buffers, seq, jnp.minimum(seq + 1, last), seq == 0, 2 * (c + 1), pass_on, stage_next, wait_next)

        @pl.when(it + 2 < steps)
        def _():
            pl.semaphore_signal(credit, inc=1, device_id={'cp': sibling}, device_id_type=MESH)

        o_ref[pl.ds(pl.multiple_of(it % 2 * TOK, TOK), TOK), :] = ot_ref[...].T

        @pl.when(it % 2 == 1)
        def _():
            project_out(it // 2)

        return carry

    lax.fori_loop(0, steps, step, 0)

    for turn in range(2):
        y_copy(turn, 0).wait()
    for c in range(last_chip + 1):
        @pl.when(chip == c)
        def _():
            for seq in range(2):
                for a in range(c + 1):
                    share(seq, a, kv_st.at[0]).wait_send()

    @pl.when(chip == 0)
    def _():
        guest_y(0).wait_send()

    @pl.when(chip == last_chip)
    def _():
        for copy in host_copies:
            copy.wait_send()
        for turn in range(GUESTS // 2):
            guest_y(turn).wait_recv()

    def drain(seq, carry):
        @pl.when(chip == 0)
        def _():
            own_send(seq, 0, 1, 0).wait_send()
            own_send(seq, 1, 2, 0).wait_send()

            @pl.when(seq >= straight)
            def _():
                forward(seq, 1, 2).wait_send()

        @pl.when((chip == 1) & (seq >= straight) & (seq < kept))
        def _():
            own_send(seq, 1, 0, 1).wait_send()

        for c in range(1, last_chip):
            @pl.when(chip == c)
            def _():
                own_send(seq, 0, last_chip, c).wait_send()

                @pl.when(forwards(c, seq))
                def _():
                    forward(seq, 0, last_chip).wait_send()

        @pl.when((chip == last_chip) & (seq < straight))
        def _():
            forward(seq, 1, 2).wait_send()

        return carry

    lax.fori_loop(0, n_seq, drain, 0)


def solution(mesh):
    n_cp = mesh.shape['cp']

    def local_block(hidden, positions, norm_gain, w_query, w_key, w_value, w_out):
        batch, tokens, dim = hidden.shape
        kv_rows = 2 * w_key.shape[1]
        rows = batch * tokens
        chips = n_cp // 2
        x = hidden.reshape(rows, dim)
        inv_freq = 10000.0 ** (-2.0 * jnp.arange(HALF, dtype=F32) / HEAD)
        angles = positions.reshape(batch, 1, tokens).astype(F32) * inv_freq[None, :, None]
        hbm = pl.BlockSpec(memory_space=pl.ANY)
        vmem = pl.BlockSpec(memory_space=pltpu.VMEM)
        dma = pltpu.SemaphoreType.DMA
        y, _, _ = pl.pallas_call(
            functools.partial(block_kernel, n_cp),
            out_shape=[jax.ShapeDtypeStruct((rows, dim), BF16), jax.ShapeDtypeStruct((batch, chips - 1, kv_rows, TOK), BF16), jax.ShapeDtypeStruct((GUESTS * TOK, dim), BF16)],
            in_specs=[hbm, vmem, hbm, hbm, hbm, hbm, vmem, vmem],
            out_specs=[hbm, hbm, hbm],
            scratch_shapes=[
                pltpu.VMEM((2, CHUNK, dim), BF16),
                pltpu.VMEM((rows, dim), BF16),
                pltpu.VMEM((2, dim, WBLOCK), BF16),
                pltpu.VMEM((kv_rows, dim), BF16),
                pltpu.VMEM((dim, dim), BF16),
                pltpu.VMEM((batch + GUESTS, kv_rows, TOK), BF16),
                pltpu.VMEM((batch + GUESTS, dim, TOK), BF16),
                pltpu.VMEM((2, n_cp, kv_rows, TOK), BF16),
                pltpu.VMEM((n_cp * TOK, GROUP * TOK), F32),
                pltpu.VMEM((8, GROUP * TOK), F32),
                pltpu.VMEM((2 * TOK, GROUP * TOK), F32),
                pltpu.VMEM((dim, TOK), BF16),
                pltpu.VMEM((2 * TOK, dim), BF16),
                pltpu.VMEM((2, 2 * TOK, dim), BF16),
                pltpu.VMEM((2, 2 * TOK, dim), BF16),
                pltpu.VMEM((1, dim), F32),
                pltpu.VMEM((2, GUESTS, HALF, TOK), F32),
                pltpu.VMEM((GUESTS * TOK, dim), BF16),
                dma((2,)), dma((2,)), dma, dma((batch, chips - 1)), dma((batch, 2)), dma((batch,)),
                dma((2, chips - 1)), dma((2, chips)), dma((2, chips)), dma((2,)), dma((2,)), dma((2, 1)), dma((2, 2)), dma((2, GUESTS // 2)),
                pltpu.SemaphoreType.REGULAR,
            ],
            compiler_params=pltpu.CompilerParams(collective_id=0, has_side_effects=True, vmem_limit_bytes=62 * 2 ** 20),
            name='block',
        )(x, norm_gain.reshape(dim // 128, 128), w_query, w_key, w_value, w_out.reshape(dim, dim), jnp.cos(angles), jnp.sin(angles))
        return y.reshape(batch, tokens, dim)

    act_spec = P('dp', 'cp', None)
    return jax.shard_map(local_block, mesh=mesh, in_specs=(act_spec, P('dp', 'cp'), P(), P(), P(), P(), P()), out_specs=act_spec, check_vma=False)
```

```python
import functools

import jax
import jax.numpy as jnp
from jax import lax
from jax.experimental import pallas as pl
from jax.experimental.pallas import tpu as pltpu
from jax.sharding import PartitionSpec as P

MESH = pl.DeviceIdType.MESH
HEAD = 64
HALF = HEAD // 2
TOK = 128
GROUP = 4
AHEAD = 4
LEAD = 0
GUESTS = 2
ROUND = 4
CHUNK = 4 * TOK
WBLOCK = 256
F32, BF16 = jnp.float32, jnp.bfloat16
NT = (((1,), (1,)), ((), ()))


def rope_rows(x, cos, sin):
    heads, n = x.shape[0] // HEAD, x.shape[1]
    x = x.reshape(heads, 2, HALF, n)
    a, b = x[:, 0], x[:, 1]
    rotated = jnp.stack([a * cos - b * sin, b * cos + a * sin], axis=1)
    return rotated.reshape(heads * HEAD, n)


def attend(q_ref, slot_ref, bias_ref, s_ref, m_ref, o_ref, seq, following, first, n_blocks, pass_on, stage_next, wait_next):
    width = slot_ref.shape[2] // 2
    pairs = width // (2 * HEAD)
    key_chunks = n_blocks // 2
    kc = 2 * TOK
    cols = GROUP * TOK

    def queries(sq, g):
        base = g * GROUP * HEAD
        return jnp.concatenate([q_ref[sq, pl.ds(pl.multiple_of(base + i * HEAD, HEAD), HEAD), :] for i in range(GROUP)], axis=1)

    def scores(q, sq, g, c, peak):
        row = pl.ds(pl.multiple_of(g * HEAD, HEAD), HEAD)
        keys = jnp.concatenate([slot_ref[sq % 2, 2 * c + i, row, :].T for i in range(2)], axis=0)
        s = jnp.dot(keys, q, preferred_element_type=F32)
        if c == key_chunks - 1:
            s = s + bias_ref[...]
        s_ref[c * kc:(c + 1) * kc, :] = s
        top = jnp.max(s.reshape(kc // 8, 8, cols), axis=0)
        return top if peak is None else jnp.maximum(peak, top)

    def unit(g, sq_next, g_next, peak):
        peak = jnp.max(peak, axis=0, keepdims=True)
        q_next = queries(sq_next, g_next)
        vrow = pl.ds(pl.multiple_of(width + g * HEAD, HEAD), HEAD)
        total, out, peak_next = None, None, None
        for c in range(key_chunks):
            prob = jnp.exp(s_ref[c * kc:(c + 1) * kc, :] - peak)
            part = jnp.sum(prob.reshape(kc // 8, 8, cols), axis=0)
            total = part if total is None else total + part
            values = jnp.concatenate([slot_ref[seq % 2, 2 * c + i, vrow, :] for i in range(2)], axis=1)
            term = jnp.dot(values, prob.astype(BF16), preferred_element_type=F32)
            out = term if out is None else out + term
            peak_next = scores(q_next, sq_next, g_next, c, peak_next)
        out = out / jnp.sum(total, axis=0, keepdims=True)
        for i in range(GROUP):
            o_ref[pl.ds(pl.multiple_of((g * GROUP + i) * HEAD, HEAD), HEAD), :] = out[:, i * TOK:(i + 1) * TOK].astype(BF16)
        return peak_next

    @pl.when(first)
    def _():
        q_first, peak = queries(seq, 0), None
        for c in range(key_chunks):
            peak = scores(q_first, seq, 0, c, peak)
        m_ref[...] = peak

    def pair(j, carry):
        @pl.when(j == 0)
        def _():
            pass_on()

        @pl.when(j == 1)
        def _():
            stage_next()

        last = j == pairs - 1

        @pl.when(last)
        def _():
            wait_next()

        sq_next = jnp.where(last, following, seq)
        g_next = jnp.where(last, 0, 2 * j + 2)
        peak = unit(2 * j, seq, 2 * j + 1, m_ref[...])
        m_ref[...] = unit(2 * j + 1, sq_next, g_next, peak)
        return carry

    lax.fori_loop(0, pairs, pair, 0)


def block_kernel(
    n_cp, x_hbm, gain_ref, wq_hbm, wk_hbm, wv_hbm, wo_hbm, cos_ref, sin_ref, y_hbm, kv_hbm, gx_hbm,
    x_st, h_ref, w_st, wkv_ref, w_ref, kv_st, q_ref, slot_ref, s_ref, m_ref, bias_ref, ot_ref, o_ref, xr_ref, y_st, gain_row, gtab, gy_st,
    x_sem, w_sem, wo_sem, recv_sem, own_sem, fwd_sem, load_sem, sib_recv, sib_send, xr_sem, y_sem, gx_sem, gt_sem, gy_sem, credit,
):
    me = lax.axis_index('cp')
    chip, core = me // 2, me % 2
    sibling = me + 1 - 2 * core
    n_seq = cos_ref.shape[0]
    kept = n_seq - GUESTS
    guest_rows = GUESTS * TOK
    straight = n_seq - ROUND
    dim = x_st.shape[2]
    kv_rows = wkv_ref.shape[0]
    n_chunks = n_seq * TOK // CHUNK
    seqs = CHUNK // TOK
    last_chip = n_cp // 2 - 1

    barrier = pltpu.get_barrier_semaphore()
    for step in range(1, n_cp):
        pl.semaphore_signal(barrier, inc=1, device_id={'cp': (me + step) % n_cp}, device_id_type=MESH)

    def x_copy(chunk):
        return pltpu.make_async_copy(x_hbm.at[pl.ds(chunk * CHUNK, CHUNK), :], x_st.at[chunk % 2], x_sem.at[chunk % 2])

    def w_copy(hbm, block, slot):
        return pltpu.make_async_copy(hbm.at[:, pl.ds(block * WBLOCK, WBLOCK)], w_st.at[slot], w_sem.at[slot])

    kv_blocks = [(wk_hbm, i) for i in range(kv_rows // 2 // WBLOCK)] + [(wv_hbm, i) for i in range(kv_rows // 2 // WBLOCK)]
    q_blocks = dim // WBLOCK
    x_copy(0).start()
    for i in range(2):
        w_copy(*kv_blocks[i], i).start()
    x_copy(1).start()

    key = lax.broadcasted_iota(jnp.int32, (2 * TOK, TOK), 0)
    tok = lax.broadcasted_iota(jnp.int32, (2 * TOK, TOK), 1)
    bias = jnp.where(key <= tok + core * TOK, 0.0, -jnp.inf).astype(F32)
    bias_ref[...] = jnp.concatenate([bias] * GROUP, axis=1)

    gain = gain_ref[...].astype(F32)
    for i in range(gain.shape[0]):
        gain_row[:, i * gain.shape[1]:(i + 1) * gain.shape[1]] = gain[i:i + 1]

    def tables(chunk):
        return [jnp.concatenate([t[chunk * seqs + i] for i in range(seqs)], axis=1) for t in (cos_ref, sin_ref)]

    for i, (hbm, block) in enumerate(kv_blocks):
        w_copy(hbm, block, i % 2).wait()
        wkv_ref[i * WBLOCK:(i + 1) * WBLOCK, :] = w_st[i % 2].T
        nxt = i + 2
        if nxt < len(kv_blocks):
            w_copy(*kv_blocks[nxt], i % 2).start()
        else:
            w_copy(wq_hbm, nxt - len(kv_blocks), i % 2).start()

    def own_send(seq, target, to_chip, from_chip):
        return pltpu.make_async_remote_copy(
            src_ref=kv_st.at[seq], dst_ref=kv_hbm.at[seq, from_chip], send_sem=own_sem.at[seq, target],
            recv_sem=recv_sem.at[seq, from_chip], device_id={'cp': 2 * to_chip + core}, device_id_type=MESH)

    def forward(seq, block, to_chip):
        return pltpu.make_async_remote_copy(
            src_ref=kv_hbm.at[seq, block], dst_ref=kv_hbm.at[seq, block], send_sem=fwd_sem.at[seq],
            recv_sem=recv_sem.at[seq, block], device_id={'cp': 2 * to_chip + core}, device_id_type=MESH)

    def to_host(src, dst, sems, k):
        return pltpu.make_async_remote_copy(
            src_ref=src, dst_ref=dst, send_sem=sems.at[0, k], recv_sem=sems.at[1, k], device_id={'cp': core}, device_id_type=MESH)

    host_copies = [
        to_host(cos_ref.at[pl.ds(kept, GUESTS)], gtab.at[0], gt_sem, 0),
        to_host(sin_ref.at[pl.ds(kept, GUESTS)], gtab.at[1], gt_sem, 1),
        to_host(x_hbm.at[pl.ds(kept * TOK, guest_rows), :], gx_hbm, gx_sem, 0),
    ]
    pl.semaphore_wait(barrier, n_cp - 1)

    @pl.when(chip == last_chip)
    def _():
        for copy in host_copies:
            copy.start()

    def normed(x):
        x = x.astype(F32)
        inv_rms = lax.rsqrt(jnp.mean(x * x, axis=-1, keepdims=True) + 1e-5)
        return (x * inv_rms * gain_row[...]).astype(BF16)

    def keep_kv(h, cos, sin, first):
        kv = lax.dot_general(wkv_ref[...], h, NT, preferred_element_type=F32)
        k = rope_rows(kv[:kv_rows // 2], cos, sin).astype(BF16)
        v = kv[kv_rows // 2:].astype(BF16)
        for i in range(h.shape[0] // TOK):
            kv_st[first + i, :kv_rows // 2, :] = k[:, i * TOK:(i + 1) * TOK]
            kv_st[first + i, kv_rows // 2:, :] = v[:, i * TOK:(i + 1) * TOK]

    def keep_q(h, cos, sin, first, base):
        q = lax.dot_general(w_ref[pl.ds(base, q_rows), :], h, NT, preferred_element_type=F32)
        q = (rope_rows(q, cos, sin) * (HEAD ** -0.5)).astype(BF16)
        for i in range(h.shape[0] // TOK):
            q_ref[first + i, pl.ds(base, q_rows), :] = q[:, i * TOK:(i + 1) * TOK]

    q_rows = dim // 2

    def send_both(chunk):
        for i in range(seqs):
            own_send(chunk * seqs + i, 0, 1, 0).start()
            own_send(chunk * seqs + i, 1, 2, 0).start()

    def project_kv(chunk, carry):
        x_copy(chunk).wait()
        rows = pl.ds(pl.multiple_of(chunk * CHUNK, CHUNK), CHUNK)
        h_ref[rows, :] = normed(x_st[chunk % 2])

        @pl.when(chunk + 2 < n_chunks)
        def _():
            x_copy(chunk + 2).start()

        keep_kv(h_ref[rows, :], *tables(chunk), chunk * seqs)

        @pl.when((chip == 0) & (chunk < n_chunks // 2))
        def _():
            send_both(chunk)

        for c in range(1, last_chip):
            @pl.when((chip == c) & (chunk == 0))
            def _():
                for i in range(AHEAD):
                    own_send(i, 0, last_chip, c).start()

            @pl.when((chip == c) & (chunk == n_chunks - 1))
            def _():
                for i in range(kept, n_seq):
                    own_send(i, 0, 0, c).start()
                if c == 1:
                    for i in range(straight, kept):
                        own_send(i, 1, 0, c).start()

        return carry

    lax.fori_loop(0, n_chunks, project_kv, 0)

    def turn_wq(i, carry):
        for k in range(2):
            w_copy(wq_hbm, 2 * i + k, k).wait()
            w_ref[pl.ds(pl.multiple_of((2 * i + k) * WBLOCK, WBLOCK), WBLOCK), :] = w_st[k].T

            @pl.when(2 * i + k + 2 < q_blocks)
            def _():
                w_copy(wq_hbm, 2 * i + k + 2, k).start()

        return carry

    lax.fori_loop(0, q_blocks // 2, turn_wq, 0)

    def forwards(c, seq):
        by_second = (core == 1) | (seq % 4 == 3)
        return (seq < kept) & (by_second if c == 2 else jnp.logical_not(by_second))

    def hop(seq):
        for c in range(1, last_chip):
            @pl.when(chip == c)
            def _():
                own_send(seq, 0, c, 0).wait_recv()

                @pl.when(forwards(c, seq))
                def _():
                    forward(seq, 0, last_chip).start()

                @pl.when((seq + LEAD >= AHEAD) & (seq + LEAD < kept))
                def _():
                    own_send(seq + LEAD, 0, last_chip, c).start()

        @pl.when(chip == last_chip)
        def _():
            own_send(seq, 0, last_chip, 1).wait_recv()
            forward(seq, 1, 2).start()

    def project_q(i, carry):
        chunk, part = i // 2, i % 2
        h = h_ref[pl.ds(pl.multiple_of(chunk * CHUNK, CHUNK), CHUNK), :]
        keep_q(h, *tables(chunk), chunk * seqs, pl.multiple_of(part * q_rows, q_rows))

        @pl.when((part == 1) & ((chip < last_chip) | (chunk < 1)))
        def _():
            hop(chunk)

        return carry

    lax.fori_loop(0, 2 * n_chunks, project_q, 0)

    @pl.when(chip == 0)
    def _():
        for copy in host_copies:
            copy.wait_recv()
        guest_in = pltpu.make_async_copy(gx_hbm, x_st.at[0, pl.ds(0, guest_rows)], x_sem.at[0])
        guest_in.start()
        guest_in.wait()
        h_ref[:guest_rows, :] = normed(x_st[0, :guest_rows])
        cos, sin = [jnp.concatenate([gtab[k, g] for g in range(GUESTS)], axis=1) for k in range(2)]
        keep_kv(h_ref[:guest_rows, :], cos, sin, n_seq)
        for part in range(2):
            keep_q(h_ref[:guest_rows, :], cos, sin, n_seq, part * q_rows)

    wo_copy = pltpu.make_async_copy(wo_hbm, w_ref, wo_sem)
    wo_copy.start()
    guest_turns = jnp.where(chip == 0, GUESTS // 2, 0)
    steps = jnp.where(chip == 0, n_seq + GUESTS, jnp.where(chip == last_chip, kept, n_seq))

    def xr_start(turn):
        @pl.when(turn < guest_turns)
        def _():
            pltpu.make_async_copy(gx_hbm.at[pl.ds(turn * 2 * TOK, 2 * TOK), :], xr_ref.at[turn % 2], xr_sem.at[turn % 2]).start()

        @pl.when(turn >= guest_turns)
        def _():
            pltpu.make_async_copy(x_hbm.at[pl.ds((turn - guest_turns) * 2 * TOK, 2 * TOK), :], xr_ref.at[turn % 2], xr_sem.at[turn % 2]).start()

    def xr_wait(turn):
        pltpu.make_async_copy(x_hbm.at[pl.ds(0, 2 * TOK), :], xr_ref.at[turn % 2], xr_sem.at[turn % 2]).wait()

    def y_copy(turn, row):
        return pltpu.make_async_copy(y_st.at[turn % 2], y_hbm.at[pl.ds(row, 2 * TOK), :], y_sem.at[turn % 2])

    def guest_y(turn):
        return pltpu.make_async_remote_copy(
            src_ref=gy_st, dst_ref=y_hbm.at[pl.ds((kept + 2 * turn) * TOK, 2 * TOK), :], send_sem=gy_sem.at[0, turn],
            recv_sem=gy_sem.at[1, turn], device_id={'cp': 2 * last_chip + core}, device_id_type=MESH)

    xr_start(jnp.int32(0))
    xr_start(jnp.int32(1))

    def load(seq, a):
        return pltpu.make_async_copy(kv_hbm.at[seq, a], slot_ref.at[seq % 2, 2 * a + core], load_sem.at[seq % 2, a])

    def share(seq, a, src):
        return pltpu.make_async_remote_copy(
            src_ref=src, dst_ref=slot_ref.at[seq % 2, 2 * a + core], send_sem=sib_send.at[seq % 2, a],
            recv_sem=sib_recv.at[seq % 2, a], device_id={'cp': sibling}, device_id_type=MESH)

    def reuse(step, shares):
        pl.semaphore_wait(credit, 1)
        for a in range(shares):
            share(step, a, kv_st.at[0]).wait_send()

    def stage(c, seq):
        if c == 0:
            @pl.when(seq < GUESTS)
            def _():
                reuse(seq, last_chip + 1)

            @pl.when(seq >= GUESTS)
            def _():
                reuse(seq, 1)
        else:
            @pl.when(seq >= 2)
            def _():
                reuse(seq, c + 1)

        share(seq, c, kv_st.at[seq]).start()
        slot_ref[seq % 2, 2 * c + core] = kv_st[seq]
        hopped = 1 if c == last_chip else 0
        for a in [hopped] + [a for a in range(c) if a != hopped] if c else []:
            if a != hopped:
                own_send(seq, 0, c, a).wait_recv()
            elif c == last_chip:
                @pl.when(seq >= straight)
                def _():
                    own_send(seq, 0, c, a).wait_recv()
            share(seq, a, kv_hbm.at[seq, a]).start()
            load(seq, a).start()

    def stage_guest(g):
        seq = kept + g

        @pl.when(g == 0)
        def _():
            for k in range(straight, kept):
                own_send(k, 1, 0, 1).wait_recv()
                forward(k, 1, 2).start()

        for a, k in ((0, seq), (last_chip, n_seq + g)):
            share(seq, a, kv_st.at[k]).start()
            slot_ref[seq % 2, 2 * a + core] = kv_st[k]
        for a in range(1, last_chip):
            own_send(seq, 0, 0, a).wait_recv()
            if a == 1:
                forward(seq, 1, 2).start()
            share(seq, a, kv_hbm.at[seq, a]).start()
            load(seq, a).start()

        @pl.when(g == GUESTS - 1)
        def _():
            for chunk in range(n_chunks // 2, n_chunks - 1):
                send_both(chunk)

    def arrived(c, seq):
        for a in range(c):
            load(seq, a).wait()
        for a in range(c + 1):
            share(seq, a, kv_st.at[0]).wait_recv()

    def guest_arrived(g):
        for a in range(1, last_chip):
            load(g, a).wait()
        for a in range(last_chip + 1):
            share(g, a, kv_st.at[0]).wait_recv()

    @pl.when(chip == 0)
    def _():
        stage_guest(0)

    for c in range(1, last_chip + 1):
        @pl.when(chip == c)
        def _():
            stage(c, 0)

    def project_out(turn):
        @pl.when(turn == 0)
        def _():
            wo_copy.wait()

        xr_wait(turn)

        @pl.when((turn >= 2) & (turn - 2 >= guest_turns))
        def _():
            y_copy(turn, 0).wait()

        width = 512
        for col in range(0, dim, width):
            proj = jnp.dot(o_ref[...], w_ref[:, col:col + width], preferred_element_type=F32)
            part = (xr_ref[turn % 2, :, col:col + width].astype(F32) + proj).astype(BF16)
            y_st[turn % 2, :, col:col + width] = part

            @pl.when(turn < guest_turns)
            def _():
                gy_st[:, col:col + width] = part

        @pl.when(turn >= guest_turns)
        def _():
            y_copy(turn, (turn - guest_turns) * 2 * TOK).start()

        @pl.when(turn < guest_turns)
        def _():
            guest_y(0).start()
            send_both(n_chunks - 1)

        @pl.when(turn + 2 < steps // 2)
        def _():
            xr_start(turn + 2)

    buffers = (q_ref, slot_ref, bias_ref, s_ref, m_ref, ot_ref)

    def step(it, carry):
        @pl.when((chip == 0) & (it < GUESTS))
        def _():
            def stage_next():
                @pl.when(it + 1 < GUESTS)
                def _():
                    stage_guest(it + 1)

                @pl.when(it + 1 == GUESTS)
                def _():
                    stage(0, jnp.int32(0))

            def wait_next():
                @pl.when(it + 1 < GUESTS)
                def _():
                    guest_arrived(it + 1)

                @pl.when(it + 1 == GUESTS)
                def _():
                    arrived(0, 0)

            @pl.when(it == 0)
            def _():
                guest_arrived(0)

            attend(*buffers, n_seq + it, n_seq + jnp.minimum(it + 1, GUESTS - 1), it == 0, n_cp, lambda: None, stage_next, wait_next)

        for c in range(last_chip + 1):
            seq = it - GUESTS if c == 0 else it
            last = steps - 1 - (GUESTS if c == 0 else 0)

            @pl.when((chip == c) & (seq >= 0))
            def _():
                if c:
                    @pl.when(seq == 0)
                    def _():
                        arrived(c, seq)

                def stage_next():
                    if c == last_chip:
                        @pl.when(seq + 1 < straight)
                        def _():
                            hop(seq + 1)

                    @pl.when(seq < last)
                    def _():
                        stage(c, seq + 1)

                def pass_on():
                    if 0 < c < last_chip:
                        @pl.when(seq + AHEAD < n_seq)
                        def _():
                            hop(seq + AHEAD)

                def wait_next():
                    @pl.when(seq < last)
                    def _():
                        arrived(c, seq + 1)

                attend(*buffers, seq, jnp.minimum(seq + 1, last), seq == 0, 2 * (c + 1), pass_on, stage_next, wait_next)

        @pl.when(it + 2 < steps)
        def _():
            pl.semaphore_signal(credit, inc=1, device_id={'cp': sibling}, device_id_type=MESH)

        o_ref[pl.ds(pl.multiple_of(it % 2 * TOK, TOK), TOK), :] = ot_ref[...].T

        @pl.when(it % 2 == 1)
        def _():
            project_out(it // 2)

        return carry

    lax.fori_loop(0, steps, step, 0)

    for turn in range(2):
        y_copy(turn, 0).wait()
    for c in range(last_chip + 1):
        @pl.when(chip == c)
        def _():
            for seq in range(2):
                for a in range(c + 1):
                    share(seq, a, kv_st.at[0]).wait_send()

    @pl.when(chip == 0)
    def _():
        guest_y(0).wait_send()

    @pl.when(chip == last_chip)
    def _():
        for copy in host_copies:
            copy.wait_send()
        for turn in range(GUESTS // 2):
            guest_y(turn).wait_recv()

    def drain(seq, carry):
        @pl.when(chip == 0)
        def _():
            own_send(seq, 0, 1, 0).wait_send()
            own_send(seq, 1, 2, 0).wait_send()

            @pl.when(seq >= straight)
            def _():
                forward(seq, 1, 2).wait_send()

        @pl.when((chip == 1) & (seq >= straight) & (seq < kept))
        def _():
            own_send(seq, 1, 0, 1).wait_send()

        for c in range(1, last_chip):
            @pl.when(chip == c)
            def _():
                own_send(seq, 0, last_chip, c).wait_send()

                @pl.when(forwards(c, seq))
                def _():
                    forward(seq, 0, last_chip).wait_send()

        @pl.when((chip == last_chip) & (seq < straight))
        def _():
            forward(seq, 1, 2).wait_send()

        return carry

    lax.fori_loop(0, n_seq, drain, 0)


def solution(mesh):
    n_cp = mesh.shape['cp']

    def local_block(hidden, positions, norm_gain, w_query, w_key, w_value, w_out):
        batch, tokens, dim = hidden.shape
        kv_rows = 2 * w_key.shape[1]
        rows = batch * tokens
        chips = n_cp // 2
        x = hidden.reshape(rows, dim)
        inv_freq = 10000.0 ** (-2.0 * jnp.arange(HALF, dtype=F32) / HEAD)
        angles = positions.reshape(batch, 1, tokens).astype(F32) * inv_freq[None, :, None]
        hbm = pl.BlockSpec(memory_space=pl.ANY)
        vmem = pl.BlockSpec(memory_space=pltpu.VMEM)
        dma = pltpu.SemaphoreType.DMA
        y, _, _ = pl.pallas_call(
            functools.partial(block_kernel, n_cp),
            out_shape=[jax.ShapeDtypeStruct((rows, dim), BF16), jax.ShapeDtypeStruct((batch, chips - 1, kv_rows, TOK), BF16), jax.ShapeDtypeStruct((GUESTS * TOK, dim), BF16)],
            in_specs=[hbm, vmem, hbm, hbm, hbm, hbm, vmem, vmem],
            out_specs=[hbm, hbm, hbm],
            scratch_shapes=[
                pltpu.VMEM((2, CHUNK, dim), BF16),
                pltpu.VMEM((rows, dim), BF16),
                pltpu.VMEM((2, dim, WBLOCK), BF16),
                pltpu.VMEM((kv_rows, dim), BF16),
                pltpu.VMEM((dim, dim), BF16),
                pltpu.VMEM((batch + GUESTS, kv_rows, TOK), BF16),
                pltpu.VMEM((batch + GUESTS, dim, TOK), BF16),
                pltpu.VMEM((2, n_cp, kv_rows, TOK), BF16),
                pltpu.VMEM((n_cp * TOK, GROUP * TOK), F32),
                pltpu.VMEM((8, GROUP * TOK), F32),
                pltpu.VMEM((2 * TOK, GROUP * TOK), F32),
                pltpu.VMEM((dim, TOK), BF16),
                pltpu.VMEM((2 * TOK, dim), BF16),
                pltpu.VMEM((2, 2 * TOK, dim), BF16),
                pltpu.VMEM((2, 2 * TOK, dim), BF16),
                pltpu.VMEM((1, dim), F32),
                pltpu.VMEM((2, GUESTS, HALF, TOK), F32),
                pltpu.VMEM((GUESTS * TOK, dim), BF16),
                dma((2,)), dma((2,)), dma, dma((batch, chips - 1)), dma((batch, 2)), dma((batch,)),
                dma((2, chips - 1)), dma((2, chips)), dma((2, chips)), dma((2,)), dma((2,)), dma((2, 1)), dma((2, 2)), dma((2, GUESTS // 2)),
                pltpu.SemaphoreType.REGULAR,
            ],
            compiler_params=pltpu.CompilerParams(collective_id=0, has_side_effects=True, vmem_limit_bytes=62 * 2 ** 20),
            name='block',
        )(x, norm_gain.reshape(dim // 128, 128), w_query, w_key, w_value, w_out.reshape(dim, dim), jnp.cos(angles), jnp.sin(angles))
        return y.reshape(batch, tokens, dim)

    act_spec = P('dp', 'cp', None)
    return jax.shard_map(local_block, mesh=mesh, in_specs=(act_spec, P('dp', 'cp'), P(), P(), P(), P(), P()), out_specs=act_spec, check_vma=False)
```

```python
import functools

import jax
import jax.numpy as jnp
from jax import lax
from jax.experimental import pallas as pl
from jax.experimental.pallas import tpu as pltpu
from jax.sharding import PartitionSpec as P

MESH = pl.DeviceIdType.MESH
HEAD = 64
HALF = HEAD // 2
TOK = 128
GROUP = 4
AHEAD = 4
LEAD = 1
GUESTS = 2
ROUND = 4
CHUNK = 4 * TOK
WBLOCK = 256
F32, BF16 = jnp.float32, jnp.bfloat16
NT = (((1,), (1,)), ((), ()))


def rope_rows(x, cos, sin):
    heads, n = x.shape[0] // HEAD, x.shape[1]
    x = x.reshape(heads, 2, HALF, n)
    a, b = x[:, 0], x[:, 1]
    rotated = jnp.stack([a * cos - b * sin, b * cos + a * sin], axis=1)
    return rotated.reshape(heads * HEAD, n)


def attend(q_ref, slot_ref, bias_ref, s_ref, m_ref, o_ref, seq, following, first, n_blocks, pass_on, stage_next, wait_next):
    width = slot_ref.shape[2] // 2
    pairs = width // (2 * HEAD)
    key_chunks = n_blocks // 2
    kc = 2 * TOK
    cols = GROUP * TOK

    def queries(sq, g):
        base = g * GROUP * HEAD
        return jnp.concatenate([q_ref[sq, pl.ds(pl.multiple_of(base + i * HEAD, HEAD), HEAD), :] for i in range(GROUP)], axis=1)

    def scores(q, sq, g, c, peak):
        row = pl.ds(pl.multiple_of(g * HEAD, HEAD), HEAD)
        keys = jnp.concatenate([slot_ref[sq % 2, 2 * c + i, row, :].T for i in range(2)], axis=0)
        s = jnp.dot(keys, q, preferred_element_type=F32)
        if c == key_chunks - 1:
            s = s + bias_ref[...]
        s_ref[c * kc:(c + 1) * kc, :] = s
        top = jnp.max(s.reshape(kc // 8, 8, cols), axis=0)
        return top if peak is None else jnp.maximum(peak, top)

    def unit(g, sq_next, g_next, peak):
        peak = jnp.max(peak, axis=0, keepdims=True)
        q_next = queries(sq_next, g_next)
        vrow = pl.ds(pl.multiple_of(width + g * HEAD, HEAD), HEAD)
        total, out, peak_next = None, None, None
        for c in range(key_chunks):
            prob = jnp.exp(s_ref[c * kc:(c + 1) * kc, :] - peak)
            part = jnp.sum(prob.reshape(kc // 8, 8, cols), axis=0)
            total = part if total is None else total + part
            values = jnp.concatenate([slot_ref[seq % 2, 2 * c + i, vrow, :] for i in range(2)], axis=1)
            term = jnp.dot(values, prob.astype(BF16), preferred_element_type=F32)
            out = term if out is None else out + term
            peak_next = scores(q_next, sq_next, g_next, c, peak_next)
        out = out / jnp.sum(total, axis=0, keepdims=True)
        for i in range(GROUP):
            o_ref[pl.ds(pl.multiple_of((g * GROUP + i) * HEAD, HEAD), HEAD), :] = out[:, i * TOK:(i + 1) * TOK].astype(BF16)
        return peak_next

    @pl.when(first)
    def _():
        q_first, peak = queries(seq, 0), None
        for c in range(key_chunks):
            peak = scores(q_first, seq, 0, c, peak)
        m_ref[...] = peak

    def pair(j, carry):
        @pl.when(j == 0)
        def _():
            pass_on()

        @pl.when(j == 1)
        def _():
            stage_next()

        last = j == pairs - 1

        @pl.when(last)
        def _():
            wait_next()

        sq_next = jnp.where(last, following, seq)
        g_next = jnp.where(last, 0, 2 * j + 2)
        peak = unit(2 * j, seq, 2 * j + 1, m_ref[...])
        m_ref[...] = unit(2 * j + 1, sq_next, g_next, peak)
        return carry

    lax.fori_loop(0, pairs, pair, 0)


def block_kernel(
    n_cp, x_hbm, gain_ref, wq_hbm, wk_hbm, wv_hbm, wo_hbm, cos_ref, sin_ref, y_hbm, kv_hbm, gx_hbm,
    x_st, h_ref, w_st, wkv_ref, w_ref, kv_st, q_ref, slot_ref, s_ref, m_ref, bias_ref, ot_ref, o_ref, xr_ref, y_st, gain_row, gtab, gy_st,
    x_sem, w_sem, wo_sem, recv_sem, own_sem, fwd_sem, load_sem, sib_recv, sib_send, xr_sem, y_sem, gx_sem, gt_sem, gy_sem, credit,
):
    me = lax.axis_index('cp')
    chip, core = me // 2, me % 2
    sibling = me + 1 - 2 * core
    n_seq = cos_ref.shape[0]
    kept = n_seq - GUESTS
    guest_rows = GUESTS * TOK
    straight = n_seq - ROUND
    dim = x_st.shape[2]
    kv_rows = wkv_ref.shape[0]
    n_chunks = n_seq * TOK // CHUNK
    seqs = CHUNK // TOK
    last_chip = n_cp // 2 - 1

    barrier = pltpu.get_barrier_semaphore()
    for step in range(1, n_cp):
        pl.semaphore_signal(barrier, inc=1, device_id={'cp': (me + step) % n_cp}, device_id_type=MESH)

    def x_copy(chunk):
        return pltpu.make_async_copy(x_hbm.at[pl.ds(chunk * CHUNK, CHUNK), :], x_st.at[chunk % 2], x_sem.at[chunk % 2])

    def w_copy(hbm, block, slot):
        return pltpu.make_async_copy(hbm.at[:, pl.ds(block * WBLOCK, WBLOCK)], w_st.at[slot], w_sem.at[slot])

    kv_blocks = [(wk_hbm, i) for i in range(kv_rows // 2 // WBLOCK)] + [(wv_hbm, i) for i in range(kv_rows // 2 // WBLOCK)]
    q_blocks = dim // WBLOCK
    x_copy(0).start()
    for i in range(2):
        w_copy(*kv_blocks[i], i).start()
    x_copy(1).start()

    key = lax.broadcasted_iota(jnp.int32, (2 * TOK, TOK), 0)
    tok = lax.broadcasted_iota(jnp.int32, (2 * TOK, TOK), 1)
    bias = jnp.where(key <= tok + core * TOK, 0.0, -jnp.inf).astype(F32)
    bias_ref[...] = jnp.concatenate([bias] * GROUP, axis=1)

    gain = gain_ref[...].astype(F32)
    for i in range(gain.shape[0]):
        gain_row[:, i * gain.shape[1]:(i + 1) * gain.shape[1]] = gain[i:i + 1]

    def tables(chunk):
        return [jnp.concatenate([t[chunk * seqs + i] for i in range(seqs)], axis=1) for t in (cos_ref, sin_ref)]

    for i, (hbm, block) in enumerate(kv_blocks):
        w_copy(hbm, block, i % 2).wait()
        wkv_ref[i * WBLOCK:(i + 1) * WBLOCK, :] = w_st[i % 2].T
        nxt = i + 2
        if nxt < len(kv_blocks):
            w_copy(*kv_blocks[nxt], i % 2).start()
        else:
            w_copy(wq_hbm, nxt - len(kv_blocks), i % 2).start()

    def own_send(seq, target, to_chip, from_chip):
        return pltpu.make_async_remote_copy(
            src_ref=kv_st.at[seq], dst_ref=kv_hbm.at[seq, from_chip], send_sem=own_sem.at[seq, target],
            recv_sem=recv_sem.at[seq, from_chip], device_id={'cp': 2 * to_chip + core}, device_id_type=MESH)

    def forward(seq, block, to_chip):
        return pltpu.make_async_remote_copy(
            src_ref=kv_hbm.at[seq, block], dst_ref=kv_hbm.at[seq, block], send_sem=fwd_sem.at[seq],
            recv_sem=recv_sem.at[seq, block], device_id={'cp': 2 * to_chip + core}, device_id_type=MESH)

    def to_host(src, dst, sems, k):
        return pltpu.make_async_remote_copy(
            src_ref=src, dst_ref=dst, send_sem=sems.at[0, k], recv_sem=sems.at[1, k], device_id={'cp': core}, device_id_type=MESH)

    host_copies = [
        to_host(cos_ref.at[pl.ds(kept, GUESTS)], gtab.at[0], gt_sem, 0),
        to_host(sin_ref.at[pl.ds(kept, GUESTS)], gtab.at[1], gt_sem, 1),
        to_host(x_hbm.at[pl.ds(kept * TOK, guest_rows), :], gx_hbm, gx_sem, 0),
    ]
    pl.semaphore_wait(barrier, n_cp - 1)

    @pl.when(chip == last_chip)
    def _():
        for copy in host_copies:
            copy.start()

    def normed(x):
        x = x.astype(F32)
        inv_rms = lax.rsqrt(jnp.mean(x * x, axis=-1, keepdims=True) + 1e-5)
        return (x * inv_rms * gain_row[...]).astype(BF16)

    def keep_kv(h, cos, sin, first):
        kv = lax.dot_general(wkv_ref[...], h, NT, preferred_element_type=F32)
        k = rope_rows(kv[:kv_rows // 2], cos, sin).astype(BF16)
        v = kv[kv_rows // 2:].astype(BF16)
        for i in range(h.shape[0] // TOK):
            kv_st[first + i, :kv_rows // 2, :] = k[:, i * TOK:(i + 1) * TOK]
            kv_st[first + i, kv_rows // 2:, :] = v[:, i * TOK:(i + 1) * TOK]

    def keep_q(h, cos, sin, first, base):
        q = lax.dot_general(w_ref[pl.ds(base, q_rows), :], h, NT, preferred_element_type=F32)
        q = (rope_rows(q, cos, sin) * (HEAD ** -0.5)).astype(BF16)
        for i in range(h.shape[0] // TOK):
            q_ref[first + i, pl.ds(base, q_rows), :] = q[:, i * TOK:(i + 1) * TOK]

    q_rows = dim // 2

    def send_both(chunk):
        for i in range(seqs):
            own_send(chunk * seqs + i, 0, 1, 0).start()
            own_send(chunk * seqs + i, 1, 2, 0).start()

    def project_kv(chunk, carry):
        x_copy(chunk).wait()
        rows = pl.ds(pl.multiple_of(chunk * CHUNK, CHUNK), CHUNK)
        h_ref[rows, :] = normed(x_st[chunk % 2])

        @pl.when(chunk + 2 < n_chunks)
        def _():
            x_copy(chunk + 2).start()

        keep_kv(h_ref[rows, :], *tables(chunk), chunk * seqs)

        @pl.when(chip == 0)
        def _():
            send_both(chunk)

        for c in range(1, last_chip):
            @pl.when((chip == c) & (chunk == 0))
            def _():
                for i in range(AHEAD):
                    own_send(i, 0, last_chip, c).start()

            @pl.when((chip == c) & (chunk == n_chunks - 1))
            def _():
                for i in range(kept, n_seq):
                    own_send(i, 0, 0, c).start()
                if c == 1:
                    for i in range(straight, kept):
                        own_send(i, 1, 0, c).start()

        return carry

    lax.fori_loop(0, n_chunks, project_kv, 0)

    def turn_wq(i, carry):
        for k in range(2):
            w_copy(wq_hbm, 2 * i + k, k).wait()
            w_ref[pl.ds(pl.multiple_of((2 * i + k) * WBLOCK, WBLOCK), WBLOCK), :] = w_st[k].T

            @pl.when(2 * i + k + 2 < q_blocks)
            def _():
                w_copy(wq_hbm, 2 * i + k + 2, k).start()

        return carry

    lax.fori_loop(0, q_blocks // 2, turn_wq, 0)

    def forwards(c, seq):
        by_second = (core == 1) | (seq % 4 == 3)
        return (seq < kept) & (by_second if c == 2 else jnp.logical_not(by_second))

    def hop(seq):
        for c in range(1, last_chip):
            @pl.when(chip == c)
            def _():
                own_send(seq, 0, c, 0).wait_recv()

                @pl.when(forwards(c, seq))
                def _():
                    forward(seq, 0, last_chip).start()

                @pl.when((seq + LEAD >= AHEAD) & (seq + LEAD < kept))
                def _():
                    own_send(seq + LEAD, 0, last_chip, c).start()

        @pl.when(chip == last_chip)
        def _():
            own_send(seq, 0, last_chip, 1).wait_recv()
            forward(seq, 1, 2).start()

    def project_q(i, carry):
        chunk, part = i // 2, i % 2
        h = h_ref[pl.ds(pl.multiple_of(chunk * CHUNK, CHUNK), CHUNK), :]
        keep_q(h, *tables(chunk), chunk * seqs, pl.multiple_of(part * q_rows, q_rows))

        @pl.when((part == 1) & ((chip < last_chip) | (chunk < 1)))
        def _():
            hop(chunk)

        return carry

    lax.fori_loop(0, 2 * n_chunks, project_q, 0)

    @pl.when(chip == 0)
    def _():
        for copy in host_copies:
            copy.wait_recv()
        guest_in = pltpu.make_async_copy(gx_hbm, x_st.at[0, pl.ds(0, guest_rows)], x_sem.at[0])
        guest_in.start()
        guest_in.wait()
        h_ref[:guest_rows, :] = normed(x_st[0, :guest_rows])
        cos, sin = [jnp.concatenate([gtab[k, g] for g in range(GUESTS)], axis=1) for k in range(2)]
        keep_kv(h_ref[:guest_rows, :], cos, sin, n_seq)
        for part in range(2):
            keep_q(h_ref[:guest_rows, :], cos, sin, n_seq, part * q_rows)

    wo_copy = pltpu.make_async_copy(wo_hbm, w_ref, wo_sem)
    wo_copy.start()
    guest_turns = jnp.where(chip == 0, GUESTS // 2, 0)
    steps = jnp.where(chip == 0, n_seq + GUESTS, jnp.where(chip == last_chip, kept, n_seq))

    def xr_start(turn):
        @pl.when(turn < guest_turns)
        def _():
            pltpu.make_async_copy(gx_hbm.at[pl.ds(turn * 2 * TOK, 2 * TOK), :], xr_ref.at[turn % 2], xr_sem.at[turn % 2]).start()

        @pl.when(turn >= guest_turns)
        def _():
            pltpu.make_async_copy(x_hbm.at[pl.ds((turn - guest_turns) * 2 * TOK, 2 * TOK), :], xr_ref.at[turn % 2], xr_sem.at[turn % 2]).start()

    def xr_wait(turn):
        pltpu.make_async_copy(x_hbm.at[pl.ds(0, 2 * TOK), :], xr_ref.at[turn % 2], xr_sem.at[turn % 2]).wait()

    def y_copy(turn, row):
        return pltpu.make_async_copy(y_st.at[turn % 2], y_hbm.at[pl.ds(row, 2 * TOK), :], y_sem.at[turn % 2])

    def guest_y(turn):
        return pltpu.make_async_remote_copy(
            src_ref=gy_st, dst_ref=y_hbm.at[pl.ds((kept + 2 * turn) * TOK, 2 * TOK), :], send_sem=gy_sem.at[0, turn],
            recv_sem=gy_sem.at[1, turn], device_id={'cp': 2 * last_chip + core}, device_id_type=MESH)

    xr_start(jnp.int32(0))
    xr_start(jnp.int32(1))

    def load(seq, a):
        return pltpu.make_async_copy(kv_hbm.at[seq, a], slot_ref.at[seq % 2, 2 * a + core], load_sem.at[seq % 2, a])

    def share(seq, a, src):
        return pltpu.make_async_remote_copy(
            src_ref=src, dst_ref=slot_ref.at[seq % 2, 2 * a + core], send_sem=sib_send.at[seq % 2, a],
            recv_sem=sib_recv.at[seq % 2, a], device_id={'cp': sibling}, device_id_type=MESH)

    def reuse(step, shares):
        pl.semaphore_wait(credit, 1)
        for a in range(shares):
            share(step, a, kv_st.at[0]).wait_send()

    def stage(c, seq):
        if c == 0:
            @pl.when(seq < GUESTS)
            def _():
                reuse(seq, last_chip + 1)

            @pl.when(seq >= GUESTS)
            def _():
                reuse(seq, 1)
        else:
            @pl.when(seq >= 2)
            def _():
                reuse(seq, c + 1)

        share(seq, c, kv_st.at[seq]).start()
        slot_ref[seq % 2, 2 * c + core] = kv_st[seq]
        hopped = 1 if c == last_chip else 0
        for a in [hopped] + [a for a in range(c) if a != hopped] if c else []:
            if a != hopped:
                own_send(seq, 0, c, a).wait_recv()
            elif c == last_chip:
                @pl.when(seq >= straight)
                def _():
                    own_send(seq, 0, c, a).wait_recv()
            share(seq, a, kv_hbm.at[seq, a]).start()
            load(seq, a).start()

    def stage_guest(g):
        seq = kept + g

        @pl.when(g == 0)
        def _():
            for k in range(straight, kept):
                own_send(k, 1, 0, 1).wait_recv()
                forward(k, 1, 2).start()

        for a, k in ((0, seq), (last_chip, n_seq + g)):
            share(seq, a, kv_st.at[k]).start()
            slot_ref[seq % 2, 2 * a + core] = kv_st[k]
        for a in range(1, last_chip):
            own_send(seq, 0, 0, a).wait_recv()
            if a == 1:
                forward(seq, 1, 2).start()
            share(seq, a, kv_hbm.at[seq, a]).start()
            load(seq, a).start()

    def arrived(c, seq):
        for a in range(c):
            load(seq, a).wait()
        for a in range(c + 1):
            share(seq, a, kv_st.at[0]).wait_recv()

    def guest_arrived(g):
        for a in range(1, last_chip):
            load(g, a).wait()
        for a in range(last_chip + 1):
            share(g, a, kv_st.at[0]).wait_recv()

    @pl.when(chip == 0)
    def _():
        stage_guest(0)

    for c in range(1, last_chip + 1):
        @pl.when(chip == c)
        def _():
            stage(c, 0)

    def project_out(turn):
        @pl.when(turn == 0)
        def _():
            wo_copy.wait()

        xr_wait(turn)

        @pl.when((turn >= 2) & (turn - 2 >= guest_turns))
        def _():
            y_copy(turn, 0).wait()

        width = 512
        for col in range(0, dim, width):
            proj = jnp.dot(o_ref[...], w_ref[:, col:col + width], preferred_element_type=F32)
            part = (xr_ref[turn % 2, :, col:col + width].astype(F32) + proj).astype(BF16)
            y_st[turn % 2, :, col:col + width] = part

            @pl.when(turn < guest_turns)
            def _():
                gy_st[:, col:col + width] = part

        @pl.when(turn >= guest_turns)
        def _():
            y_copy(turn, (turn - guest_turns) * 2 * TOK).start()

        @pl.when(turn < guest_turns)
        def _():
            guest_y(0).start()

        @pl.when(turn + 2 < steps // 2)
        def _():
            xr_start(turn + 2)

    buffers = (q_ref, slot_ref, bias_ref, s_ref, m_ref, ot_ref)

    def step(it, carry):
        @pl.when((chip == 0) & (it < GUESTS))
        def _():
            def stage_next():
                @pl.when(it + 1 < GUESTS)
                def _():
                    stage_guest(it + 1)

                @pl.when(it + 1 == GUESTS)
                def _():
                    stage(0, jnp.int32(0))

            def wait_next():
                @pl.when(it + 1 < GUESTS)
                def _():
                    guest_arrived(it + 1)

                @pl.when(it + 1 == GUESTS)
                def _():
                    arrived(0, 0)

            @pl.when(it == 0)
            def _():
                guest_arrived(0)

            attend(*buffers, n_seq + it, n_seq + jnp.minimum(it + 1, GUESTS - 1), it == 0, n_cp, lambda: None, stage_next, wait_next)

        for c in range(last_chip + 1):
            seq = it - GUESTS if c == 0 else it
            last = steps - 1 - (GUESTS if c == 0 else 0)

            @pl.when((chip == c) & (seq >= 0))
            def _():
                if c:
                    @pl.when(seq == 0)
                    def _():
                        arrived(c, seq)

                def stage_next():
                    if c == last_chip:
                        @pl.when(seq + 1 < straight)
                        def _():
                            hop(seq + 1)

                    @pl.when(seq < last)
                    def _():
                        stage(c, seq + 1)

                def pass_on():
                    if 0 < c < last_chip:
                        @pl.when(seq + AHEAD < n_seq)
                        def _():
                            hop(seq + AHEAD)

                def wait_next():
                    @pl.when(seq < last)
                    def _():
                        arrived(c, seq + 1)

                attend(*buffers, seq, jnp.minimum(seq + 1, last), seq == 0, 2 * (c + 1), pass_on, stage_next, wait_next)

        @pl.when(it + 2 < steps)
        def _():
            pl.semaphore_signal(credit, inc=1, device_id={'cp': sibling}, device_id_type=MESH)

        o_ref[pl.ds(pl.multiple_of(it % 2 * TOK, TOK), TOK), :] = ot_ref[...].T

        @pl.when(it % 2 == 1)
        def _():
            project_out(it // 2)

        return carry

    lax.fori_loop(0, steps, step, 0)

    for turn in range(2):
        y_copy(turn, 0).wait()
    for c in range(last_chip + 1):
        @pl.when(chip == c)
        def _():
            for seq in range(2):
                for a in range(c + 1):
                    share(seq, a, kv_st.at[0]).wait_send()

    @pl.when(chip == 0)
    def _():
        guest_y(0).wait_send()

    @pl.when(chip == last_chip)
    def _():
        for copy in host_copies:
            copy.wait_send()
        for turn in range(GUESTS // 2):
            guest_y(turn).wait_recv()

    def drain(seq, carry):
        @pl.when(chip == 0)
        def _():
            own_send(seq, 0, 1, 0).wait_send()
            own_send(seq, 1, 2, 0).wait_send()

            @pl.when(seq >= straight)
            def _():
                forward(seq, 1, 2).wait_send()

        @pl.when((chip == 1) & (seq >= straight) & (seq < kept))
        def _():
            own_send(seq, 1, 0, 1).wait_send()

        for c in range(1, last_chip):
            @pl.when(chip == c)
            def _():
                own_send(seq, 0, last_chip, c).wait_send()

                @pl.when(forwards(c, seq))
                def _():
                    forward(seq, 0, last_chip).wait_send()

        @pl.when((chip == last_chip) & (seq < straight))
        def _():
            forward(seq, 1, 2).wait_send()

        return carry

    lax.fori_loop(0, n_seq, drain, 0)


def solution(mesh):
    n_cp = mesh.shape['cp']

    def local_block(hidden, positions, norm_gain, w_query, w_key, w_value, w_out):
        batch, tokens, dim = hidden.shape
        kv_rows = 2 * w_key.shape[1]
        rows = batch * tokens
        chips = n_cp // 2
        x = hidden.reshape(rows, dim)
        inv_freq = 10000.0 ** (-2.0 * jnp.arange(HALF, dtype=F32) / HEAD)
        angles = positions.reshape(batch, 1, tokens).astype(F32) * inv_freq[None, :, None]
        hbm = pl.BlockSpec(memory_space=pl.ANY)
        vmem = pl.BlockSpec(memory_space=pltpu.VMEM)
        dma = pltpu.SemaphoreType.DMA
        y, _, _ = pl.pallas_call(
            functools.partial(block_kernel, n_cp),
            out_shape=[jax.ShapeDtypeStruct((rows, dim), BF16), jax.ShapeDtypeStruct((batch, chips - 1, kv_rows, TOK), BF16), jax.ShapeDtypeStruct((GUESTS * TOK, dim), BF16)],
            in_specs=[hbm, vmem, hbm, hbm, hbm, hbm, vmem, vmem],
            out_specs=[hbm, hbm, hbm],
            scratch_shapes=[
                pltpu.VMEM((2, CHUNK, dim), BF16),
                pltpu.VMEM((rows, dim), BF16),
                pltpu.VMEM((2, dim, WBLOCK), BF16),
                pltpu.VMEM((kv_rows, dim), BF16),
                pltpu.VMEM((dim, dim), BF16),
                pltpu.VMEM((batch + GUESTS, kv_rows, TOK), BF16),
                pltpu.VMEM((batch + GUESTS, dim, TOK), BF16),
                pltpu.VMEM((2, n_cp, kv_rows, TOK), BF16),
                pltpu.VMEM((n_cp * TOK, GROUP * TOK), F32),
                pltpu.VMEM((8, GROUP * TOK), F32),
                pltpu.VMEM((2 * TOK, GROUP * TOK), F32),
                pltpu.VMEM((dim, TOK), BF16),
                pltpu.VMEM((2 * TOK, dim), BF16),
                pltpu.VMEM((2, 2 * TOK, dim), BF16),
                pltpu.VMEM((2, 2 * TOK, dim), BF16),
                pltpu.VMEM((1, dim), F32),
                pltpu.VMEM((2, GUESTS, HALF, TOK), F32),
                pltpu.VMEM((GUESTS * TOK, dim), BF16),
                dma((2,)), dma((2,)), dma, dma((batch, chips - 1)), dma((batch, 2)), dma((batch,)),
                dma((2, chips - 1)), dma((2, chips)), dma((2, chips)), dma((2,)), dma((2,)), dma((2, 1)), dma((2, 2)), dma((2, GUESTS // 2)),
                pltpu.SemaphoreType.REGULAR,
            ],
            compiler_params=pltpu.CompilerParams(collective_id=0, has_side_effects=True, vmem_limit_bytes=62 * 2 ** 20),
            name='block',
        )(x, norm_gain.reshape(dim // 128, 128), w_query, w_key, w_value, w_out.reshape(dim, dim), jnp.cos(angles), jnp.sin(angles))
        return y.reshape(batch, tokens, dim)

    act_spec = P('dp', 'cp', None)
    return jax.shard_map(local_block, mesh=mesh, in_specs=(act_spec, P('dp', 'cp'), P(), P(), P(), P(), P()), out_specs=act_spec, check_vma=False)
```

```python
import functools

import jax
import jax.numpy as jnp
from jax import lax
from jax.experimental import pallas as pl
from jax.experimental.pallas import tpu as pltpu
from jax.sharding import PartitionSpec as P

MESH = pl.DeviceIdType.MESH
HEAD = 64
HALF = HEAD // 2
TOK = 128
GROUP = 4
AHEAD = 4
LEAD = 2
CHUNK = 4 * TOK
WBLOCK = 256
F32, BF16 = jnp.float32, jnp.bfloat16
NT = (((1,), (1,)), ((), ()))


def rope_rows(x, cos, sin):
    heads, n = x.shape[0] // HEAD, x.shape[1]
    x = x.reshape(heads, 2, HALF, n)
    a, b = x[:, 0], x[:, 1]
    rotated = jnp.stack([a * cos - b * sin, b * cos + a * sin], axis=1)
    return rotated.reshape(heads * HEAD, n)


def attend(q_ref, slot_ref, bias_ref, s_ref, m_ref, o_ref, seq, n_seq, n_blocks, pass_on, stage_next, wait_next):
    width = slot_ref.shape[2] // 2
    pairs = width // (2 * HEAD)
    key_chunks = n_blocks // 2
    kc = 2 * TOK
    cols = GROUP * TOK

    def queries(sq, g):
        base = g * GROUP * HEAD
        return jnp.concatenate([q_ref[sq, pl.ds(pl.multiple_of(base + i * HEAD, HEAD), HEAD), :] for i in range(GROUP)], axis=1)

    def scores(q, sq, g, c, peak):
        row = pl.ds(pl.multiple_of(g * HEAD, HEAD), HEAD)
        keys = jnp.concatenate([slot_ref[sq % 2, 2 * c + i, row, :].T for i in range(2)], axis=0)
        s = jnp.dot(keys, q, preferred_element_type=F32)
        if c == key_chunks - 1:
            s = s + bias_ref[...]
        s_ref[c * kc:(c + 1) * kc, :] = s
        top = jnp.max(s.reshape(kc // 8, 8, cols), axis=0)
        return top if peak is None else jnp.maximum(peak, top)

    def unit(g, sq_next, g_next, peak):
        peak = jnp.max(peak, axis=0, keepdims=True)
        q_next = queries(sq_next, g_next)
        vrow = pl.ds(pl.multiple_of(width + g * HEAD, HEAD), HEAD)
        total, out, peak_next = None, None, None
        for c in range(key_chunks):
            prob = jnp.exp(s_ref[c * kc:(c + 1) * kc, :] - peak)
            part = jnp.sum(prob.reshape(kc // 8, 8, cols), axis=0)
            total = part if total is None else total + part
            values = jnp.concatenate([slot_ref[seq % 2, 2 * c + i, vrow, :] for i in range(2)], axis=1)
            term = jnp.dot(values, prob.astype(BF16), preferred_element_type=F32)
            out = term if out is None else out + term
            peak_next = scores(q_next, sq_next, g_next, c, peak_next)
        out = out / jnp.sum(total, axis=0, keepdims=True)
        for i in range(GROUP):
            o_ref[pl.ds(pl.multiple_of((g * GROUP + i) * HEAD, HEAD), HEAD), :] = out[:, i * TOK:(i + 1) * TOK].astype(BF16)
        return peak_next

    @pl.when(seq == 0)
    def _():
        q_first, peak = queries(seq, 0), None
        for c in range(key_chunks):
            peak = scores(q_first, seq, 0, c, peak)
        m_ref[...] = peak

    def pair(j, carry):
        @pl.when(j == 0)
        def _():
            pass_on()

        @pl.when(j == 1)
        def _():
            stage_next()

        last = j == pairs - 1

        @pl.when(last)
        def _():
            wait_next()

        sq_next = jnp.where(last, jnp.minimum(seq + 1, n_seq - 1), seq)
        g_next = jnp.where(last, 0, 2 * j + 2)
        peak = unit(2 * j, seq, 2 * j + 1, m_ref[...])
        m_ref[...] = unit(2 * j + 1, sq_next, g_next, peak)
        return carry

    lax.fori_loop(0, pairs, pair, 0)


def block_kernel(
    n_cp, x_hbm, gain_ref, wq_hbm, wk_hbm, wv_hbm, wo_hbm, cos_ref, sin_ref, y_hbm, kv_hbm,
    x_st, h_ref, w_st, wkv_ref, w_ref, kv_st, q_ref, slot_ref, s_ref, m_ref, bias_ref, ot_ref, o_ref, xr_ref, y_st, gain_row,
    x_sem, w_sem, wo_sem, recv_sem, own_sem, fwd_sem, load_sem, sib_recv, sib_send, xr_sem, y_sem, credit,
):
    me = lax.axis_index('cp')
    chip, core = me // 2, me % 2
    sibling = me + 1 - 2 * core
    n_seq = kv_st.shape[0]
    dim = x_st.shape[2]
    kv_rows = wkv_ref.shape[0]
    n_chunks = n_seq * TOK // CHUNK
    seqs = CHUNK // TOK
    last_chip = n_cp // 2 - 1

    barrier = pltpu.get_barrier_semaphore()
    for step in range(1, n_cp):
        pl.semaphore_signal(barrier, inc=1, device_id={'cp': (me + step) % n_cp}, device_id_type=MESH)

    def x_copy(chunk):
        return pltpu.make_async_copy(x_hbm.at[pl.ds(chunk * CHUNK, CHUNK), :], x_st.at[chunk % 2], x_sem.at[chunk % 2])

    def w_copy(hbm, block, slot):
        return pltpu.make_async_copy(hbm.at[:, pl.ds(block * WBLOCK, WBLOCK)], w_st.at[slot], w_sem.at[slot])

    kv_blocks = [(wk_hbm, i) for i in range(kv_rows // 2 // WBLOCK)] + [(wv_hbm, i) for i in range(kv_rows // 2 // WBLOCK)]
    q_blocks = dim // WBLOCK
    x_copy(0).start()
    for i in range(2):
        w_copy(*kv_blocks[i], i).start()
    x_copy(1).start()

    key = lax.broadcasted_iota(jnp.int32, (2 * TOK, TOK), 0)
    tok = lax.broadcasted_iota(jnp.int32, (2 * TOK, TOK), 1)
    bias = jnp.where(key <= tok + core * TOK, 0.0, -jnp.inf).astype(F32)
    bias_ref[...] = jnp.concatenate([bias] * GROUP, axis=1)

    gain = gain_ref[...].astype(F32)
    for i in range(gain.shape[0]):
        gain_row[:, i * gain.shape[1]:(i + 1) * gain.shape[1]] = gain[i:i + 1]

    def tables(chunk):
        return [jnp.concatenate([t[chunk * seqs + i] for i in range(seqs)], axis=1) for t in (cos_ref, sin_ref)]

    for i, (hbm, block) in enumerate(kv_blocks):
        w_copy(hbm, block, i % 2).wait()
        wkv_ref[i * WBLOCK:(i + 1) * WBLOCK, :] = w_st[i % 2].T
        nxt = i + 2
        if nxt < len(kv_blocks):
            w_copy(*kv_blocks[nxt], i % 2).start()
        else:
            w_copy(wq_hbm, nxt - len(kv_blocks), i % 2).start()

    def own_send(seq, target, to_chip, from_chip):
        return pltpu.make_async_remote_copy(
            src_ref=kv_st.at[seq], dst_ref=kv_hbm.at[seq, from_chip], send_sem=own_sem.at[seq, target],
            recv_sem=recv_sem.at[seq, from_chip], device_id={'cp': 2 * to_chip + core}, device_id_type=MESH)

    def forward(seq, block, to_chip):
        return pltpu.make_async_remote_copy(
            src_ref=kv_hbm.at[seq, block], dst_ref=kv_hbm.at[seq, block], send_sem=fwd_sem.at[seq],
            recv_sem=recv_sem.at[seq, block], device_id={'cp': 2 * to_chip + core}, device_id_type=MESH)

    def project_kv(chunk, carry):
        x_copy(chunk).wait()
        x = x_st[chunk % 2].astype(F32)
        inv_rms = lax.rsqrt(jnp.mean(x * x, axis=-1, keepdims=True) + 1e-5)
        rows = pl.ds(pl.multiple_of(chunk * CHUNK, CHUNK), CHUNK)
        h_ref[rows, :] = (x * inv_rms * gain_row[...]).astype(BF16)

        @pl.when(chunk + 2 < n_chunks)
        def _():
            x_copy(chunk + 2).start()

        kv = lax.dot_general(wkv_ref[...], h_ref[rows, :], NT, preferred_element_type=F32)
        k = rope_rows(kv[:kv_rows // 2], *tables(chunk)).astype(BF16)
        v = kv[kv_rows // 2:].astype(BF16)
        for i in range(seqs):
            kv_st[chunk * seqs + i, :kv_rows // 2, :] = k[:, i * TOK:(i + 1) * TOK]
            kv_st[chunk * seqs + i, kv_rows // 2:, :] = v[:, i * TOK:(i + 1) * TOK]

        @pl.when(chunk == 0)
        def _():
            pl.semaphore_wait(barrier, n_cp - 1)

        @pl.when(chip == 0)
        def _():
            for i in range(seqs):
                own_send(chunk * seqs + i, 0, 1, 0).start()
                own_send(chunk * seqs + i, 1, 2, 0).start()

        for c in range(1, last_chip):
            @pl.when((chip == c) & (chunk == 0))
            def _():
                for i in range(AHEAD):
                    own_send(i, 0, last_chip, c).start()

        return carry

    lax.fori_loop(0, n_chunks, project_kv, 0)

    def turn_wq(i, carry):
        for k in range(2):
            w_copy(wq_hbm, 2 * i + k, k).wait()
            w_ref[pl.ds(pl.multiple_of((2 * i + k) * WBLOCK, WBLOCK), WBLOCK), :] = w_st[k].T

            @pl.when(2 * i + k + 2 < q_blocks)
            def _():
                w_copy(wq_hbm, 2 * i + k + 2, k).start()

        return carry

    lax.fori_loop(0, q_blocks // 2, turn_wq, 0)

    def hop(seq):
        for c in range(1, last_chip):
            @pl.when(chip == c)
            def _():
                own_send(seq, 0, c, 0).wait_recv()

                @pl.when(core == c - 1)
                def _():
                    forward(seq, 0, last_chip).start()

                @pl.when((seq + LEAD >= AHEAD) & (seq + LEAD < n_seq))
                def _():
                    own_send(seq + LEAD, 0, last_chip, c).start()

        @pl.when(chip == last_chip)
        def _():
            own_send(seq, 0, last_chip, 1).wait_recv()
            forward(seq, 1, 2).start()

    q_rows = dim // 2

    def project_q(i, carry):
        chunk, part = i // 2, i % 2
        base = pl.multiple_of(part * q_rows, q_rows)
        h = h_ref[pl.ds(pl.multiple_of(chunk * CHUNK, CHUNK), CHUNK), :]
        q = lax.dot_general(w_ref[pl.ds(base, q_rows), :], h, NT, preferred_element_type=F32)
        q = (rope_rows(q, *tables(chunk)) * (HEAD ** -0.5)).astype(BF16)
        for k in range(seqs):
            q_ref[chunk * seqs + k, pl.ds(base, q_rows), :] = q[:, k * TOK:(k + 1) * TOK]

        @pl.when((part == 1) & ((chip < last_chip) | (chunk < LEAD)))
        def _():
            hop(chunk)

        return carry

    lax.fori_loop(0, 2 * n_chunks, project_q, 0)
    wo_copy = pltpu.make_async_copy(wo_hbm, w_ref, wo_sem)
    wo_copy.start()

    def xr_copy(p):
        return pltpu.make_async_copy(x_hbm.at[pl.ds(p * 2 * TOK, 2 * TOK), :], xr_ref.at[p % 2], xr_sem.at[p % 2])

    def y_copy(p):
        return pltpu.make_async_copy(y_st.at[p % 2], y_hbm.at[pl.ds(p * 2 * TOK, 2 * TOK), :], y_sem.at[p % 2])

    xr_copy(0).start()
    xr_copy(1).start()

    def load(seq, a):
        return pltpu.make_async_copy(kv_hbm.at[seq, a], slot_ref.at[seq % 2, 2 * a + core], load_sem.at[seq % 2, a])

    def share(seq, a, src):
        return pltpu.make_async_remote_copy(
            src_ref=src, dst_ref=slot_ref.at[seq % 2, 2 * a + core], send_sem=sib_send.at[seq % 2, a],
            recv_sem=sib_recv.at[seq % 2, a], device_id={'cp': sibling}, device_id_type=MESH)

    def stage(c, seq):
        @pl.when(seq >= 2)
        def _():
            pl.semaphore_wait(credit, 1)
            for a in range(c + 1):
                share(seq, a, kv_st.at[seq]).wait_send()

        share(seq, c, kv_st.at[seq]).start()
        slot_ref[seq % 2, 2 * c + core] = kv_st[seq]
        hopped = 1 if c == last_chip else 0
        for a in [hopped] + [a for a in range(c) if a != hopped] if c else []:
            if a != hopped:
                own_send(seq, 0, c, a).wait_recv()
            share(seq, a, kv_hbm.at[seq, a]).start()
            load(seq, a).start()

    @pl.when(chip < last_chip)
    def _():
        hop(AHEAD)

    for c in range(last_chip + 1):
        @pl.when(chip == c)
        def _():
            stage(c, 0)

    def project_out(p):
        @pl.when(p == 0)
        def _():
            wo_copy.wait()

        xr_copy(p).wait()

        @pl.when(p >= 2)
        def _():
            y_copy(p - 2).wait()

        step = 512
        for col in range(0, dim, step):
            proj = jnp.dot(o_ref[...], w_ref[:, col:col + step], preferred_element_type=F32)
            y_st[p % 2, :, col:col + step] = (xr_ref[p % 2, :, col:col + step].astype(F32) + proj).astype(BF16)
        y_copy(p).start()

        @pl.when(p + 2 < n_seq // 2)
        def _():
            xr_copy(p + 2).start()

    def sequence(seq, carry):
        for c in range(last_chip + 1):
            @pl.when(chip == c)
            def _():
                def arrived(sq):
                    for a in range(c):
                        load(sq, a).wait()
                    for a in range(c + 1):
                        share(sq, a, kv_st.at[sq]).wait_recv()

                @pl.when(seq == 0)
                def _():
                    arrived(seq)

                def stage_next():
                    if c == last_chip:
                        @pl.when(seq + LEAD < n_seq)
                        def _():
                            hop(seq + LEAD)

                    @pl.when(seq + 1 < n_seq)
                    def _():
                        stage(c, seq + 1)

                def pass_on():
                    if 0 < c < last_chip:
                        due = AHEAD + 1 + seq + seq // 4

                        @pl.when(due < n_seq)
                        def _():
                            hop(due)

                        @pl.when((seq % 4 == 3) & (due + 1 < n_seq))
                        def _():
                            hop(due + 1)

                def wait_next():
                    @pl.when(seq + 1 < n_seq)
                    def _():
                        arrived(seq + 1)

                attend(q_ref, slot_ref, bias_ref, s_ref, m_ref, ot_ref, seq, n_seq, 2 * (c + 1), pass_on, stage_next, wait_next)

        @pl.when(seq + 2 < n_seq)
        def _():
            pl.semaphore_signal(credit, inc=1, device_id={'cp': sibling}, device_id_type=MESH)

        o_ref[pl.ds(pl.multiple_of(seq % 2 * TOK, TOK), TOK), :] = ot_ref[...].T

        @pl.when(seq % 2 == 1)
        def _():
            project_out(seq // 2)

        return carry

    lax.fori_loop(0, n_seq, sequence, 0)

    for p in (n_seq // 2 - 2, n_seq // 2 - 1):
        y_copy(p).wait()
    for c in range(last_chip + 1):
        @pl.when(chip == c)
        def _():
            for seq in (n_seq - 2, n_seq - 1):
                for a in range(c + 1):
                    share(seq, a, kv_st.at[seq]).wait_send()

    def drain(seq, carry):
        @pl.when(chip == 0)
        def _():
            own_send(seq, 0, 1, 0).wait_send()
            own_send(seq, 1, 2, 0).wait_send()

        for c in range(1, last_chip):
            @pl.when(chip == c)
            def _():
                own_send(seq, 0, last_chip, c).wait_send()

                @pl.when(core == c - 1)
                def _():
                    forward(seq, 0, last_chip).wait_send()

        @pl.when(chip == last_chip)
        def _():
            forward(seq, 1, 2).wait_send()

        return carry

    lax.fori_loop(0, n_seq, drain, 0)


def solution(mesh):
    n_cp = mesh.shape['cp']

    def local_block(hidden, positions, norm_gain, w_query, w_key, w_value, w_out):
        batch, tokens, dim = hidden.shape
        kv_rows = 2 * w_key.shape[1]
        rows = batch * tokens
        chips = n_cp // 2
        x = hidden.reshape(rows, dim)
        inv_freq = 10000.0 ** (-2.0 * jnp.arange(HALF, dtype=F32) / HEAD)
        angles = positions.reshape(batch, 1, tokens).astype(F32) * inv_freq[None, :, None]
        hbm = pl.BlockSpec(memory_space=pl.ANY)
        vmem = pl.BlockSpec(memory_space=pltpu.VMEM)
        dma = pltpu.SemaphoreType.DMA
        y, _ = pl.pallas_call(
            functools.partial(block_kernel, n_cp),
            out_shape=[jax.ShapeDtypeStruct((rows, dim), BF16), jax.ShapeDtypeStruct((batch, chips - 1, kv_rows, TOK), BF16)],
            in_specs=[hbm, vmem, hbm, hbm, hbm, hbm, vmem, vmem],
            out_specs=[hbm, hbm],
            scratch_shapes=[
                pltpu.VMEM((2, CHUNK, dim), BF16),
                pltpu.VMEM((rows, dim), BF16),
                pltpu.VMEM((2, dim, WBLOCK), BF16),
                pltpu.VMEM((kv_rows, dim), BF16),
                pltpu.VMEM((dim, dim), BF16),
                pltpu.VMEM((batch, kv_rows, TOK), BF16),
                pltpu.VMEM((batch, dim, TOK), BF16),
                pltpu.VMEM((2, n_cp, kv_rows, TOK), BF16),
                pltpu.VMEM((n_cp * TOK, GROUP * TOK), F32),
                pltpu.VMEM((8, GROUP * TOK), F32),
                pltpu.VMEM((2 * TOK, GROUP * TOK), F32),
                pltpu.VMEM((dim, TOK), BF16),
                pltpu.VMEM((2 * TOK, dim), BF16),
                pltpu.VMEM((2, 2 * TOK, dim), BF16),
                pltpu.VMEM((2, 2 * TOK, dim), BF16),
                pltpu.VMEM((1, dim), F32),
                dma((2,)), dma((2,)), dma, dma((batch, chips - 1)), dma((batch, 2)), dma((batch,)),
                dma((2, chips - 1)), dma((2, chips)), dma((2, chips)), dma((2,)), dma((2,)),
                pltpu.SemaphoreType.REGULAR,
            ],
            compiler_params=pltpu.CompilerParams(collective_id=0, has_side_effects=True, vmem_limit_bytes=62 * 2 ** 20),
            name='block',
        )(x, norm_gain.reshape(dim // 128, 128), w_query, w_key, w_value, w_out.reshape(dim, dim), jnp.cos(angles), jnp.sin(angles))
        return y.reshape(batch, tokens, dim)

    act_spec = P('dp', 'cp', None)
    return jax.shard_map(local_block, mesh=mesh, in_specs=(act_spec, P('dp', 'cp'), P(), P(), P(), P(), P()), out_specs=act_spec, check_vma=False)
```

```python
import functools

import jax
import jax.numpy as jnp
from jax import lax
from jax.experimental import pallas as pl
from jax.experimental.pallas import tpu as pltpu
from jax.sharding import PartitionSpec as P

MESH = pl.DeviceIdType.MESH
HEAD = 64
HALF = HEAD // 2
TOK = 128
GROUP = 4
AHEAD = 4
LEAD = 2
CHUNK = 4 * TOK
WBLOCK = 256
F32, BF16 = jnp.float32, jnp.bfloat16
NT = (((1,), (1,)), ((), ()))


def rope_rows(x, cos, sin):
    heads, n = x.shape[0] // HEAD, x.shape[1]
    x = x.reshape(heads, 2, HALF, n)
    a, b = x[:, 0], x[:, 1]
    rotated = jnp.stack([a * cos - b * sin, b * cos + a * sin], axis=1)
    return rotated.reshape(heads * HEAD, n)


def attend(q_ref, slot_ref, bias_ref, s_ref, m_ref, o_ref, seq, n_seq, n_blocks, pass_on, stage_next, wait_next):
    width = slot_ref.shape[2] // 2
    pairs = width // (2 * HEAD)
    key_chunks = n_blocks // 2
    kc = 2 * TOK
    cols = GROUP * TOK

    def queries(sq, g):
        base = g * GROUP * HEAD
        return jnp.concatenate([q_ref[sq, pl.ds(pl.multiple_of(base + i * HEAD, HEAD), HEAD), :] for i in range(GROUP)], axis=1)

    def scores(q, sq, g, c, peak):
        row = pl.ds(pl.multiple_of(g * HEAD, HEAD), HEAD)
        keys = jnp.concatenate([slot_ref[sq % 2, 2 * c + i, row, :].T for i in range(2)], axis=0)
        s = jnp.dot(keys, q, preferred_element_type=F32)
        if c == key_chunks - 1:
            s = s + bias_ref[...]
        s_ref[c * kc:(c + 1) * kc, :] = s
        top = jnp.max(s.reshape(kc // 8, 8, cols), axis=0)
        return top if peak is None else jnp.maximum(peak, top)

    def unit(g, sq_next, g_next, peak):
        peak = jnp.max(peak, axis=0, keepdims=True)
        q_next = queries(sq_next, g_next)
        vrow = pl.ds(pl.multiple_of(width + g * HEAD, HEAD), HEAD)
        total, out, peak_next = None, None, None
        for c in range(key_chunks):
            prob = jnp.exp(s_ref[c * kc:(c + 1) * kc, :] - peak)
            part = jnp.sum(prob.reshape(kc // 8, 8, cols), axis=0)
            total = part if total is None else total + part
            values = jnp.concatenate([slot_ref[seq % 2, 2 * c + i, vrow, :] for i in range(2)], axis=1)
            term = jnp.dot(values, prob.astype(BF16), preferred_element_type=F32)
            out = term if out is None else out + term
            peak_next = scores(q_next, sq_next, g_next, c, peak_next)
        out = out / jnp.sum(total, axis=0, keepdims=True)
        for i in range(GROUP):
            o_ref[pl.ds(pl.multiple_of((g * GROUP + i) * HEAD, HEAD), HEAD), :] = out[:, i * TOK:(i + 1) * TOK].astype(BF16)
        return peak_next

    @pl.when(seq == 0)
    def _():
        q_first, peak = queries(seq, 0), None
        for c in range(key_chunks):
            peak = scores(q_first, seq, 0, c, peak)
        m_ref[...] = peak

    def pair(j, carry):
        @pl.when(j == 0)
        def _():
            pass_on()

        @pl.when(j == 1)
        def _():
            stage_next()

        last = j == pairs - 1

        @pl.when(last)
        def _():
            wait_next()

        sq_next = jnp.where(last, jnp.minimum(seq + 1, n_seq - 1), seq)
        g_next = jnp.where(last, 0, 2 * j + 2)
        peak = unit(2 * j, seq, 2 * j + 1, m_ref[...])
        m_ref[...] = unit(2 * j + 1, sq_next, g_next, peak)
        return carry

    lax.fori_loop(0, pairs, pair, 0)


def block_kernel(
    n_cp, x_hbm, gain_ref, wq_hbm, wk_hbm, wv_hbm, wo_hbm, cos_ref, sin_ref, y_hbm, kv_hbm,
    x_st, h_ref, w_st, wkv_ref, w_ref, kv_st, q_ref, slot_ref, s_ref, m_ref, bias_ref, ot_ref, o_ref, xr_ref, y_st, gain_row,
    x_sem, w_sem, wo_sem, recv_sem, own_sem, fwd_sem, load_sem, sib_recv, sib_send, xr_sem, y_sem, credit,
):
    me = lax.axis_index('cp')
    chip, core = me // 2, me % 2
    sibling = me + 1 - 2 * core
    n_seq = kv_st.shape[0]
    dim = x_st.shape[2]
    kv_rows = wkv_ref.shape[0]
    n_chunks = n_seq * TOK // CHUNK
    seqs = CHUNK // TOK
    last_chip = n_cp // 2 - 1

    barrier = pltpu.get_barrier_semaphore()
    for step in range(1, n_cp):
        pl.semaphore_signal(barrier, inc=1, device_id={'cp': (me + step) % n_cp}, device_id_type=MESH)

    def x_copy(chunk):
        return pltpu.make_async_copy(x_hbm.at[pl.ds(chunk * CHUNK, CHUNK), :], x_st.at[chunk % 2], x_sem.at[chunk % 2])

    def w_copy(hbm, block, slot):
        return pltpu.make_async_copy(hbm.at[:, pl.ds(block * WBLOCK, WBLOCK)], w_st.at[slot], w_sem.at[slot])

    kv_blocks = [(wk_hbm, i) for i in range(kv_rows // 2 // WBLOCK)] + [(wv_hbm, i) for i in range(kv_rows // 2 // WBLOCK)]
    q_blocks = dim // WBLOCK
    x_copy(0).start()
    for i in range(2):
        w_copy(*kv_blocks[i], i).start()
    x_copy(1).start()

    key = lax.broadcasted_iota(jnp.int32, (2 * TOK, TOK), 0)
    tok = lax.broadcasted_iota(jnp.int32, (2 * TOK, TOK), 1)
    bias = jnp.where(key <= tok + core * TOK, 0.0, -jnp.inf).astype(F32)
    bias_ref[...] = jnp.concatenate([bias] * GROUP, axis=1)

    gain = gain_ref[...].astype(F32)
    for i in range(gain.shape[0]):
        gain_row[:, i * gain.shape[1]:(i + 1) * gain.shape[1]] = gain[i:i + 1]

    def tables(chunk):
        return [jnp.concatenate([t[chunk * seqs + i] for i in range(seqs)], axis=1) for t in (cos_ref, sin_ref)]

    for i, (hbm, block) in enumerate(kv_blocks):
        w_copy(hbm, block, i % 2).wait()
        wkv_ref[i * WBLOCK:(i + 1) * WBLOCK, :] = w_st[i % 2].T
        nxt = i + 2
        if nxt < len(kv_blocks):
            w_copy(*kv_blocks[nxt], i % 2).start()
        else:
            w_copy(wq_hbm, nxt - len(kv_blocks), i % 2).start()

    def own_send(seq, target, to_chip, from_chip):
        return pltpu.make_async_remote_copy(
            src_ref=kv_st.at[seq], dst_ref=kv_hbm.at[seq, from_chip], send_sem=own_sem.at[seq, target],
            recv_sem=recv_sem.at[seq, from_chip], device_id={'cp': 2 * to_chip + core}, device_id_type=MESH)

    def forward(seq, block, to_chip):
        return pltpu.make_async_remote_copy(
            src_ref=kv_hbm.at[seq, block], dst_ref=kv_hbm.at[seq, block], send_sem=fwd_sem.at[seq],
            recv_sem=recv_sem.at[seq, block], device_id={'cp': 2 * to_chip + core}, device_id_type=MESH)

    def project_kv(chunk, carry):
        x_copy(chunk).wait()
        x = x_st[chunk % 2].astype(F32)
        inv_rms = lax.rsqrt(jnp.mean(x * x, axis=-1, keepdims=True) + 1e-5)
        rows = pl.ds(pl.multiple_of(chunk * CHUNK, CHUNK), CHUNK)
        h_ref[rows, :] = (x * inv_rms * gain_row[...]).astype(BF16)

        @pl.when(chunk + 2 < n_chunks)
        def _():
            x_copy(chunk + 2).start()

        kv = lax.dot_general(wkv_ref[...], h_ref[rows, :], NT, preferred_element_type=F32)
        k = rope_rows(kv[:kv_rows // 2], *tables(chunk)).astype(BF16)
        v = kv[kv_rows // 2:].astype(BF16)
        for i in range(seqs):
            kv_st[chunk * seqs + i, :kv_rows // 2, :] = k[:, i * TOK:(i + 1) * TOK]
            kv_st[chunk * seqs + i, kv_rows // 2:, :] = v[:, i * TOK:(i + 1) * TOK]

        @pl.when(chunk == 0)
        def _():
            pl.semaphore_wait(barrier, n_cp - 1)

        @pl.when(chip == 0)
        def _():
            for i in range(seqs):
                own_send(chunk * seqs + i, 0, 1, 0).start()
                own_send(chunk * seqs + i, 1, 2, 0).start()

        for c in range(1, last_chip):
            @pl.when((chip == c) & (chunk == 0))
            def _():
                for i in range(AHEAD):
                    own_send(i, 0, last_chip, c).start()

        return carry

    lax.fori_loop(0, n_chunks, project_kv, 0)

    def turn_wq(i, carry):
        for k in range(2):
            w_copy(wq_hbm, 2 * i + k, k).wait()
            w_ref[pl.ds(pl.multiple_of((2 * i + k) * WBLOCK, WBLOCK), WBLOCK), :] = w_st[k].T

            @pl.when(2 * i + k + 2 < q_blocks)
            def _():
                w_copy(wq_hbm, 2 * i + k + 2, k).start()

        return carry

    lax.fori_loop(0, q_blocks // 2, turn_wq, 0)

    def hop(seq):
        for c in range(1, last_chip):
            @pl.when(chip == c)
            def _():
                own_send(seq, 0, c, 0).wait_recv()

                @pl.when(core == c - 1)
                def _():
                    forward(seq, 0, last_chip).start()

                @pl.when((seq + LEAD >= AHEAD) & (seq + LEAD < n_seq))
                def _():
                    own_send(seq + LEAD, 0, last_chip, c).start()

        @pl.when(chip == last_chip)
        def _():
            own_send(seq, 0, last_chip, 1).wait_recv()
            forward(seq, 1, 2).start()

    q_rows = dim // 2

    def project_q(i, carry):
        chunk, part = i // 2, i % 2
        base = pl.multiple_of(part * q_rows, q_rows)
        h = h_ref[pl.ds(pl.multiple_of(chunk * CHUNK, CHUNK), CHUNK), :]
        q = lax.dot_general(w_ref[pl.ds(base, q_rows), :], h, NT, preferred_element_type=F32)
        q = (rope_rows(q, *tables(chunk)) * (HEAD ** -0.5)).astype(BF16)
        for k in range(seqs):
            q_ref[chunk * seqs + k, pl.ds(base, q_rows), :] = q[:, k * TOK:(k + 1) * TOK]

        @pl.when((part == 1) & ((chip < last_chip) | (chunk < LEAD)))
        def _():
            hop(chunk)

        return carry

    lax.fori_loop(0, 2 * n_chunks, project_q, 0)
    wo_copy = pltpu.make_async_copy(wo_hbm, w_ref, wo_sem)
    wo_copy.start()

    def xr_copy(p):
        return pltpu.make_async_copy(x_hbm.at[pl.ds(p * 2 * TOK, 2 * TOK), :], xr_ref.at[p % 2], xr_sem.at[p % 2])

    def y_copy(p):
        return pltpu.make_async_copy(y_st.at[p % 2], y_hbm.at[pl.ds(p * 2 * TOK, 2 * TOK), :], y_sem.at[p % 2])

    xr_copy(0).start()
    xr_copy(1).start()

    def load(seq, a):
        return pltpu.make_async_copy(kv_hbm.at[seq, a], slot_ref.at[seq % 2, 2 * a + core], load_sem.at[seq % 2, a])

    def share(seq, a, src):
        return pltpu.make_async_remote_copy(
            src_ref=src, dst_ref=slot_ref.at[seq % 2, 2 * a + core], send_sem=sib_send.at[seq % 2, a],
            recv_sem=sib_recv.at[seq % 2, a], device_id={'cp': sibling}, device_id_type=MESH)

    def stage(c, seq):
        @pl.when(seq >= 2)
        def _():
            pl.semaphore_wait(credit, 1)
            for a in range(c + 1):
                share(seq, a, kv_st.at[seq]).wait_send()

        share(seq, c, kv_st.at[seq]).start()
        slot_ref[seq % 2, 2 * c + core] = kv_st[seq]
        hopped = 1 if c == last_chip else 0
        for a in [hopped] + [a for a in range(c) if a != hopped] if c else []:
            if a != hopped:
                own_send(seq, 0, c, a).wait_recv()
            share(seq, a, kv_hbm.at[seq, a]).start()
            load(seq, a).start()

    @pl.when(chip < last_chip)
    def _():
        hop(AHEAD)

    for c in range(last_chip + 1):
        @pl.when(chip == c)
        def _():
            stage(c, 0)

    def project_out(p):
        @pl.when(p == 0)
        def _():
            wo_copy.wait()

        xr_copy(p).wait()

        @pl.when(p >= 2)
        def _():
            y_copy(p - 2).wait()

        step = 512
        for col in range(0, dim, step):
            proj = jnp.dot(o_ref[...], w_ref[:, col:col + step], preferred_element_type=F32)
            y_st[p % 2, :, col:col + step] = (xr_ref[p % 2, :, col:col + step].astype(F32) + proj).astype(BF16)
        y_copy(p).start()

        @pl.when(p + 2 < n_seq // 2)
        def _():
            xr_copy(p + 2).start()

    def sequence(seq, carry):
        for c in range(last_chip + 1):
            @pl.when(chip == c)
            def _():
                def arrived(sq):
                    for a in range(c):
                        load(sq, a).wait()
                    for a in range(c + 1):
                        share(sq, a, kv_st.at[sq]).wait_recv()

                @pl.when(seq == 0)
                def _():
                    arrived(seq)

                def stage_next():
                    if c == last_chip:
                        @pl.when(seq + LEAD < n_seq)
                        def _():
                            hop(seq + LEAD)

                    @pl.when(seq + 1 < n_seq)
                    def _():
                        stage(c, seq + 1)

                def pass_on():
                    if 0 < c < last_chip:
                        due = AHEAD + 1 + seq + seq // 4

                        @pl.when(due < n_seq)
                        def _():
                            hop(due)

                        @pl.when((seq % 4 == 3) & (due + 1 < n_seq))
                        def _():
                            hop(due + 1)

                def wait_next():
                    @pl.when(seq + 1 < n_seq)
                    def _():
                        arrived(seq + 1)

                attend(q_ref, slot_ref, bias_ref, s_ref, m_ref, ot_ref, seq, n_seq, 2 * (c + 1), pass_on, stage_next, wait_next)

        @pl.when(seq + 2 < n_seq)
        def _():
            pl.semaphore_signal(credit, inc=1, device_id={'cp': sibling}, device_id_type=MESH)

        o_ref[pl.ds(pl.multiple_of(seq % 2 * TOK, TOK), TOK), :] = ot_ref[...].T

        @pl.when(seq % 2 == 1)
        def _():
            project_out(seq // 2)

        return carry

    lax.fori_loop(0, n_seq, sequence, 0)

    for p in (n_seq // 2 - 2, n_seq // 2 - 1):
        y_copy(p).wait()
    for c in range(last_chip + 1):
        @pl.when(chip == c)
        def _():
            for seq in (n_seq - 2, n_seq - 1):
                for a in range(c + 1):
                    share(seq, a, kv_st.at[seq]).wait_send()

    def drain(seq, carry):
        @pl.when(chip == 0)
        def _():
            own_send(seq, 0, 1, 0).wait_send()
            own_send(seq, 1, 2, 0).wait_send()

        for c in range(1, last_chip):
            @pl.when(chip == c)
            def _():
                own_send(seq, 0, last_chip, c).wait_send()

                @pl.when(core == c - 1)
                def _():
                    forward(seq, 0, last_chip).wait_send()

        @pl.when(chip == last_chip)
        def _():
            forward(seq, 1, 2).wait_send()

        return carry

    lax.fori_loop(0, n_seq, drain, 0)


def copy_kernel(src, dst, buffer, in_sem, out_sem):
    pieces, rows = buffer.shape[0], buffer.shape[1]
    part = lambda ref, i: ref.at[pl.ds(i * rows, rows), :]
    loads = [pltpu.make_async_copy(part(src, i), buffer.at[i], in_sem.at[i]) for i in range(pieces)]
    stores = [pltpu.make_async_copy(buffer.at[i], part(dst, i), out_sem.at[i]) for i in range(pieces)]
    for load in loads:
        load.start()
    for load, store in zip(loads, stores):
        load.wait()
        store.start()
    for store in stores:
        store.wait()


def solution(mesh):
    n_cp = mesh.shape['cp']

    def local_block(hidden, positions, norm_gain, w_query, w_key, w_value, w_out):
        batch, tokens, dim = hidden.shape
        kv_rows = 2 * w_key.shape[1]
        rows = batch * tokens
        chips = n_cp // 2
        x = hidden.reshape(rows, dim)
        inv_freq = 10000.0 ** (-2.0 * jnp.arange(HALF, dtype=F32) / HEAD)
        angles = positions.reshape(batch, 1, tokens).astype(F32) * inv_freq[None, :, None]
        hbm = pl.BlockSpec(memory_space=pl.ANY)
        vmem = pl.BlockSpec(memory_space=pltpu.VMEM)
        dma = pltpu.SemaphoreType.DMA
        y, _ = pl.pallas_call(
            functools.partial(block_kernel, n_cp),
            out_shape=[jax.ShapeDtypeStruct((rows, dim), BF16), jax.ShapeDtypeStruct((batch, chips - 1, kv_rows, TOK), BF16)],
            in_specs=[hbm, vmem, hbm, hbm, hbm, hbm, vmem, vmem],
            out_specs=[hbm, hbm],
            scratch_shapes=[
                pltpu.VMEM((2, CHUNK, dim), BF16),
                pltpu.VMEM((rows, dim), BF16),
                pltpu.VMEM((2, dim, WBLOCK), BF16),
                pltpu.VMEM((kv_rows, dim), BF16),
                pltpu.VMEM((dim, dim), BF16),
                pltpu.VMEM((batch, kv_rows, TOK), BF16),
                pltpu.VMEM((batch, dim, TOK), BF16),
                pltpu.VMEM((2, n_cp, kv_rows, TOK), BF16),
                pltpu.VMEM((n_cp * TOK, GROUP * TOK), F32),
                pltpu.VMEM((8, GROUP * TOK), F32),
                pltpu.VMEM((2 * TOK, GROUP * TOK), F32),
                pltpu.VMEM((dim, TOK), BF16),
                pltpu.VMEM((2 * TOK, dim), BF16),
                pltpu.VMEM((2, 2 * TOK, dim), BF16),
                pltpu.VMEM((2, 2 * TOK, dim), BF16),
                pltpu.VMEM((1, dim), F32),
                dma((2,)), dma((2,)), dma, dma((batch, chips - 1)), dma((batch, 2)), dma((batch,)),
                dma((2, chips - 1)), dma((2, chips)), dma((2, chips)), dma((2,)), dma((2,)),
                pltpu.SemaphoreType.REGULAR,
            ],
            compiler_params=pltpu.CompilerParams(collective_id=0, has_side_effects=True, vmem_limit_bytes=62 * 2 ** 20),
            name='block',
        )(x, norm_gain.reshape(dim // 128, 128), w_query, w_key, w_value, w_out.reshape(dim, dim), jnp.cos(angles), jnp.sin(angles))
        y = pl.pallas_call(
            copy_kernel,
            out_shape=jax.ShapeDtypeStruct((rows, dim), BF16),
            in_specs=[hbm],
            out_specs=hbm,
            scratch_shapes=[pltpu.VMEM((batch, tokens, dim), BF16), dma((batch,)), dma((batch,))],
            compiler_params=pltpu.CompilerParams(vmem_limit_bytes=62 * 2 ** 20),
            name='result',
        )(y)
        return y.reshape(batch, tokens, dim)

    act_spec = P('dp', 'cp', None)
    return jax.shard_map(local_block, mesh=mesh, in_specs=(act_spec, P('dp', 'cp'), P(), P(), P(), P(), P()), out_specs=act_spec, check_vma=False)
```
